32 devices in a mesh: dp: 8 (over z, x), expert: 4 (over y, core).
Axes of the slice: x: 2, y: 2, z: 4, core: 2. Of those that a mesh axis runs over, the one named last changes fastest.
Arguments:
- tokens: bfloat16 [12288, 1024], P(('dp', 'expert')), may hold values from -50 to 50
- cotangent: bfloat16 [12288, 1024], P(('dp', 'expert')), may hold values from -6 to 6
- routes: int32 [12288, 2], P(('dp', 'expert')), may hold values from 0 to 3, all different within a row; in each aligned block of 384 rows (0 to 383, 384 to 767, ...) at most 240 rows name the same one
- prefix: int32 [32], P(('dp', 'expert')), may hold values from 0 to 384
- buckets: int32 [767], replicated, may hold values from 0 to 31
- step_count: int32 [], replicated, may hold values from 1 to 20
- learn_rate: float32 [], replicated, may hold values from 0.02 to 0.1
- weight_decay: float32 [], replicated, may hold values from 0.1 to 0.5
- attend_master: float32 [3, 1024, 1024], P(None, ('dp', 'expert')), may hold values from -0.1875 to 0.1875
- attend_first: float32 [3, 1024, 1024], P(None, ('dp', 'expert')), may hold values from -0.625 to 0.625
- attend_second: float32 [3, 1024, 1024], P(None, ('dp', 'expert')), may hold values from 0.053 to 0.21
- outward_master: float32 [1024, 1024], P(('dp', 'expert')), may hold values from -2.5 to 2.5
- outward_first: float32 [1024, 1024], P(('dp', 'expert')), may hold values from -0.625 to 0.625
- outward_second: float32 [1024, 1024], P(('dp', 'expert')), may hold values from 0.053 to 0.21
- router_master: float32 [1024, 4], P(('dp', 'expert')), may hold values from -0.1875 to 0.1875
- router_first: float32 [1024, 4], P(('dp', 'expert')), may hold values from -0.625 to 0.625
- router_second: float32 [1024, 4], P(('dp', 'expert')), may hold values from 0.053 to 0.21
- gains_master: float32 [2, 1024], P(None, ('dp', 'expert')), may hold values from 0.5 to 1.5
- gains_first: float32 [2, 1024], P(None, ('dp', 'expert')), may hold values from -0.625 to 0.625
- gains_second: float32 [2, 1024], P(None, ('dp', 'expert')), may hold values from 0.053 to 0.21
- bias_master: float32 [512], P(('dp', 'expert')), may hold values from -6 to 6
- bias_first: float32 [512], P(('dp', 'expert')), may hold values from -0.625 to 0.625
- bias_second: float32 [512], P(('dp', 'expert')), may hold values from 0.053 to 0.21
- upward_master: float32 [2, 4, 1024, 2816], P(None, 'expert', 'dp'), may hold values from -0.1875 to 0.1875
- upward_first: float32 [2, 4, 1024, 2816], P(None, 'expert', 'dp'), may hold values from -0.625 to 0.625
- upward_second: float32 [2, 4, 1024, 2816], P(None, 'expert', 'dp'), may hold values from 0.053 to 0.21
- downward_master: float32 [4, 2816, 1024], P('expert', 'dp'), may hold values from -0.109375 to 0.109375
- downward_first: float32 [4, 2816, 1024], P('expert', 'dp'), may hold values from -0.625 to 0.625
- downward_second: float32 [4, 2816, 1024], P('expert', 'dp'), may hold values from 0.053 to 0.21
Outputs:
- block_output: bfloat16 [12288, 1024], P(('dp', 'expert'))
- input_grad: bfloat16 [12288, 1024], P(('dp', 'expert'))
- attend_grad: float32 [3, 1024, 1024], P(None, ('dp', 'expert'))
- attend_updated: float32 [3, 1024, 1024], P(None, ('dp', 'expert'))
- attend_mean: float32 [3, 1024, 1024], P(None, ('dp', 'expert'))
- attend_square: float32 [3, 1024, 1024], P(None, ('dp', 'expert'))
- outward_grad: float32 [1024, 1024], P(('dp', 'expert'))
- outward_updated: float32 [1024, 1024], P(('dp', 'expert'))
- outward_mean: float32 [1024, 1024], P(('dp', 'expert'))
- outward_square: float32 [1024, 1024], P(('dp', 'expert'))
- router_grad: float32 [1024, 4], P(('dp', 'expert'))
- router_updated: float32 [1024, 4], P(('dp', 'expert'))
- router_mean: float32 [1024, 4], P(('dp', 'expert'))
- router_square: float32 [1024, 4], P(('dp', 'expert'))
- gains_grad: float32 [2, 1024], P(None, ('dp', 'expert'))
- gains_updated: float32 [2, 1024], P(None, ('dp', 'expert'))
- gains_mean: float32 [2, 1024], P(None, ('dp', 'expert'))
- gains_square: float32 [2, 1024], P(None, ('dp', 'expert'))
- bias_grad: float32 [512], P(('dp', 'expert'))
- bias_updated: float32 [512], P(('dp', 'expert'))
- bias_mean: float32 [512], P(('dp', 'expert'))
- bias_square: float32 [512], P(('dp', 'expert'))
- upward_grad: float32 [2, 4, 1024, 2816], P(None, 'expert', 'dp')
- upward_updated: float32 [2, 4, 1024, 2816], P(None, 'expert', 'dp')
- upward_mean: float32 [2, 4, 1024, 2816], P(None, 'expert', 'dp')
- upward_square: float32 [2, 4, 1024, 2816], P(None, 'expert', 'dp')
- downward_grad: float32 [4, 2816, 1024], P('expert', 'dp')
- downward_updated: float32 [4, 2816, 1024], P('expert', 'dp')
- downward_mean: float32 [4, 2816, 1024], P('expert', 'dp')
- downward_square: float32 [4, 2816, 1024], P('expert', 'dp')
- grad_rms: float32 [7], replicated
The draws below stay inside these ranges and needn't reach their ends.
Inputs may be any that keep to these rules, and one draw needn't show every extreme that they name: `routes`: each row names 2 different experts; among the 384 rows of one sequence no expert is named more than 240 times, and in some sequence one expert is named exactly 240 times.
All inputs are finite; a program needn't handle non-finite values.
Results may differ from the reference program's by a relative error of at most 0.014.
The reference program's roundings to bfloat16 on the way count: a program that leaves them out, or rounds other values in their place, can miss the bound.
Values may be sent and summed in bfloat16 or wider, within the bound.
A program may use at most 384 MiB of HBM per device.

```python
import math
import jax
import jax.numpy as jnp
import numpy as np
from jax import lax

D = 1024
HEADS = 16
HEAD_DIM = 64
FF = 2816
BUCKETS = 32
TOP = 2
TOK_DEV = 384
EXPERTS = 4
SEQS = 32
TOKENS = 12288
CAP = 240


def draw_tokens(key, part):
    columns = jnp.arange(D).astype(jnp.float32) / (D - 1)
    base = jnp.clip(jax.random.normal(key, (TOKENS, D), jnp.float32), -5.0, 5.0)
    spread = math.sqrt((10.0 ** 2.0 - 1.0) / (2.0 * math.log(10.0)))
    column_scale = jnp.power(jnp.float32(10.0), columns) / spread
    return (base * column_scale[None, :]).astype(jnp.bfloat16)


def touch_ends(array, stream_key, smallest, largest):
    spot = [jax.random.randint(jax.random.fold_in(stream_key, axis), (), 0, length) for axis, length in enumerate(array.shape)]
    main_axis = array.shape.index(max(array.shape))
    neighbour = spot[:main_axis] + [(spot[main_axis] + 1) % array.shape[main_axis]] + spot[main_axis + 1:]
    return array.at[tuple(spot)].set(smallest).at[tuple(neighbour)].set(largest)


def levels(own_key, dims, cuts, least, largest):
    def one(position, parts):
        heights = jax.random.uniform(jax.random.fold_in(jax.random.fold_in(own_key, 6), position), (parts,), jnp.float32, least / len(cuts), largest / len(cuts))
        return jnp.repeat(jnp.exp(heights), dims[position] // parts).reshape((-1,) + (1,) * (len(dims) - position - 1))

    level = one(*cuts[0])
    for cut in cuts[1:]:
        level = level * one(*cut)
    return level


def routed_block(key, own, number, rows, count, top, bound, lean):
    ranking = jax.random.permutation(key, count)
    crowded, usual = load_shares(count, rows * top, bound, lean, True), load_shares(count, rows * top, bound, lean, False)
    places = jnp.arange(count)

    def named(lengths, offset_by):
        used = int((lengths > 0).sum())
        fixed = max(1, used // 4)
        passed = fixed + (places - fixed + offset_by * (used - fixed)) % max(1, count - fixed)
        return jnp.zeros((count,), jnp.int32).at[ranking[jnp.where(places < fixed, places, passed)]].set(jnp.asarray(lengths, jnp.int32))

    lengths = jnp.where(number % 4 == 0, named(crowded, number // 4), named(usual, number - number // 4 - 1))
    mixed = jax.random.permutation(jax.random.fold_in(own, 3), count)
    source_of, receiver = mixed[0:count // 2 * 2:2], mixed[1:count // 2 * 2:2]
    margin = jnp.minimum(lengths[source_of] - 1, bound - lengths[receiver]) // 2
    margin = jnp.where((source_of == ranking[0]) | (receiver == ranking[0]) | (lengths[receiver] == 0), 0, jnp.maximum(margin, 0))
    passed = jax.random.randint(jax.random.fold_in(own, 4), (count // 2,), 0, 1 << 20) % (margin + 1)
    lengths = lengths.at[source_of].add(-passed).at[receiver].add(passed)
    items = jnp.searchsorted(jnp.cumsum(lengths), jnp.arange(rows * top), side="right").astype(jnp.int32)
    grid = items.reshape(top, rows).T
    grid = grid[jax.random.permutation(jax.random.fold_in(own, 1), rows)]
    offset_by = jax.random.randint(jax.random.fold_in(own, 2), (rows, 1), 0, top)
    return jnp.take_along_axis(grid, (jnp.arange(top)[None, :] + offset_by) % top, axis=1)


def load_shares(count, total, most, slope, full):
    portions = [(1 << 20) // math.isqrt(rank ** slope) + 1 for rank in range(1, count + 1)]
    largest = most if full else min(most, max(-(-total // count), total * portions[0] // sum(portions)))
    least = 1 if total - largest >= count - 1 else 0
    counts, surplus = [largest] + [least] * (count - 1), total - largest - least * (count - 1)
    while surplus > 0:
        movable = [i for i in range(1, count) if counts[i] < largest] or [i for i in range(1, count) if counts[i] < most]
        mass, remaining = sum([portions[i] for i in movable]), surplus
        for i in movable:
            addition = min(most - counts[i], max(1, remaining * portions[i] // mass), surplus)
            counts[i] = counts[i] + addition
            surplus = surplus - addition
    return np.array(counts)


def bell_draw(key, extent, scale, bound, cuts=(), dtype=jnp.bfloat16):
    array = jax.random.normal(key, extent, jnp.float32) * scale
    if len(cuts) > 0:
        array = levels(key, extent, cuts, -0.22, 0.18) * array
    return jnp.clip(array, min=-bound, max=bound).astype(dtype)


def setup_inputs(seed: int = 0) -> dict:
    key_of = jax.random.split(jax.random.key(seed), 30)
    tokens = draw_tokens(jax.random.fold_in(key_of[29], 71), 0)
    cotangent = bell_draw(key_of[1], (TOKENS, D), 1.0, 6.0, ((0, 32),))
    routes_keys = jax.random.split(jax.random.fold_in(key_of[2], 1), TOKENS // TOK_DEV)
    routes_turns = jax.random.permutation(jax.random.fold_in(key_of[2], 3), TOKENS // TOK_DEV)
    routes = jax.vmap(lambda own, number: routed_block(jax.random.fold_in(key_of[2], 2), own, number, TOK_DEV, EXPERTS, TOP, CAP, 1))(routes_keys, routes_turns).reshape((TOKENS, TOP))
    prefix = touch_ends(jax.random.randint(key_of[3], (SEQS,), 0, TOK_DEV + 1), jax.random.fold_in(key_of[3], 1), 0, TOK_DEV).astype(jnp.int32)
    buckets = touch_ends(jax.random.randint(key_of[4], (2 * TOK_DEV - 1,), 0, BUCKETS), jax.random.fold_in(key_of[4], 1), 0, BUCKETS - 1).astype(jnp.int32)
    step_count = jax.random.randint(key_of[5], (), 1, 21).astype(jnp.int32)
    learn_rate = jnp.clip(jnp.exp(jax.random.uniform(key_of[6], (), jnp.float32, math.log(0.02), math.log(0.1))), 0.02, 0.1)
    weight_decay = jnp.clip(jax.random.uniform(key_of[7], (), jnp.float32, 0.1, 0.5), 0.1, 0.5)
    attend_master = bell_draw(key_of[8], (3, D, D), D ** -0.5, 0.1875, ((1, 32),), jnp.float32)
    attend_first = bell_draw(key_of[9], (3, D, D), 0.11, 0.625, ((1, 32),), jnp.float32)
    attend_second = jnp.clip(jnp.exp(math.log(0.21) - 1.3768156 * jax.random.uniform(key_of[10], (3, D, D), jnp.float32) ** levels(key_of[10], (3, D, D), ((1, 32),), -0.2, 0.2)), 0.053, 0.21)
    outward_master = bell_draw(key_of[11], (D, D), (D * 2 // TOK_DEV) ** -0.5, 2.5, ((0, 32),), jnp.float32)
    outward_first = bell_draw(key_of[12], (D, D), 0.11, 0.625, ((0, 32),), jnp.float32)
    outward_second = jnp.clip(jnp.exp(math.log(0.21) - 1.3768156 * jax.random.uniform(key_of[13], (D, D), jnp.float32) ** levels(key_of[13], (D, D), ((0, 32),), -0.2, 0.2)), 0.053, 0.21)
    router_master = bell_draw(key_of[14], (D, EXPERTS), D ** -0.5, 0.1875, ((0, 32),), jnp.float32)
    router_first = bell_draw(key_of[15], (D, EXPERTS), 0.11, 0.625, ((0, 32),), jnp.float32)
    router_second = jnp.clip(jnp.exp(math.log(0.21) - 1.3768156 * jax.random.uniform(key_of[16], (D, EXPERTS), jnp.float32) ** levels(key_of[16], (D, EXPERTS), ((0, 32),), -0.2, 0.2)), 0.053, 0.21)
    gains_master = jnp.clip(1.0 + 0.1 * jax.random.normal(key_of[17], (2, D), jnp.float32), 0.5, 1.5)
    gains_first = bell_draw(key_of[18], (2, D), 0.11, 0.625, ((1, 32),), jnp.float32)
    gains_second = jnp.clip(jnp.exp(math.log(0.21) - 1.3768156 * jax.random.uniform(key_of[19], (2, D), jnp.float32) ** levels(key_of[19], (2, D), ((1, 32),), -0.2, 0.2)), 0.053, 0.21)
    bias_master = bell_draw(key_of[20], (HEADS * BUCKETS,), 1.0, 6.0, ((0, 32),), jnp.float32)
    bias_first = bell_draw(key_of[21], (HEADS * BUCKETS,), 0.11, 0.625, ((0, 32),), jnp.float32)
    bias_second = jnp.clip(jnp.exp(math.log(0.21) - 1.3768156 * jax.random.uniform(key_of[22], (HEADS * BUCKETS,), jnp.float32) ** levels(key_of[22], (HEADS * BUCKETS,), ((0, 32),), -0.2, 0.2)), 0.053, 0.21)
    upward_master = bell_draw(key_of[23], (2, EXPERTS, D, FF), D ** -0.5, 0.1875, ((1, 4), (2, 8)), jnp.float32)
    upward_first = bell_draw(key_of[24], (2, EXPERTS, D, FF), 0.11, 0.625, ((1, 4), (2, 8)), jnp.float32)
    upward_second = jnp.clip(jnp.exp(math.log(0.21) - 1.3768156 * jax.random.uniform(key_of[25], (2, EXPERTS, D, FF), jnp.float32) ** levels(key_of[25], (2, EXPERTS, D, FF), ((1, 4), (2, 8)), -0.2, 0.2)), 0.053, 0.21)
    downward_master = bell_draw(key_of[26], (EXPERTS, FF, D), FF ** -0.5, 0.109375, ((0, 4), (1, 8)), jnp.float32)
    downward_first = bell_draw(key_of[27], (EXPERTS, FF, D), 0.11, 0.625, ((0, 4), (1, 8)), jnp.float32)
    downward_second = jnp.clip(jnp.exp(math.log(0.21) - 1.3768156 * jax.random.uniform(key_of[28], (EXPERTS, FF, D), jnp.float32) ** levels(key_of[28], (EXPERTS, FF, D), ((0, 4), (1, 8)), -0.2, 0.2)), 0.053, 0.21)
    return dict(tokens=tokens, cotangent=cotangent, routes=routes, prefix=prefix, buckets=buckets, step_count=step_count, learn_rate=learn_rate, weight_decay=weight_decay, attend_master=attend_master, attend_first=attend_first, attend_second=attend_second, outward_master=outward_master, outward_first=outward_first, outward_second=outward_second, router_master=router_master, router_first=router_first, router_second=router_second, gains_master=gains_master, gains_first=gains_first, gains_second=gains_second, bias_master=bias_master, bias_first=bias_first, bias_second=bias_second, upward_master=upward_master, upward_first=upward_first, upward_second=upward_second, downward_master=downward_master, downward_first=downward_first, downward_second=downward_second)


@jax.custom_vjp
def low(v):
    return lax.optimization_barrier(v.astype(jnp.bfloat16)).astype(jnp.float32)

@jax.custom_vjp
def low_back(v):
    return v

def low_keep(v):
    return (low(v), None)

def low_pass(kept, grad):
    return (grad,)

def back_keep(v):
    return (v, None)

def back_low(kept, grad):
    return (low(grad),)
low.defvjp(low_keep, low_pass)
low_back.defvjp(back_keep, back_low)
HIGHEST = lax.Precision.HIGHEST
MASKED = -1e+30

def normed(values, scale_gain):
    return values * lax.rsqrt(lax.optimization_barrier(jnp.mean(values * values, -1, keepdims=True)) + 1e-06) * scale_gain

def adamw_update(master, first_moment, second, gradient, step_float, learn_rate, weight_decay, decayed):
    mean_new = 0.9 * first_moment + 0.1 * gradient
    square_new = 0.95 * second + 0.05 * gradient * gradient
    mean_hat = mean_new / (1.0 - jnp.power(jnp.float32(0.9), step_float))
    square_hat = square_new / (1.0 - jnp.power(jnp.float32(0.95), step_float))
    change = learn_rate * (mean_hat / (jnp.sqrt(square_hat) + 1e-08))
    updated = master - change
    if decayed:
        updated = updated - weight_decay * master
    return (updated, mean_new, square_new, -change)

def group_forward(inputs, route_ids, prefix_len, weights, buckets):
    attend_w, outward_w, router_w, gains_w, bias_w, upward_w, downward_w = weights
    groups_here = inputs.shape[0]
    seqlen = inputs.shape[1]
    hidden_one = low(normed(inputs, gains_w[0]))
    projected = [low_back(low(jnp.einsum('gsd,de->gse', hidden_one, attend_w[member], precision=HIGHEST))) for member in range(3)]
    heads_shape = (groups_here, seqlen, HEADS, HEAD_DIM)
    query_heads = projected[0].reshape(heads_shape)
    key_heads = projected[1].reshape(heads_shape)
    value_heads = projected[2].reshape(heads_shape)
    positions = jnp.arange(seqlen).astype(jnp.int32)
    offsets = positions[None, :] - positions[:, None] + (seqlen - 1)
    table = bias_w.reshape(HEADS, BUCKETS)
    bias_full = table[:, buckets[offsets]]
    allowed = (positions[None, None, :] <= positions[None, :, None]) | (positions[None, None, :] < prefix_len[:, None, None])
    raw = low_back(jnp.einsum('gqhd,gkhd->ghqk', query_heads, key_heads, precision=HIGHEST) * 0.125 + bias_full[None])
    scores = jnp.where(allowed[:, None], raw, MASKED)
    soft_scores = low(jax.nn.softmax(scores, axis=-1))
    attended = low(low_back(jnp.einsum('ghqk,gkhd->gqhd', soft_scores, value_heads, precision=HIGHEST)))
    attended = attended.reshape(groups_here, seqlen, D)
    residual = inputs + low_back(jnp.einsum('gsd,de->gse', attended, outward_w, precision=HIGHEST))
    second_normed = normed(residual, gains_w[1])
    logits = jnp.einsum('gsd,de->gse', second_normed, router_w, precision=HIGHEST)
    router_soft = jax.nn.softmax(logits, axis=-1)
    route_hits = (route_ids[..., None] == jnp.arange(EXPERTS).astype(jnp.int32)).astype(jnp.float32)
    chosen = lax.optimization_barrier(jnp.sum(router_soft[:, :, None, :] * route_hits, -1))
    combine = chosen / lax.optimization_barrier(jnp.sum(chosen, -1, keepdims=True))
    per_expert = lax.optimization_barrier(jnp.sum(combine[..., None] * route_hits, 2))
    dispatched = low(second_normed)
    expert_sum = jnp.zeros_like(residual)
    for expert_id in range(EXPERTS):
        arrived = low_back(dispatched)
        gate_value = low_back(jnp.einsum('gsd,df->gsf', arrived, upward_w[0, expert_id], precision=HIGHEST))
        up_value = low_back(jnp.einsum('gsd,df->gsf', arrived, upward_w[1, expert_id], precision=HIGHEST))
        hidden_mid = low(jax.nn.gelu(gate_value, approximate=True) * up_value)
        expert_out = low_back(low(jnp.einsum('gsf,fd->gsd', hidden_mid, downward_w[expert_id], precision=HIGHEST)))
        expert_sum = expert_sum + per_expert[..., expert_id:expert_id + 1] * expert_out
    return residual + expert_sum

def reference(tokens, cotangent, routes, prefix, buckets, step_count, learn_rate, weight_decay, attend_master, attend_first, attend_second, outward_master, outward_first, outward_second, router_master, router_first, router_second, gains_master, gains_first, gains_second, bias_master, bias_first, bias_second, upward_master, upward_first, upward_second, downward_master, downward_first, downward_second):
    masters = (attend_master, outward_master, router_master, gains_master, bias_master, upward_master, downward_master)
    firsts = (attend_first, outward_first, router_first, gains_first, bias_first, upward_first, downward_first)
    seconds = (attend_second, outward_second, router_second, gains_second, bias_second, upward_second, downward_second)
    weights = (low(attend_master), low(outward_master), router_master, gains_master, bias_master, low(upward_master), low(downward_master))
    per_group = 1
    while per_group * 2 * TOK_DEV <= 4096 and SEQS % (per_group * 2) == 0:
        per_group = per_group * 2
    group_count = SEQS // per_group
    inputs = tokens.astype(jnp.float32).reshape(group_count, per_group, TOK_DEV, D)
    route_groups = routes.reshape(group_count, per_group, TOK_DEV, TOP)
    prefix_groups = prefix.reshape(group_count, per_group)

    def whole(inputs_all, weights_all):

        def one_group(pieces):
            return group_forward(pieces[0], pieces[1], pieces[2], weights_all, buckets)
        return lax.map(jax.checkpoint(one_group), (inputs_all, route_groups, prefix_groups))
    outputs, pullback = jax.vjp(whole, inputs, weights)
    input_cot, weight_grads = pullback(cotangent.astype(jnp.float32).reshape(outputs.shape))
    step_float = step_count.astype(jnp.float32)
    flags = (True, True, True, False, False, True, True)
    mean_squares = [jnp.mean(member_grad * member_grad) for member_grad in weight_grads]
    scaled = [weight_grads[member] * lax.rsqrt(mean_squares[member] + 1e-06) for member in range(7)]
    updates = [adamw_update(masters[member], firsts[member], seconds[member], scaled[member], step_float, learn_rate, weight_decay, flags[member]) for member in range(7)]
    grad_rms = jnp.stack([jnp.sqrt(value) for value in mean_squares])
    return (outputs.reshape(TOKENS, D).astype(jnp.bfloat16), input_cot.reshape(TOKENS, D).astype(jnp.bfloat16), weight_grads[0], updates[0][0], updates[0][1], updates[0][2], weight_grads[1], updates[1][0], updates[1][1], updates[1][2], weight_grads[2], updates[2][0], updates[2][1], updates[2][2], weight_grads[3], updates[3][3], updates[3][1], updates[3][2], weight_grads[4], updates[4][3], updates[4][1], updates[4][2], weight_grads[5], updates[5][0], updates[5][1], updates[5][2], weight_grads[6], updates[6][0], updates[6][1], updates[6][2], grad_rms)
```

```python
import functools

import jax
import jax.numpy as jnp
from jax import lax
from jax.experimental import pallas as pl
from jax.experimental.pallas import tpu as pltpu
from jax.sharding import PartitionSpec as P

D = 1024
HEADS = 16
HEAD_DIM = 64
FF = 2816
BUCKETS = 32
TOP = 2
BOTH = ("dp", "expert")
BF = jnp.bfloat16
F32 = jnp.float32

HIGHEST = lax.Precision.HIGHEST
MASKED = -1e30


def normed(values, scale_gain):
    return values * lax.rsqrt(jnp.mean(values * values, -1, keepdims=True) + 1e-06) * scale_gain


def gelu_tanh(values):
    return jax.nn.gelu(values, approximate=True)


def adamw_update(
    master, first_moment, second, gradient, step_float, learn_rate, weight_decay, decayed
):
    mean_new = 0.9 * first_moment + 0.1 * gradient
    square_new = 0.95 * second + 0.05 * gradient * gradient
    mean_hat = mean_new / (1.0 - jnp.power(jnp.float32(0.9), step_float))
    square_hat = square_new / (1.0 - jnp.power(jnp.float32(0.95), step_float))
    change = learn_rate * (mean_hat / (jnp.sqrt(square_hat) + 1e-08))
    updated = master - change
    if decayed:
        updated = updated - weight_decay * master
    return (updated, mean_new, square_new, -change)


def is_line():
    return lax.axis_size("dp") == 8 and lax.axis_size("expert") == 4


def spot():
    index = lax.axis_index("dp")
    return index // 2, index % 2


def along(array, moves):
    pairs = [(2 * a + x, 2 * b + x) for a, b in moves for x in range(2)]
    return lax.ppermute(array, "dp", pairs)


def across(array, rows=(0, 1, 2, 3)):
    pairs = [(2 * z + x, 2 * z + 1 - x) for z in rows for x in range(2)]
    return lax.ppermute(array, "dp", pairs)


RIGHT = ((0, 1), (1, 2), (2, 3))
LEFT = ((1, 0), (2, 1), (3, 2))


def gather_line(shard):
    z, x = spot()
    right1, left1 = along(shard, RIGHT), along(shard, LEFT)
    over0 = across(shard)
    over_right1, over_left1 = across(right1, (1, 2, 3)), across(left1, (0, 1, 2))
    right2, left2 = along(right1, ((1, 2), (2, 3))), along(left1, ((1, 0), (2, 1)))
    second = jnp.where(z >= 2, right2, left2)
    over_second = across(second)
    third = along(second, ((2, 3), (1, 0)))
    over_third = across(third, (0, 3))
    full = jnp.zeros((8,) + shard.shape, shard.dtype)

    def put(full, piece, row, column):
        return lax.dynamic_update_slice(full, piece[None], (2 * row + column, 0, 0))

    for piece0, right, left, two, three, column in (
        (shard, right1, left1, second, third, x),
        (over0, over_right1, over_left1, over_second, over_third, 1 - x),
    ):
        full = put(full, piece0, z, column)
        full = put(full, jnp.where(z == 0, three, right), (z + 3) % 4, column)
        full = put(full, jnp.where(z == 3, three, left), (z + 1) % 4, column)
        full = put(full, two, (z + 2) % 4, column)
    return full


def scatter_line(parts):
    z, x = spot()

    def pick(row, column):
        return lax.dynamic_slice(parts, (2 * row + column, 0, 0), (1,) + parts.shape[1:])[0]

    def total(*terms):
        return functools.reduce(jnp.add, [term.astype(F32) for term in terms])

    other = 1 - x
    far, two = jnp.where(z == 0, 3, 0), (z + 2) % 4
    up, down = jnp.minimum(z + 1, 3), jnp.maximum(z - 1, 0)
    over_far = across(pick(far, other), (0, 3))
    over_two = across(pick(two, other))
    over_up = across(pick(up, other), (0, 1, 2))
    over_down = across(pick(down, other), (1, 2, 3))
    over_own = across(pick(z, other))
    first = along(total(pick(far, x), over_far).astype(BF), ((0, 1), (3, 2)))
    sum_two = total(pick(two, x), over_two, first).astype(BF)
    right2 = along(sum_two, ((0, 1), (1, 2)))
    left2 = along(sum_two, ((3, 2), (2, 1)))
    right3 = along(total(pick(up, x), over_up, right2).astype(BF), RIGHT)
    left3 = along(total(pick(down, x), over_down, left2).astype(BF), LEFT)
    return total(pick(z, x), over_own, right3, left3)


def gather_dp(shard):
    if is_line():
        return gather_line(shard)
    return lax.all_gather(shard, "dp", axis=0)


def scatter_dp(parts):
    if is_line():
        return scatter_line(parts)
    return lax.psum_scatter(parts.astype(F32), "dp", scatter_dimension=0, tiled=False)


def swap_expert(array, bit):
    return lax.ppermute(array, "expert", [(e, e ^ bit) for e in range(4)])


def scatter_all(parts):
    if not is_line():
        return lax.psum_scatter(parts.astype(F32), BOTH, scatter_dimension=0, tiled=False)
    expert = lax.axis_index("expert")
    y, core = expert // 2, expert % 2
    shape = parts.shape[1:]
    parts = parts.reshape((8, 2, 2) + shape)

    def half(array, axis, index):
        return lax.dynamic_index_in_dim(array, index, axis, keepdims=False)

    mine = half(parts, 2, core).astype(F32) + swap_expert(half(parts, 2, 1 - core), 1).astype(F32)
    mine = mine.astype(BF)
    mine = half(mine, 1, y).astype(F32) + swap_expert(half(mine, 1, 1 - y), 2).astype(F32)
    return scatter_line(mine.astype(BF))


def sum_all(array):
    if not is_line():
        return lax.psum(array, BOTH)
    for bit in (1, 2):
        array = array + swap_expert(array, bit)
    for bit in (1, 2, 4):
        array = array + lax.ppermute(array, "dp", [(d, d ^ bit) for d in range(8)])
    return array


def bias_rows(table, seqlen):
    width = table.shape[-1]
    wide = jnp.broadcast_to(table, (128, width))
    return pltpu.roll(wide, width - 127, 1, stride=1, stride_axis=0)


def probabilities(query, key, rows, prefix, block, seqlen):
    blocks = seqlen // 128
    raw = (
        lax.dot_general(query, key, (((1,), (1,)), ((), ())), preferred_element_type=F32) * 0.125
    )
    start = 128 * (blocks - 1 - block)
    raw = raw + rows[:, start : start + seqlen]
    i = lax.broadcasted_iota(jnp.int32, raw.shape, 0) + 128 * block
    j = lax.broadcasted_iota(jnp.int32, raw.shape, 1)
    raw = jnp.where((j <= i) | (j < prefix), raw, MASKED)
    shifted = jnp.exp(raw - jnp.max(raw, -1, keepdims=True))
    return shifted / jnp.sum(shifted, -1, keepdims=True)


def attend_kernel(prefix_ref, table_ref, query_ref, key_ref, value_ref, out_ref):
    seqlen = query_ref.shape[0]
    prefix = prefix_ref[0]
    for head in range(2):
        lanes = slice(head * HEAD_DIM, (head + 1) * HEAD_DIM)
        rows = bias_rows(table_ref[0, head : head + 1, :], seqlen)
        key, value = key_ref[:, lanes], value_ref[:, lanes]
        for block in range(seqlen // 128):
            at = slice(128 * block, 128 * (block + 1))
            probs = probabilities(query_ref[at, lanes], key, rows, prefix, block, seqlen)
            out = jnp.dot(probs.astype(BF), value, preferred_element_type=F32)
            out_ref[at, lanes] = out.astype(BF)


def attend_back_kernel(
    prefix_ref,
    table_ref,
    query_ref,
    key_ref,
    value_ref,
    upstream_ref,
    query_grad_ref,
    key_grad_ref,
    value_grad_ref,
    bias_ref,
):
    seqlen = query_ref.shape[0]
    blocks = seqlen // 128
    prefix = prefix_ref[0]
    flip = (((0,), (0,)), ((), ()))
    for head in range(2):
        lanes = slice(head * HEAD_DIM, (head + 1) * HEAD_DIM)
        rows = bias_rows(table_ref[0, head : head + 1, :], seqlen)
        query, key, value = query_ref[:, lanes], key_ref[:, lanes], value_ref[:, lanes]
        upstream = upstream_ref[:, lanes]
        probs_low, scores_low, scores = [], [], []
        for block in range(blocks):
            at = slice(128 * block, 128 * (block + 1))
            probs = probabilities(query[at], key, rows, prefix, block, seqlen)
            probs_grad = lax.dot_general(
                upstream[at], value, (((1,), (1,)), ((), ())), preferred_element_type=F32
            )
            inner = jnp.sum(probs * probs_grad, -1, keepdims=True)
            low = (probs * (probs_grad - inner)).astype(BF)
            probs_low.append(probs.astype(BF))
            scores_low.append(low)
            scores.append(low.astype(F32))
            out = jnp.dot(low, key, preferred_element_type=F32) * 0.125
            query_grad_ref[at, lanes] = out.astype(BF)
        probs_all = jnp.concatenate(probs_low, 0)
        scores_all = jnp.concatenate(scores_low, 0)
        out = lax.dot_general(probs_all, upstream, flip, preferred_element_type=F32)
        value_grad_ref[:, lanes] = out.astype(BF)
        out = lax.dot_general(scores_all, query, flip, preferred_element_type=F32) * 0.125
        key_grad_ref[:, lanes] = out.astype(BF)
        columns = []
        for column in range(2 * blocks - 1):
            terms = []
            for block in range(blocks):
                piece = column - (blocks - 1 - block)
                if 0 <= piece < blocks:
                    terms.append(scores[block][:, 128 * piece : 128 * (piece + 1)])
            columns.append(functools.reduce(jnp.add, terms))
        columns.append(jnp.zeros_like(columns[0]))
        wide = jnp.concatenate(columns, 1)
        total = jnp.zeros((8, wide.shape[1]), F32)
        for group in range(16):
            total = total + pltpu.roll(wide[8 * group : 8 * group + 8], 127 - 8 * group, 1)
        bias_ref[0, head] = total


def attention_specs(seqlen, width):
    pairs = HEADS // 2
    table = pl.BlockSpec((1, 2, width), lambda p: (p, 0, 0))
    return (
        [pl.BlockSpec(memory_space=pltpu.SMEM), table]
        + [
            pl.BlockSpec((seqlen, 128), lambda p, part=part: (0, part * pairs + p))
            for part in range(3)
        ],
        pl.BlockSpec((seqlen, 128), lambda p: (0, p)),
    )


def attend(prefix, table, projected):
    seqlen = projected.shape[0]
    ins, out = attention_specs(seqlen, table.shape[-1])
    return pl.pallas_call(
        attend_kernel,
        grid=(HEADS // 2,),
        in_specs=ins,
        out_specs=out,
        out_shape=jax.ShapeDtypeStruct((seqlen, D), BF),
        cost_estimate=pl.CostEstimate(
            flops=4 * seqlen * seqlen * D,
            bytes_accessed=8 * seqlen * D,
            transcendentals=HEADS * seqlen * seqlen,
        ),
        name="attend",
    )(prefix, table, projected, projected, projected)


def attend_back(prefix, table, projected, upstream):
    seqlen = projected.shape[0]
    width = table.shape[-1]
    ins, out = attention_specs(seqlen, width)
    grad = jax.ShapeDtypeStruct((seqlen, D), BF)
    return pl.pallas_call(
        attend_back_kernel,
        grid=(HEADS // 2,),
        in_specs=ins + [out],
        out_specs=[out, out, out, pl.BlockSpec((1, 2, 8, width), lambda p: (p, 0, 0, 0))],
        out_shape=[grad, grad, grad, jax.ShapeDtypeStruct((HEADS // 2, 2, 8, width), F32)],
        cost_estimate=pl.CostEstimate(
            flops=10 * seqlen * seqlen * D,
            bytes_accessed=14 * seqlen * D,
            transcendentals=HEADS * seqlen * seqlen,
        ),
        name="attend_back",
    )(prefix, table, projected, projected, projected, upstream)


def split_three(values):
    high = lax.reduce_precision(values, 8, 7)
    middle = lax.reduce_precision(values - high, 8, 7)
    low = lax.reduce_precision(values - high - middle, 8, 7)
    return jnp.concatenate([high, middle, low]).astype(BF)


def on_device(
    tokens,
    cotangent,
    routes,
    prefix,
    buckets,
    step_count,
    learn_rate,
    weight_decay,
    attend_master,
    attend_first,
    attend_second,
    outward_master,
    outward_first,
    outward_second,
    router_master,
    router_first,
    router_second,
    gains_master,
    gains_first,
    gains_second,
    bias_master,
    bias_first,
    bias_second,
    upward_master,
    upward_first,
    upward_second,
    downward_master,
    downward_first,
    downward_second,
):
    devices = lax.axis_size(BOTH)
    share = attend_master.shape[1]
    seqlen = tokens.shape[0]
    experts = router_master.shape[1]
    capacity = seqlen * TOP * 5 // (4 * experts)

    slices = lax.axis_size("dp")
    upward_w = gather_dp(upward_master.astype(BF).reshape(2 * D // slices, FF))
    upward_w = upward_w.reshape(slices, 2, D // slices, FF)
    gate_w, up_w = upward_w[:, 0].reshape(D, FF), upward_w[:, 1].reshape(D, FF)
    downward_w = gather_dp(downward_master[0].astype(BF)).reshape(FF, D)

    small = split_three(
        jnp.concatenate(
            [router_master.reshape(-1), gains_master.reshape(-1), bias_master.reshape(-1)]
        )
    )
    count = small.shape[0]
    extra = -(-count // (16 * D)) * 16
    small = jnp.pad(small, (0, extra * D - count)).reshape(extra, D)
    sent = jnp.concatenate([attend_master.astype(BF).reshape(3 * share, D), small], 0)
    got = lax.all_gather(sent, BOTH, axis=0)
    outward_w = lax.all_gather(outward_master.astype(BF), BOTH, axis=0, tiled=True)
    attend_w = got[:, : 3 * share].reshape(devices, 3, share, D).transpose(1, 0, 2, 3)
    attend_w = attend_w.reshape(3, D, D)
    small = got[:, 3 * share :].reshape(devices, extra * D)[:, :count].astype(F32)
    small = small.reshape(devices, 3, count // 3).sum(1)
    router_size, gains_size = router_master.size, gains_master.size
    router_w = small[:, :router_size].reshape(D, experts)
    gains_w = small[:, router_size : router_size + gains_size].reshape(devices, 2, share)
    gains_w = gains_w.transpose(1, 0, 2).reshape(2, D)
    bias_w = small[:, router_size + gains_size :].reshape(-1)

    bucket_hits = (buckets[:, None] == jnp.arange(BUCKETS, dtype=jnp.int32)[None, :]).astype(F32)
    offsets = buckets.shape[0]
    table = jnp.dot(bias_w.reshape(HEADS, BUCKETS), bucket_hits.T, precision=HIGHEST)
    table = jnp.pad(table, ((0, 0), (0, 2 * seqlen - offsets))).reshape(HEADS // 2, 2, 2 * seqlen)

    inputs = tokens.astype(F32)
    first_normed, first_pull = jax.vjp(normed, inputs, gains_w[0])
    hidden_one = first_normed.astype(BF)
    projected = jnp.concatenate(
        [
            jnp.dot(hidden_one, attend_w[part], preferred_element_type=F32).astype(BF)
            for part in range(3)
        ],
        1,
    )
    attended = attend(prefix, table, projected)
    residual = inputs + jnp.dot(attended, outward_w, preferred_element_type=F32)

    kinds = jnp.arange(experts, dtype=jnp.int32)
    route_hits = (routes[:, :, None] == kinds[None, None, :]).astype(F32)

    def gate_piece(residual_in, scale_gain, router_in):
        second_normed = normed(residual_in, scale_gain)
        logits = jnp.dot(second_normed, router_in, precision=HIGHEST)
        router_soft = jax.nn.softmax(logits, axis=-1)
        chosen = jnp.sum(router_soft[:, None, :] * route_hits, -1)
        return (second_normed, chosen / jnp.sum(chosen, -1, keepdims=True))

    (second_normed, combine), gate_pull = jax.vjp(gate_piece, residual, gains_w[1], router_w)
    second_low = second_normed.astype(BF)

    hits = jnp.sum(route_hits, 1)
    places = jnp.arange(seqlen, dtype=jnp.int32)
    earlier = (places[None, :] < places[:, None]).astype(BF)
    rank = jnp.dot(earlier, hits.astype(BF), preferred_element_type=F32)
    rank = jnp.where(hits > 0, rank, -1.0).astype(jnp.int32)
    slots = jnp.arange(capacity, dtype=jnp.int32)
    taken = rank.T[:, None, :] == slots[None, :, None]
    choose = taken.astype(BF).reshape(experts * capacity, seqlen)
    weight = jnp.sum(combine[:, :, None] * route_hits, 1)
    slot_weight = jnp.sum(jnp.where(taken, weight.T[:, None, :], 0.0), -1)
    backs = [
        (
            (rank[:, :, None] == slots[None, None, :])
            & (routes[:, k][:, None, None] == kinds[None, :, None])
        )
        .astype(BF)
        .reshape(seqlen, experts * capacity)
        for k in range(TOP)
    ]
    back = (rank[:, :, None] == slots[None, None, :]).astype(BF)
    back = back.reshape(seqlen, experts * capacity)

    def exchange(rows, home):
        if home:
            rows = rows.reshape(1, experts, capacity, D)
            rows = lax.all_to_all(rows, "expert", split_axis=1, concat_axis=0, tiled=True)
        else:
            rows = rows.reshape(experts, 1, capacity, D)
            rows = lax.all_to_all(rows, "expert", split_axis=0, concat_axis=1, tiled=True)
        return rows.reshape(experts * capacity, D)

    sent_rows = jnp.dot(choose, second_low, preferred_element_type=F32).astype(BF)
    arrived = exchange(sent_rows, False)
    upstream_rows = jnp.dot(choose, cotangent, preferred_element_type=F32)
    grad_rows = (slot_weight.reshape(-1, 1) * upstream_rows).astype(BF)
    grad_arrived = exchange(grad_rows, False)

    gate_value = jnp.dot(arrived, gate_w, preferred_element_type=F32)
    up_value = jnp.dot(arrived, up_w, preferred_element_type=F32)
    gelu_value, gelu_pull = jax.vjp(gelu_tanh, gate_value)
    hidden_mid = (gelu_value * up_value).astype(BF)
    expert_out = jnp.dot(hidden_mid, downward_w, preferred_element_type=F32).astype(BF)
    returned = exchange(expert_out, True)

    turned = (((1,), (1,)), ((), ()))
    flipped = (((0,), (0,)), ((), ()))
    grad_mid = lax.dot_general(grad_arrived, downward_w, turned, preferred_element_type=F32)
    grad_gate = gelu_pull(grad_mid * up_value)[0].astype(BF)
    grad_up = (grad_mid * gelu_value).astype(BF)
    grad_sent = lax.dot_general(grad_gate, gate_w, turned, preferred_element_type=F32)
    grad_sent = grad_sent + lax.dot_general(grad_up, up_w, turned, preferred_element_type=F32)
    grad_home = exchange(grad_sent.astype(BF), True)


    def weight_grad(left, right):
        full = lax.dot_general(left, right, flipped, preferred_element_type=F32).astype(BF)
        return full.reshape(slices, -1, full.shape[1])

    downward_g = scatter_dp(weight_grad(hidden_mid, grad_arrived))[None]
    upward_g = scatter_dp(
        jnp.concatenate([weight_grad(arrived, grad_gate), weight_grad(arrived, grad_up)], 1)
    ).reshape(2, 1, D // slices, FF)

    came_back = jnp.stack(
        [jnp.dot(one, returned, preferred_element_type=F32) for one in backs], 1
    )
    expert_sum = jnp.sum(combine[..., None] * came_back, 1)
    block_output = (residual + expert_sum).astype(BF)
    upstream = cotangent.astype(F32)
    combine_grad = jnp.sum(upstream[:, None, :] * came_back, -1)

    grad_normed = jnp.dot(back, grad_home, preferred_element_type=F32)
    residual_part, gain_two_grad, router_full = gate_pull((grad_normed, combine_grad))
    grad_residual = upstream + residual_part
    grad_branch = grad_residual.astype(BF)
    outward_full = lax.dot_general(attended, grad_branch, flipped, preferred_element_type=F32)
    outward_g = scatter_all(outward_full.astype(BF).reshape(devices, share, D))
    grad_attended = lax.dot_general(grad_branch, outward_w, turned, preferred_element_type=F32)
    query_grad, key_grad, value_grad, bias_parts = attend_back(
        prefix, table, projected, grad_attended.astype(BF)
    )
    projected_grads = (query_grad, key_grad, value_grad)
    attend_g = scatter_all(
        jnp.concatenate(
            [
                lax.dot_general(hidden_one, part, flipped, preferred_element_type=F32)
                .astype(BF)
                .reshape(devices, share, D)
                for part in projected_grads
            ],
            1,
        )
    ).reshape(3, share, D)
    grad_hidden_one = functools.reduce(
        jnp.add,
        [
            lax.dot_general(part, attend_w[which], turned, preferred_element_type=F32)
            for which, part in enumerate(projected_grads)
        ],
    )
    inputs_part, gain_one_grad = first_pull(grad_hidden_one)
    input_grad = (grad_residual + inputs_part).astype(BF)

    bias_parts = bias_parts.reshape(HEADS, 8, 2 * seqlen)
    bias_parts = jnp.pad(bias_parts, ((0, 0), (0, 0), (0, 8)))
    per_offset = functools.reduce(
        jnp.add, [bias_parts[:, row, row : row + offsets] for row in range(8)]
    )
    bias_full = jnp.dot(per_offset, bucket_hits, precision=HIGHEST).reshape(-1)

    smalls = sum_all(
        jnp.concatenate([router_full.reshape(-1), gain_one_grad, gain_two_grad, bias_full])
    )
    place = lax.axis_index(BOTH)
    router_g = lax.dynamic_slice(smalls, (place * router_size,), (router_size,))
    router_g = router_g.reshape(share, experts)
    start = D * experts
    gains_g = jnp.stack(
        [
            lax.dynamic_slice(smalls, (start + row * D + place * share,), (share,))
            for row in range(2)
        ]
    )
    bias_g = lax.dynamic_slice(smalls, (start + 2 * D + place * bias_master.size,), bias_master.shape)

    grads_all = (attend_g, outward_g, router_g, gains_g, bias_g, upward_g, downward_g)
    squares = jnp.stack([jnp.sum(member_grad * member_grad) for member_grad in grads_all])
    totals = sum_all(squares)
    counts_all = jnp.array(
        [
            3 * D * D,
            D * D,
            D * experts,
            2 * D,
            HEADS * BUCKETS,
            2 * experts * D * FF,
            experts * FF * D,
        ],
        jnp.float32,
    )
    mean_squares = totals / counts_all
    grad_rms = jnp.sqrt(mean_squares)
    factors = lax.rsqrt(mean_squares + 1e-06)
    step_float = step_count.astype(jnp.float32)
    masters = (
        attend_master,
        outward_master,
        router_master,
        gains_master,
        bias_master,
        upward_master,
        downward_master,
    )
    firsts = (
        attend_first,
        outward_first,
        router_first,
        gains_first,
        bias_first,
        upward_first,
        downward_first,
    )
    seconds = (
        attend_second,
        outward_second,
        router_second,
        gains_second,
        bias_second,
        upward_second,
        downward_second,
    )
    flags = (True, True, True, False, False, True, True)
    updates = [
        adamw_update(
            masters[member],
            firsts[member],
            seconds[member],
            grads_all[member] * factors[member],
            step_float,
            learn_rate,
            weight_decay,
            flags[member],
        )
        for member in range(7)
    ]
    return (
        block_output,
        input_grad,
        grads_all[0],
        updates[0][0],
        updates[0][1],
        updates[0][2],
        grads_all[1],
        updates[1][0],
        updates[1][1],
        updates[1][2],
        grads_all[2],
        updates[2][0],
        updates[2][1],
        updates[2][2],
        grads_all[3],
        updates[3][3],
        updates[3][1],
        updates[3][2],
        grads_all[4],
        updates[4][3],
        updates[4][1],
        updates[4][2],
        grads_all[5],
        updates[5][0],
        updates[5][1],
        updates[5][2],
        grads_all[6],
        updates[6][0],
        updates[6][1],
        updates[6][2],
        grad_rms,
    )


def solution(mesh):
    placed = (
        P(("dp", "expert"), None),
        P(("dp", "expert"), None),
        P(("dp", "expert"), None),
        P(("dp", "expert")),
        P(),
        P(),
        P(),
        P(),
        P(None, ("dp", "expert"), None),
        P(None, ("dp", "expert"), None),
        P(None, ("dp", "expert"), None),
        P(("dp", "expert"), None),
        P(("dp", "expert"), None),
        P(("dp", "expert"), None),
        P(("dp", "expert"), None),
        P(("dp", "expert"), None),
        P(("dp", "expert"), None),
        P(None, ("dp", "expert")),
        P(None, ("dp", "expert")),
        P(None, ("dp", "expert")),
        P(("dp", "expert")),
        P(("dp", "expert")),
        P(("dp", "expert")),
        P(None, "expert", "dp", None),
        P(None, "expert", "dp", None),
        P(None, "expert", "dp", None),
        P("expert", "dp", None),
        P("expert", "dp", None),
        P("expert", "dp", None),
    )
    return jax.shard_map(
        on_device,
        mesh=mesh,
        in_specs=placed,
        out_specs=(
            P(("dp", "expert"), None),
            P(("dp", "expert"), None),
            P(None, ("dp", "expert"), None),
            P(None, ("dp", "expert"), None),
            P(None, ("dp", "expert"), None),
            P(None, ("dp", "expert"), None),
            P(("dp", "expert"), None),
            P(("dp", "expert"), None),
            P(("dp", "expert"), None),
            P(("dp", "expert"), None),
            P(("dp", "expert"), None),
            P(("dp", "expert"), None),
            P(("dp", "expert"), None),
            P(("dp", "expert"), None),
            P(None, ("dp", "expert")),
            P(None, ("dp", "expert")),
            P(None, ("dp", "expert")),
            P(None, ("dp", "expert")),
            P(("dp", "expert")),
            P(("dp", "expert")),
            P(("dp", "expert")),
            P(("dp", "expert")),
            P(None, "expert", "dp", None),
            P(None, "expert", "dp", None),
            P(None, "expert", "dp", None),
            P(None, "expert", "dp", None),
            P("expert", "dp", None),
            P("expert", "dp", None),
            P("expert", "dp", None),
            P("expert", "dp", None),
            P(),
        ),
        check_vma=False,
    )
```

```python
import functools

import jax
import jax.numpy as jnp
from jax import lax
from jax.experimental import pallas as pl
from jax.experimental.pallas import tpu as pltpu
from jax.sharding import PartitionSpec as P

D = 1024
HEADS = 16
HEAD_DIM = 64
FF = 2816
BUCKETS = 32
TOP = 2
BOTH = ("dp", "expert")
BF = jnp.bfloat16
F32 = jnp.float32

HIGHEST = lax.Precision.HIGHEST
MASKED = -1e30


def normed(values, scale_gain):
    return values * lax.rsqrt(jnp.mean(values * values, -1, keepdims=True) + 1e-06) * scale_gain


def gelu_tanh(values):
    return jax.nn.gelu(values, approximate=True)


def adamw_update(
    master, first_moment, second, gradient, step_float, learn_rate, weight_decay, decayed
):
    mean_new = 0.9 * first_moment + 0.1 * gradient
    square_new = 0.95 * second + 0.05 * gradient * gradient
    mean_hat = mean_new / (1.0 - jnp.power(jnp.float32(0.9), step_float))
    square_hat = square_new / (1.0 - jnp.power(jnp.float32(0.95), step_float))
    change = learn_rate * (mean_hat / (jnp.sqrt(square_hat) + 1e-08))
    updated = master - change
    if decayed:
        updated = updated - weight_decay * master
    return (updated, mean_new, square_new, -change)


def is_line():
    return lax.axis_size("dp") == 8 and lax.axis_size("expert") == 4


def spot():
    index = lax.axis_index("dp")
    return index // 2, index % 2


def along(array, moves):
    pairs = [(2 * a + x, 2 * b + x) for a, b in moves for x in range(2)]
    return lax.ppermute(array, "dp", pairs)


def across(array, rows=(0, 1, 2, 3)):
    pairs = [(2 * z + x, 2 * z + 1 - x) for z in rows for x in range(2)]
    return lax.ppermute(array, "dp", pairs)


RIGHT = ((0, 1), (1, 2), (2, 3))
LEFT = ((1, 0), (2, 1), (3, 2))


def scatter_line(parts):
    z, x = spot()

    def pick(row, column):
        return lax.dynamic_slice(parts, (2 * row + column, 0, 0), (1,) + parts.shape[1:])[0]

    def total(*terms):
        return functools.reduce(jnp.add, [term.astype(F32) for term in terms])

    other = 1 - x
    far, two = jnp.where(z == 0, 3, 0), (z + 2) % 4
    up, down = jnp.minimum(z + 1, 3), jnp.maximum(z - 1, 0)
    over_far = across(pick(far, other), (0, 3))
    over_two = across(pick(two, other))
    over_up = across(pick(up, other), (0, 1, 2))
    over_down = across(pick(down, other), (1, 2, 3))
    over_own = across(pick(z, other))
    first = along(total(pick(far, x), over_far).astype(BF), ((0, 1), (3, 2)))
    sum_two = total(pick(two, x), over_two, first).astype(BF)
    right2 = along(sum_two, ((0, 1), (1, 2)))
    left2 = along(sum_two, ((3, 2), (2, 1)))
    right3 = along(total(pick(up, x), over_up, right2).astype(BF), RIGHT)
    left3 = along(total(pick(down, x), over_down, left2).astype(BF), LEFT)
    return total(pick(z, x), over_own, right3, left3)


def gather_dp(shard):
    return lax.all_gather(shard, "dp", axis=0)


def scatter_dp(parts):
    if is_line():
        return scatter_line(parts)
    return lax.psum_scatter(parts.astype(F32), "dp", scatter_dimension=0, tiled=False)


def swap_expert(array, bit):
    return lax.ppermute(array, "expert", [(e, e ^ bit) for e in range(4)])


def scatter_all(parts):
    if not is_line():
        return lax.psum_scatter(parts.astype(F32), BOTH, scatter_dimension=0, tiled=False)
    expert = lax.axis_index("expert")
    y, core = expert // 2, expert % 2
    shape = parts.shape[1:]
    parts = parts.reshape((8, 2, 2) + shape)

    def half(array, axis, index):
        return lax.dynamic_index_in_dim(array, index, axis, keepdims=False)

    mine = half(parts, 2, core).astype(F32) + swap_expert(half(parts, 2, 1 - core), 1).astype(F32)
    mine = mine.astype(BF)
    mine = half(mine, 1, y).astype(F32) + swap_expert(half(mine, 1, 1 - y), 2).astype(F32)
    return scatter_line(mine.astype(BF))


def sum_all(array):
    if not is_line():
        return lax.psum(array, BOTH)
    for bit in (1, 2):
        array = array + swap_expert(array, bit)
    for bit in (1, 2, 4):
        array = array + lax.ppermute(array, "dp", [(d, d ^ bit) for d in range(8)])
    return array


def bias_rows(table, seqlen):
    width = table.shape[-1]
    wide = jnp.broadcast_to(table, (128, width))
    return pltpu.roll(wide, width - 127, 1, stride=1, stride_axis=0)


def probabilities(query, key, rows, prefix, block, seqlen):
    blocks = seqlen // 128
    raw = (
        lax.dot_general(query, key, (((1,), (1,)), ((), ())), preferred_element_type=F32) * 0.125
    )
    start = 128 * (blocks - 1 - block)
    raw = raw + rows[:, start : start + seqlen]
    i = lax.broadcasted_iota(jnp.int32, raw.shape, 0) + 128 * block
    j = lax.broadcasted_iota(jnp.int32, raw.shape, 1)
    raw = jnp.where((j <= i) | (j < prefix), raw, MASKED)
    shifted = jnp.exp(raw - jnp.max(raw, -1, keepdims=True))
    return shifted / jnp.sum(shifted, -1, keepdims=True)


def attend_kernel(prefix_ref, table_ref, query_ref, key_ref, value_ref, out_ref):
    seqlen = query_ref.shape[0]
    prefix = prefix_ref[0]
    for head in range(2):
        lanes = slice(head * HEAD_DIM, (head + 1) * HEAD_DIM)
        rows = bias_rows(table_ref[0, head : head + 1, :], seqlen)
        key, value = key_ref[:, lanes], value_ref[:, lanes]
        for block in range(seqlen // 128):
            at = slice(128 * block, 128 * (block + 1))
            probs = probabilities(query_ref[at, lanes], key, rows, prefix, block, seqlen)
            out = jnp.dot(probs.astype(BF), value, preferred_element_type=F32)
            out_ref[at, lanes] = out.astype(BF)


def attend_back_kernel(
    prefix_ref,
    table_ref,
    query_ref,
    key_ref,
    value_ref,
    upstream_ref,
    query_grad_ref,
    key_grad_ref,
    value_grad_ref,
    bias_ref,
):
    seqlen = query_ref.shape[0]
    blocks = seqlen // 128
    prefix = prefix_ref[0]
    flip = (((0,), (0,)), ((), ()))
    for head in range(2):
        lanes = slice(head * HEAD_DIM, (head + 1) * HEAD_DIM)
        rows = bias_rows(table_ref[0, head : head + 1, :], seqlen)
        query, key, value = query_ref[:, lanes], key_ref[:, lanes], value_ref[:, lanes]
        upstream = upstream_ref[:, lanes]
        probs_low, scores_low, scores = [], [], []
        for block in range(blocks):
            at = slice(128 * block, 128 * (block + 1))
            probs = probabilities(query[at], key, rows, prefix, block, seqlen)
            probs_grad = lax.dot_general(
                upstream[at], value, (((1,), (1,)), ((), ())), preferred_element_type=F32
            )
            inner = jnp.sum(probs * probs_grad, -1, keepdims=True)
            low = (probs * (probs_grad - inner)).astype(BF)
            probs_low.append(probs.astype(BF))
            scores_low.append(low)
            scores.append(low.astype(F32))
            out = jnp.dot(low, key, preferred_element_type=F32) * 0.125
            query_grad_ref[at, lanes] = out.astype(BF)
        probs_all = jnp.concatenate(probs_low, 0)
        scores_all = jnp.concatenate(scores_low, 0)
        out = lax.dot_general(probs_all, upstream, flip, preferred_element_type=F32)
        value_grad_ref[:, lanes] = out.astype(BF)
        out = lax.dot_general(scores_all, query, flip, preferred_element_type=F32) * 0.125
        key_grad_ref[:, lanes] = out.astype(BF)
        columns = []
        for column in range(2 * blocks - 1):
            terms = []
            for block in range(blocks):
                piece = column - (blocks - 1 - block)
                if 0 <= piece < blocks:
                    terms.append(scores[block][:, 128 * piece : 128 * (piece + 1)])
            columns.append(functools.reduce(jnp.add, terms))
        columns.append(jnp.zeros_like(columns[0]))
        wide = jnp.concatenate(columns, 1)
        total = jnp.zeros((8, wide.shape[1]), F32)
        for group in range(16):
            total = total + pltpu.roll(wide[8 * group : 8 * group + 8], 127 - 8 * group, 1)
        bias_ref[0, head] = total


def attention_specs(seqlen, width):
    pairs = HEADS // 2
    table = pl.BlockSpec((1, 2, width), lambda p: (p, 0, 0))
    return (
        [pl.BlockSpec(memory_space=pltpu.SMEM), table]
        + [
            pl.BlockSpec((seqlen, 128), lambda p, part=part: (0, part * pairs + p))
            for part in range(3)
        ],
        pl.BlockSpec((seqlen, 128), lambda p: (0, p)),
    )


def attend(prefix, table, projected):
    seqlen = projected.shape[0]
    ins, out = attention_specs(seqlen, table.shape[-1])
    return pl.pallas_call(
        attend_kernel,
        grid=(HEADS // 2,),
        in_specs=ins,
        out_specs=out,
        out_shape=jax.ShapeDtypeStruct((seqlen, D), BF),
        cost_estimate=pl.CostEstimate(
            flops=4 * seqlen * seqlen * D,
            bytes_accessed=8 * seqlen * D,
            transcendentals=HEADS * seqlen * seqlen,
        ),
        name="attend",
    )(prefix, table, projected, projected, projected)


def attend_back(prefix, table, projected, upstream):
    seqlen = projected.shape[0]
    width = table.shape[-1]
    ins, out = attention_specs(seqlen, width)
    grad = jax.ShapeDtypeStruct((seqlen, D), BF)
    return pl.pallas_call(
        attend_back_kernel,
        grid=(HEADS // 2,),
        in_specs=ins + [out],
        out_specs=[out, out, out, pl.BlockSpec((1, 2, 8, width), lambda p: (p, 0, 0, 0))],
        out_shape=[grad, grad, grad, jax.ShapeDtypeStruct((HEADS // 2, 2, 8, width), F32)],
        cost_estimate=pl.CostEstimate(
            flops=10 * seqlen * seqlen * D,
            bytes_accessed=14 * seqlen * D,
            transcendentals=HEADS * seqlen * seqlen,
        ),
        name="attend_back",
    )(prefix, table, projected, projected, projected, upstream)


def where_am_i():
    dp, expert = lax.axis_index("dp"), lax.axis_index("expert")
    return dp // 2, dp % 2, expert // 2, expert % 2


def device_at(z, x, y, core):
    return (2 * z + x, 2 * y + core)


def greet(z, x, y, core):
    barrier = pltpu.get_barrier_semaphore()

    def call(*place):
        pl.semaphore_signal(
            barrier, inc=1, device_id=device_at(*place), device_id_type=pl.DeviceIdType.MESH
        )

    call(z, 1 - x, y, core)
    call(z, x, 1 - y, core)
    call(z, x, y, 1 - core)

    @pl.when(z > 0)
    def _():
        call(z - 1, x, y, core)

    @pl.when(z < 3)
    def _():
        call(z + 1, x, y, core)

    pl.semaphore_wait(barrier, 3 + (z > 0).astype(jnp.int32) + (z < 3).astype(jnp.int32))


def gather_kernel(
    up_ref,
    down_ref,
    dense_ref,
    small_ref,
    tokens_ref,
    hits_ref,
    prefix_ref,
    up_full,
    down_full,
    dense_full,
    small_full,
    hidden_ref,
    projected_ref,
    attended_ref,
    residual_ref,
    table_ref,
    local_sem,
    z_send,
    z_recv,
    x_send,
    x_recv,
    dz_send,
    dz_recv,
    d_send,
    d_recv,
):
    z, x, y, core = where_am_i()
    greet(z, x, y, core)
    share = dense_ref.shape[1]
    half = up_ref.shape[1]
    sides = {1: z < 3, -1: z > 0}

    def piece(c, row, column):
        if c < 2:
            return up_full.at[2 * row + column, c]
        return down_full.at[2 * row + column]

    def mine(c):
        return up_ref.at[c] if c < 2 else down_ref

    def copy_z(c, row, side, own=False):
        return pltpu.make_async_remote_copy(
            src_ref=mine(c) if own else piece(c, row, x),
            dst_ref=piece(c, row, x),
            send_sem=z_send.at[c, (side + 1) // 2, row],
            recv_sem=z_recv.at[c, row],
            device_id=device_at(z + side, x, y, core),
            device_id_type=pl.DeviceIdType.MESH,
        )

    def copy_x(c, row, own=False):
        return pltpu.make_async_remote_copy(
            src_ref=mine(c) if own else piece(c, row, x),
            dst_ref=piece(c, row, x),
            send_sem=x_send.at[c, row],
            recv_sem=x_recv.at[c, row],
            device_id=device_at(z, 1 - x, y, core),
            device_id_type=pl.DeviceIdType.MESH,
        )

    def send_own(c):
        for side in (1, -1):
            @pl.when(sides[side])
            def _(side=side):
                copy_z(c, z, side, True).start()
        copy_x(c, z, True).start()

    def slot(row, column, line, number):
        return row * 8 + column * 4 + line * 2 + number

    def dense_copies(row, column, line, link, own=False):
        at = slot(row, column, line, core)
        target, sems, index = {
            "right": (device_at(z + 1, x, y, core), dz_send, (1, row)),
            "left": (device_at(z - 1, x, y, core), dz_send, (0, row)),
            "x": (device_at(z, 1 - x, y, core), d_send, (0, row)),
            "y": (device_at(z, x, 1 - y, core), d_send, (1, row * 2 + column)),
            "core": (device_at(z, x, y, 1 - core), d_send, (2, row * 4 + column * 2 + line)),
        }[link]
        if sems is dz_send:
            recv, place = dz_recv, (row,)
        else:
            recv, place = d_recv, index
        rows = pl.ds(pl.multiple_of(at * share, share), share)
        return [
            pltpu.make_async_remote_copy(
                src_ref=dense_ref if own else dense_full.at[:, rows],
                dst_ref=dense_full.at[:, rows],
                send_sem=sems.at[(0,) + index],
                recv_sem=recv.at[(0,) + place],
                device_id=target,
                device_id_type=pl.DeviceIdType.MESH,
            ),
            pltpu.make_async_remote_copy(
                src_ref=small_ref if own else small_full.at[at],
                dst_ref=small_full.at[at],
                send_sem=sems.at[(1,) + index],
                recv_sem=recv.at[(1,) + place],
                device_id=target,
                device_id_type=pl.DeviceIdType.MESH,
            ),
        ]

    def each(copies, step):
        for copy in copies:
            getattr(copy, step)()

    own_at = slot(z, x, y, core)
    own_rows = pl.ds(pl.multiple_of(own_at * share, share), share)
    local = [
        pltpu.make_async_copy(up_ref, up_full.at[2 * z + x], local_sem.at[0]),
        pltpu.make_async_copy(down_ref, down_full.at[2 * z + x], local_sem.at[1]),
        pltpu.make_async_copy(dense_ref, dense_full.at[:, own_rows], local_sem.at[2]),
        pltpu.make_async_copy(small_ref, small_full.at[own_at], local_sem.at[3]),
    ]

    for side, link in ((1, "right"), (-1, "left")):
        @pl.when(sides[side])
        def _(link=link):
            each(dense_copies(z, x, y, link, True), "start")
    for link in ("x", "y", "core"):
        each(dense_copies(z, x, y, link, True), "start")
    send_own(0)
    each(local, "start")

    def x_arrived(row):
        each(dense_copies(row, 1 - x, y, "x"), "wait_recv")
        each(dense_copies(row, 1 - x, y, "y"), "start")
        each(dense_copies(row, 1 - x, y, "core"), "start")

    for s in (1, 2, 3):
        for side, link in ((1, "right"), (-1, "left")):
            row = z - side * s
            there = (z >= s) if side > 0 else (z + s <= 3)

            @pl.when(there)
            def _(row=row, side=side, link=link):
                each(dense_copies(row, x, y, link), "wait_recv")

                @pl.when(sides[side])
                def _():
                    each(dense_copies(row, x, y, link), "start")

                for other in ("x", "y", "core"):
                    each(dense_copies(row, x, y, other), "start")
        if s == 1:
            x_arrived(z)
        if s < 3:
            send_own(s)
    for s in (1, 2, 3):
        for row, there in ((z - s, z >= s), (z + s, z + s <= 3)):
            @pl.when(there)
            def _(row=row):
                x_arrived(row)
    for s in range(4):
        for column in range(2):
            row = lax.rem(z + s, 4)
            each(dense_copies(row, column, 1 - y, "y"), "wait_recv")
            each(dense_copies(row, column, 1 - y, "core"), "start")

    def pass_on(c, s):
        for side in (1, -1):
            row = z - side * s
            there = (z >= s) if side > 0 else (z + s <= 3)

            @pl.when(there)
            def _(row=row, side=side):
                copy_z(c, row, side).wait_recv()

                @pl.when(sides[side])
                def _():
                    copy_z(c, row, side).start()

                copy_x(c, row).start()

    for c in range(3):
        pass_on(c, 1)

    for row in range(4):
        for column in range(2):
            for line in range(2):
                at = slot(row, column, line, 1 - core)
                rows = pl.ds(pl.multiple_of(at * share, share), share)
                index = row * 4 + column * 2 + line
                for part, ref in enumerate((dense_full.at[:, rows], small_full.at[at])):
                    pltpu.make_async_remote_copy(
                        src_ref=ref,
                        dst_ref=ref,
                        send_sem=d_send.at[part, 2, index],
                        recv_sem=d_recv.at[part, 2, index],
                        device_id=device_at(z, x, y, 1 - core),
                        device_id_type=pl.DeviceIdType.MESH,
                    ).wait_recv()
    each(local, "wait")

    width = dense_full.shape[2]
    lane = lax.broadcasted_iota(jnp.int32, (small_full.shape[0], width), 1)
    line_of = lax.broadcasted_iota(jnp.int32, (small_full.shape[0], width), 0)
    gain_parts = small_full[:, 1, 0:share]
    spread = (
        lax.broadcasted_iota(jnp.int32, (share, width), 1) % share
        == lax.broadcasted_iota(jnp.int32, (share, width), 0)
    ).astype(F32)
    wide = jnp.dot(gain_parts, spread, precision=HIGHEST, preferred_element_type=F32)
    gain = jnp.sum(jnp.where(lane // share == line_of, wide, 0.0), 0, keepdims=True)
    bias_parts = small_full[:, 2, 0 : BUCKETS // 2]
    low = jnp.dot(bias_parts, hits_ref[: BUCKETS // 2], precision=HIGHEST, preferred_element_type=F32)
    high = jnp.dot(bias_parts, hits_ref[BUCKETS // 2 :], precision=HIGHEST, preferred_element_type=F32)
    for head in range(HEADS):
        table_ref[head : head + 1] = low[2 * head : 2 * head + 1] + high[2 * head + 1 : 2 * head + 2]
    seqlen = tokens_ref.shape[0]
    step = 128

    @pl.loop(0, seqlen // step)
    def _(i):
        at = pl.ds(pl.multiple_of(i * step, step), step)
        hidden_ref[at] = normed(tokens_ref[at].astype(F32), gain).astype(BF)

    tile = 256
    for part in range(3):
        @pl.loop(0, width // tile)
        def _(n, part=part):
            at = pl.ds(pl.multiple_of(n * tile, tile), tile)
            out = jnp.dot(hidden_ref[...], dense_full[part, :, at], preferred_element_type=F32)
            at = pl.ds(pl.multiple_of(part * width + n * tile, tile), tile)
            projected_ref[:, at] = out.astype(BF)

    prefix = prefix_ref[0]

    @pl.loop(0, HEADS // 2)
    def _(pair):
        def window(part):
            return pl.ds(pl.multiple_of(part * width + pair * 128, 128), 128)

        query_ref = projected_ref.at[:, window(0)]
        key_ref = projected_ref.at[:, window(1)]
        value_ref = projected_ref.at[:, window(2)]
        out_ref = attended_ref.at[:, window(0)]
        for head in range(2):
            lanes = slice(head * HEAD_DIM, (head + 1) * HEAD_DIM)
            rows = bias_rows(table_ref[pl.ds(2 * pair + head, 1), :], seqlen)
            key, value = key_ref[:, lanes], value_ref[:, lanes]
            for block in range(seqlen // 128):
                at = slice(128 * block, 128 * (block + 1))
                probs = probabilities(query_ref[at, lanes], key, rows, prefix, block, seqlen)
                out = jnp.dot(probs.astype(BF), value, preferred_element_type=F32)
                out_ref[at, lanes] = out.astype(BF)

        for c in range(3):
            for s in (2, 3):
                @pl.when(pair == 3 * (s - 2) + c + 1)
                def _(c=c, s=s):
                    pass_on(c, s)

    @pl.loop(0, width // tile)
    def _(n):
        at = pl.ds(pl.multiple_of(n * tile, tile), tile)
        out = jnp.dot(attended_ref[...], dense_full[3, :, at], preferred_element_type=F32)
        residual_ref[:, at] = tokens_ref[:, at].astype(F32) + out

    for row in range(4):
        for column in range(2):
            for line in range(2):
                each(dense_copies(row, column, line, "core"), "wait_send")
        for column in range(2):
            each(dense_copies(row, column, y, "y"), "wait_send")
        each(dense_copies(row, x, y, "x"), "wait_send")
        for side, link in ((1, "right"), (-1, "left")):
            sent = sides[side] & ((row <= z) if side > 0 else (row >= z))

            @pl.when(sent)
            def _(row=row, side=side, link=link):
                each(dense_copies(row, x, y, link), "wait_send")
                for c in range(3):
                    copy_z(c, row, side).wait_send()
        for c in range(3):
            copy_x(c, row).wait_recv()
            copy_x(c, row).wait_send()


def gather_weights(up, down, dense, small, tokens, hits, prefix):
    seqlen, width = tokens.shape
    devices = lax.axis_size(BOTH)
    slices = lax.axis_size("dp")
    vmem, hbm = pl.BlockSpec(memory_space=pltpu.VMEM), pl.BlockSpec(memory_space=pl.ANY)
    dma = pltpu.SemaphoreType.DMA
    return pl.pallas_call(
        gather_kernel,
        in_specs=[vmem] * 6 + [pl.BlockSpec(memory_space=pltpu.SMEM)],
        out_specs=[hbm] * 2 + [vmem] * 7,
        out_shape=[
            jax.ShapeDtypeStruct((slices,) + up.shape, BF),
            jax.ShapeDtypeStruct((slices,) + down.shape, BF),
            jax.ShapeDtypeStruct((dense.shape[0], devices * dense.shape[1], dense.shape[2]), BF),
            jax.ShapeDtypeStruct((devices,) + small.shape, F32),
            jax.ShapeDtypeStruct((seqlen, width), BF),
            jax.ShapeDtypeStruct((seqlen, 3 * width), BF),
            jax.ShapeDtypeStruct((seqlen, width), BF),
            jax.ShapeDtypeStruct((seqlen, width), F32),
            jax.ShapeDtypeStruct((HEADS, hits.shape[1]), F32),
        ],
        scratch_shapes=[
            dma((4,)),
            dma((3, 2, 4)),
            dma((3, 4)),
            dma((3, 4)),
            dma((3, 4)),
            dma((2, 2, 4)),
            dma((2, 4)),
            dma((2, 3, 16)),
            dma((2, 3, 16)),
        ],
        compiler_params=pltpu.CompilerParams(collective_id=1, has_side_effects=True, vmem_limit_bytes=60 * 2**20),
        name="gather_weights",
    )(up, down, dense, small, tokens, hits, prefix)


def on_device(
    tokens,
    cotangent,
    routes,
    prefix,
    buckets,
    step_count,
    learn_rate,
    weight_decay,
    attend_master,
    attend_first,
    attend_second,
    outward_master,
    outward_first,
    outward_second,
    router_master,
    router_first,
    router_second,
    gains_master,
    gains_first,
    gains_second,
    bias_master,
    bias_first,
    bias_second,
    upward_master,
    upward_first,
    upward_second,
    downward_master,
    downward_first,
    downward_second,
):
    devices = lax.axis_size(BOTH)
    share = attend_master.shape[1]
    seqlen = tokens.shape[0]
    experts = router_master.shape[1]
    capacity = seqlen * TOP * 5 // (4 * experts)

    slices = lax.axis_size("dp")
    router_size, gains_size = router_master.size, gains_master.size
    bucket_hits = (buckets[:, None] == jnp.arange(BUCKETS, dtype=jnp.int32)[None, :]).astype(F32)
    offsets = buckets.shape[0]
    inputs = tokens.astype(F32)
    if is_line():
        hits_wide = jnp.pad(bucket_hits.T, ((0, 0), (0, 2 * seqlen - offsets)))
        small = jnp.concatenate(
            [
                jnp.pad(one.reshape(1, -1), ((0, 0), (0, 128 - one.size)))
                for one in (router_master, gains_master, bias_master)
            ]
            + [jnp.zeros((5, 128), F32)]
        )
        dense = jnp.concatenate([attend_master.astype(BF), outward_master.astype(BF)[None]])
        (
            upward_w,
            downward_w,
            dense_w,
            small,
            hidden_one,
            projected,
            attended,
            residual,
            table,
        ) = gather_weights(
            upward_master[:, 0].astype(BF),
            downward_master[0].astype(BF),
            dense,
            small,
            tokens,
            hits_wide,
            prefix,
        )
        attend_w, outward_w = dense_w[:3], dense_w[3]
        gate_w, up_w = upward_w[:, 0].reshape(D, FF), upward_w[:, 1].reshape(D, FF)
        downward_w = downward_w.reshape(FF, D)
        router_w = small[:, 0].reshape(D, experts)
        gains_w = small[:, 1, :gains_size].reshape(devices, 2, share).transpose(1, 0, 2).reshape(2, D)
        table = table.reshape(HEADS // 2, 2, 2 * seqlen)
        first_pull = jax.vjp(normed, inputs, gains_w[0])[1]
    else:
        gate_w = gather_dp(upward_master[0, 0].astype(BF)).reshape(D, FF)
        up_w = gather_dp(upward_master[1, 0].astype(BF)).reshape(D, FF)
        downward_w = gather_dp(downward_master[0].astype(BF)).reshape(FF, D)
        attend_w = lax.all_gather(attend_master.astype(BF), BOTH, axis=1, tiled=True)
        outward_w = lax.all_gather(outward_master.astype(BF), BOTH, axis=0, tiled=True)
        router_w = lax.all_gather(router_master, BOTH, axis=0, tiled=True)
        gains_w = lax.all_gather(gains_master, BOTH, axis=1, tiled=True)
        bias_w = lax.all_gather(bias_master, BOTH, axis=0, tiled=True)
        table = jnp.dot(bias_w.reshape(HEADS, BUCKETS), bucket_hits.T, precision=HIGHEST)
        table = jnp.pad(table, ((0, 0), (0, 2 * seqlen - offsets)))
        table = table.reshape(HEADS // 2, 2, 2 * seqlen)
        first_normed, first_pull = jax.vjp(normed, inputs, gains_w[0])
        hidden_one = first_normed.astype(BF)
        projected = jnp.concatenate(
            [
                jnp.dot(hidden_one, attend_w[part], preferred_element_type=F32).astype(BF)
                for part in range(3)
            ],
            1,
        )
        attended = attend(prefix, table, projected)
        residual = inputs + jnp.dot(attended, outward_w, preferred_element_type=F32)

    kinds = jnp.arange(experts, dtype=jnp.int32)
    route_hits = (routes[:, :, None] == kinds[None, None, :]).astype(F32)

    def gate_piece(residual_in, scale_gain, router_in):
        second_normed = normed(residual_in, scale_gain)
        logits = jnp.dot(second_normed, router_in, precision=HIGHEST)
        router_soft = jax.nn.softmax(logits, axis=-1)
        chosen = jnp.sum(router_soft[:, None, :] * route_hits, -1)
        return (second_normed, chosen / jnp.sum(chosen, -1, keepdims=True))

    (second_normed, combine), gate_pull = jax.vjp(gate_piece, residual, gains_w[1], router_w)
    second_low = second_normed.astype(BF)

    hits = jnp.sum(route_hits, 1)
    places = jnp.arange(seqlen, dtype=jnp.int32)
    earlier = (places[None, :] < places[:, None]).astype(BF)
    rank = jnp.dot(earlier, hits.astype(BF), preferred_element_type=F32)
    rank = jnp.where(hits > 0, rank, -1.0).astype(jnp.int32)
    slots = jnp.arange(capacity, dtype=jnp.int32)
    taken = rank.T[:, None, :] == slots[None, :, None]
    choose = taken.astype(BF).reshape(experts * capacity, seqlen)
    weight = jnp.sum(combine[:, :, None] * route_hits, 1)
    slot_weight = jnp.sum(jnp.where(taken, weight.T[:, None, :], 0.0), -1)
    backs = [
        (
            (rank[:, :, None] == slots[None, None, :])
            & (routes[:, k][:, None, None] == kinds[None, :, None])
        )
        .astype(BF)
        .reshape(seqlen, experts * capacity)
        for k in range(TOP)
    ]
    back = (rank[:, :, None] == slots[None, None, :]).astype(BF)
    back = back.reshape(seqlen, experts * capacity)

    def exchange(rows, home):
        if home:
            rows = rows.reshape(1, experts, capacity, D)
            rows = lax.all_to_all(rows, "expert", split_axis=1, concat_axis=0, tiled=True)
        else:
            rows = rows.reshape(experts, 1, capacity, D)
            rows = lax.all_to_all(rows, "expert", split_axis=0, concat_axis=1, tiled=True)
        return rows.reshape(experts * capacity, D)

    sent_rows = jnp.dot(choose, second_low, preferred_element_type=F32).astype(BF)
    arrived = exchange(sent_rows, False)
    upstream_rows = jnp.dot(choose, cotangent, preferred_element_type=F32)
    grad_rows = (slot_weight.reshape(-1, 1) * upstream_rows).astype(BF)
    grad_arrived = exchange(grad_rows, False)

    gate_value = jnp.dot(arrived, gate_w, preferred_element_type=F32)
    up_value = jnp.dot(arrived, up_w, preferred_element_type=F32)
    gelu_value, gelu_pull = jax.vjp(gelu_tanh, gate_value)
    hidden_mid = (gelu_value * up_value).astype(BF)
    expert_out = jnp.dot(hidden_mid, downward_w, preferred_element_type=F32).astype(BF)
    returned = exchange(expert_out, True)

    turned = (((1,), (1,)), ((), ()))
    flipped = (((0,), (0,)), ((), ()))
    grad_mid = lax.dot_general(grad_arrived, downward_w, turned, preferred_element_type=F32)
    grad_gate = gelu_pull(grad_mid * up_value)[0].astype(BF)
    grad_up = (grad_mid * gelu_value).astype(BF)
    grad_sent = lax.dot_general(grad_gate, gate_w, turned, preferred_element_type=F32)
    grad_sent = grad_sent + lax.dot_general(grad_up, up_w, turned, preferred_element_type=F32)
    grad_home = exchange(grad_sent.astype(BF), True)


    def weight_grad(left, right):
        full = lax.dot_general(left, right, flipped, preferred_element_type=F32).astype(BF)
        return full.reshape(slices, -1, full.shape[1])

    downward_g = scatter_dp(weight_grad(hidden_mid, grad_arrived))[None]
    upward_g = scatter_dp(
        jnp.concatenate([weight_grad(arrived, grad_gate), weight_grad(arrived, grad_up)], 1)
    ).reshape(2, 1, D // slices, FF)

    came_back = jnp.stack(
        [jnp.dot(one, returned, preferred_element_type=F32) for one in backs], 1
    )
    expert_sum = jnp.sum(combine[..., None] * came_back, 1)
    block_output = (residual + expert_sum).astype(BF)
    upstream = cotangent.astype(F32)
    combine_grad = jnp.sum(upstream[:, None, :] * came_back, -1)

    grad_normed = jnp.dot(back, grad_home, preferred_element_type=F32)
    residual_part, gain_two_grad, router_full = gate_pull((grad_normed, combine_grad))
    grad_residual = upstream + residual_part
    grad_branch = grad_residual.astype(BF)
    outward_full = lax.dot_general(attended, grad_branch, flipped, preferred_element_type=F32)
    outward_g = scatter_all(outward_full.astype(BF).reshape(devices, share, D))
    grad_attended = lax.dot_general(grad_branch, outward_w, turned, preferred_element_type=F32)
    query_grad, key_grad, value_grad, bias_parts = attend_back(
        prefix, table, projected, grad_attended.astype(BF)
    )
    projected_grads = (query_grad, key_grad, value_grad)
    attend_g = scatter_all(
        jnp.concatenate(
            [
                lax.dot_general(hidden_one, part, flipped, preferred_element_type=F32)
                .astype(BF)
                .reshape(devices, share, D)
                for part in projected_grads
            ],
            1,
        )
    ).reshape(3, share, D)
    grad_hidden_one = functools.reduce(
        jnp.add,
        [
            lax.dot_general(part, attend_w[which], turned, preferred_element_type=F32)
            for which, part in enumerate(projected_grads)
        ],
    )
    inputs_part, gain_one_grad = first_pull(grad_hidden_one)
    input_grad = (grad_residual + inputs_part).astype(BF)

    bias_parts = bias_parts.reshape(HEADS, 8, 2 * seqlen)
    bias_parts = jnp.pad(bias_parts, ((0, 0), (0, 0), (0, 8)))
    per_offset = functools.reduce(
        jnp.add, [bias_parts[:, row, row : row + offsets] for row in range(8)]
    )
    bias_full = jnp.dot(per_offset, bucket_hits, precision=HIGHEST).reshape(-1)

    smalls = sum_all(
        jnp.concatenate([router_full.reshape(-1), gain_one_grad, gain_two_grad, bias_full])
    )
    place = lax.axis_index(BOTH)
    router_g = lax.dynamic_slice(smalls, (place * router_size,), (router_size,))
    router_g = router_g.reshape(share, experts)
    start = D * experts
    gains_g = jnp.stack(
        [
            lax.dynamic_slice(smalls, (start + row * D + place * share,), (share,))
            for row in range(2)
        ]
    )
    bias_g = lax.dynamic_slice(smalls, (start + 2 * D + place * bias_master.size,), bias_master.shape)

    grads_all = (attend_g, outward_g, router_g, gains_g, bias_g, upward_g, downward_g)
    squares = jnp.stack([jnp.sum(member_grad * member_grad) for member_grad in grads_all])
    totals = sum_all(squares)
    counts_all = jnp.array(
        [
            3 * D * D,
            D * D,
            D * experts,
            2 * D,
            HEADS * BUCKETS,
            2 * experts * D * FF,
            experts * FF * D,
        ],
        jnp.float32,
    )
    mean_squares = totals / counts_all
    grad_rms = jnp.sqrt(mean_squares)
    factors = lax.rsqrt(mean_squares + 1e-06)
    step_float = step_count.astype(jnp.float32)
    masters = (
        attend_master,
        outward_master,
        router_master,
        gains_master,
        bias_master,
        upward_master,
        downward_master,
    )
    firsts = (
        attend_first,
        outward_first,
        router_first,
        gains_first,
        bias_first,
        upward_first,
        downward_first,
    )
    seconds = (
        attend_second,
        outward_second,
        router_second,
        gains_second,
        bias_second,
        upward_second,
        downward_second,
    )
    flags = (True, True, True, False, False, True, True)
    updates = [
        adamw_update(
            masters[member],
            firsts[member],
            seconds[member],
            grads_all[member] * factors[member],
            step_float,
            learn_rate,
            weight_decay,
            flags[member],
        )
        for member in range(7)
    ]
    return (
        block_output,
        input_grad,
        grads_all[0],
        updates[0][0],
        updates[0][1],
        updates[0][2],
        grads_all[1],
        updates[1][0],
        updates[1][1],
        updates[1][2],
        grads_all[2],
        updates[2][0],
        updates[2][1],
        updates[2][2],
        grads_all[3],
        updates[3][3],
        updates[3][1],
        updates[3][2],
        grads_all[4],
        updates[4][3],
        updates[4][1],
        updates[4][2],
        grads_all[5],
        updates[5][0],
        updates[5][1],
        updates[5][2],
        grads_all[6],
        updates[6][0],
        updates[6][1],
        updates[6][2],
        grad_rms,
    )


def solution(mesh):
    placed = (
        P(("dp", "expert"), None),
        P(("dp", "expert"), None),
        P(("dp", "expert"), None),
        P(("dp", "expert")),
        P(),
        P(),
        P(),
        P(),
        P(None, ("dp", "expert"), None),
        P(None, ("dp", "expert"), None),
        P(None, ("dp", "expert"), None),
        P(("dp", "expert"), None),
        P(("dp", "expert"), None),
        P(("dp", "expert"), None),
        P(("dp", "expert"), None),
        P(("dp", "expert"), None),
        P(("dp", "expert"), None),
        P(None, ("dp", "expert")),
        P(None, ("dp", "expert")),
        P(None, ("dp", "expert")),
        P(("dp", "expert")),
        P(("dp", "expert")),
        P(("dp", "expert")),
        P(None, "expert", "dp", None),
        P(None, "expert", "dp", None),
        P(None, "expert", "dp", None),
        P("expert", "dp", None),
        P("expert", "dp", None),
        P("expert", "dp", None),
    )
    return jax.shard_map(
        on_device,
        mesh=mesh,
        in_specs=placed,
        out_specs=(
            P(("dp", "expert"), None),
            P(("dp", "expert"), None),
            P(None, ("dp", "expert"), None),
            P(None, ("dp", "expert"), None),
            P(None, ("dp", "expert"), None),
            P(None, ("dp", "expert"), None),
            P(("dp", "expert"), None),
            P(("dp", "expert"), None),
            P(("dp", "expert"), None),
            P(("dp", "expert"), None),
            P(("dp", "expert"), None),
            P(("dp", "expert"), None),
            P(("dp", "expert"), None),
            P(("dp", "expert"), None),
            P(None, ("dp", "expert")),
            P(None, ("dp", "expert")),
            P(None, ("dp", "expert")),
            P(None, ("dp", "expert")),
            P(("dp", "expert")),
            P(("dp", "expert")),
            P(("dp", "expert")),
            P(("dp", "expert")),
            P(None, "expert", "dp", None),
            P(None, "expert", "dp", None),
            P(None, "expert", "dp", None),
            P(None, "expert", "dp", None),
            P("expert", "dp", None),
            P("expert", "dp", None),
            P("expert", "dp", None),
            P("expert", "dp", None),
            P(),
        ),
        check_vma=False,
    )
```

```python
import functools

import jax
import jax.numpy as jnp
from jax import lax
from jax.experimental import pallas as pl
from jax.experimental.pallas import tpu as pltpu
from jax.sharding import PartitionSpec as P

D = 1024
HEADS = 16
HEAD_DIM = 64
FF = 2816
BUCKETS = 32
TOP = 2
BOTH = ("dp", "expert")
BF = jnp.bfloat16
F32 = jnp.float32

HIGHEST = lax.Precision.HIGHEST
MASKED = -1e30


def normed(values, scale_gain):
    return values * lax.rsqrt(jnp.mean(values * values, -1, keepdims=True) + 1e-06) * scale_gain


def gelu_tanh(values):
    return jax.nn.gelu(values, approximate=True)


def adamw_update(
    master, first_moment, second, gradient, step_float, learn_rate, weight_decay, decayed
):
    mean_new = 0.9 * first_moment + 0.1 * gradient
    square_new = 0.95 * second + 0.05 * gradient * gradient
    mean_hat = mean_new / (1.0 - jnp.power(jnp.float32(0.9), step_float))
    square_hat = square_new / (1.0 - jnp.power(jnp.float32(0.95), step_float))
    change = learn_rate * (mean_hat / (jnp.sqrt(square_hat) + 1e-08))
    updated = master - change
    if decayed:
        updated = updated - weight_decay * master
    return (updated, mean_new, square_new, -change)


def is_line():
    return lax.axis_size("dp") == 8 and lax.axis_size("expert") == 4


def gather_dp(shard):
    return lax.all_gather(shard, "dp", axis=0)


def scatter_dp(parts):
    return lax.psum_scatter(parts.astype(F32), "dp", scatter_dimension=0, tiled=False)


def scatter_all(parts):
    return lax.psum_scatter(parts.astype(F32), BOTH, scatter_dimension=0, tiled=False)


def swap_expert(array, bit):
    return lax.ppermute(array, "expert", [(e, e ^ bit) for e in range(4)])


def sum_all(array):
    if not is_line():
        return lax.psum(array, BOTH)
    for bit in (1, 2):
        array = array + swap_expert(array, bit)
    for bit in (1, 2, 4):
        array = array + lax.ppermute(array, "dp", [(d, d ^ bit) for d in range(8)])
    return array


def bias_rows(table, seqlen):
    width = table.shape[-1]
    wide = jnp.broadcast_to(table, (128, width))
    return pltpu.roll(wide, width - 127, 1, stride=1, stride_axis=0)


def probabilities(query, key, rows, prefix, block, seqlen):
    blocks = seqlen // 128
    raw = (
        lax.dot_general(query, key, (((1,), (1,)), ((), ())), preferred_element_type=F32) * 0.125
    )
    start = 128 * (blocks - 1 - block)
    raw = raw + rows[:, start : start + seqlen]
    i = lax.broadcasted_iota(jnp.int32, raw.shape, 0) + 128 * block
    j = lax.broadcasted_iota(jnp.int32, raw.shape, 1)
    raw = jnp.where((j <= i) | (j < prefix), raw, MASKED)
    shifted = jnp.exp(raw - jnp.max(raw, -1, keepdims=True))
    return shifted / jnp.sum(shifted, -1, keepdims=True)


def attend_kernel(prefix_ref, table_ref, query_ref, key_ref, value_ref, out_ref):
    seqlen = query_ref.shape[0]
    prefix = prefix_ref[0]
    for head in range(2):
        lanes = slice(head * HEAD_DIM, (head + 1) * HEAD_DIM)
        rows = bias_rows(table_ref[0, head : head + 1, :], seqlen)
        key, value = key_ref[:, lanes], value_ref[:, lanes]
        for block in range(seqlen // 128):
            at = slice(128 * block, 128 * (block + 1))
            probs = probabilities(query_ref[at, lanes], key, rows, prefix, block, seqlen)
            out = jnp.dot(probs.astype(BF), value, preferred_element_type=F32)
            out_ref[at, lanes] = out.astype(BF)


def diagonals(scores):
    blocks = len(scores)
    columns = []
    for column in range(2 * blocks - 1):
        terms = []
        for block in range(blocks):
            piece = column - (blocks - 1 - block)
            if 0 <= piece < blocks:
                terms.append(scores[block][:, 128 * piece : 128 * (piece + 1)])
        columns.append(functools.reduce(jnp.add, terms))
    columns.append(jnp.zeros_like(columns[0]))
    wide = jnp.concatenate(columns, 1)
    total = jnp.zeros((8, wide.shape[1]), F32)
    for group in range(16):
        total = total + pltpu.roll(wide[8 * group : 8 * group + 8], 127 - 8 * group, 1)
    return total


def attend_back_kernel(
    prefix_ref,
    table_ref,
    query_ref,
    key_ref,
    value_ref,
    upstream_ref,
    query_grad_ref,
    key_grad_ref,
    value_grad_ref,
    bias_ref,
):
    seqlen = query_ref.shape[0]
    blocks = seqlen // 128
    prefix = prefix_ref[0]
    flip = (((0,), (0,)), ((), ()))
    for head in range(2):
        lanes = slice(head * HEAD_DIM, (head + 1) * HEAD_DIM)
        rows = bias_rows(table_ref[0, head : head + 1, :], seqlen)
        query, key, value = query_ref[:, lanes], key_ref[:, lanes], value_ref[:, lanes]
        upstream = upstream_ref[:, lanes]
        probs_low, scores_low, scores = [], [], []
        for block in range(blocks):
            at = slice(128 * block, 128 * (block + 1))
            probs = probabilities(query[at], key, rows, prefix, block, seqlen)
            probs_grad = lax.dot_general(
                upstream[at], value, (((1,), (1,)), ((), ())), preferred_element_type=F32
            )
            inner = jnp.sum(probs * probs_grad, -1, keepdims=True)
            low = (probs * (probs_grad - inner)).astype(BF)
            probs_low.append(probs.astype(BF))
            scores_low.append(low)
            scores.append(low.astype(F32))
            out = jnp.dot(low, key, preferred_element_type=F32) * 0.125
            query_grad_ref[at, lanes] = out.astype(BF)
        probs_all = jnp.concatenate(probs_low, 0)
        scores_all = jnp.concatenate(scores_low, 0)
        out = lax.dot_general(probs_all, upstream, flip, preferred_element_type=F32)
        value_grad_ref[:, lanes] = out.astype(BF)
        out = lax.dot_general(scores_all, query, flip, preferred_element_type=F32) * 0.125
        key_grad_ref[:, lanes] = out.astype(BF)
        bias_ref[0, head] = diagonals(scores)


def attention_specs(seqlen, width):
    pairs = HEADS // 2
    table = pl.BlockSpec((1, 2, width), lambda p: (p, 0, 0))
    return (
        [pl.BlockSpec(memory_space=pltpu.SMEM), table]
        + [
            pl.BlockSpec((seqlen, 128), lambda p, part=part: (0, part * pairs + p))
            for part in range(3)
        ],
        pl.BlockSpec((seqlen, 128), lambda p: (0, p)),
    )


def attend(prefix, table, projected):
    seqlen = projected.shape[0]
    ins, out = attention_specs(seqlen, table.shape[-1])
    return pl.pallas_call(
        attend_kernel,
        grid=(HEADS // 2,),
        in_specs=ins,
        out_specs=out,
        out_shape=jax.ShapeDtypeStruct((seqlen, D), BF),
        cost_estimate=pl.CostEstimate(
            flops=4 * seqlen * seqlen * D,
            bytes_accessed=8 * seqlen * D,
            transcendentals=HEADS * seqlen * seqlen,
        ),
        name="attend",
    )(prefix, table, projected, projected, projected)


def attend_back(prefix, table, projected, upstream):
    seqlen = projected.shape[0]
    width = table.shape[-1]
    ins, out = attention_specs(seqlen, width)
    grad = jax.ShapeDtypeStruct((seqlen, D), BF)
    return pl.pallas_call(
        attend_back_kernel,
        grid=(HEADS // 2,),
        in_specs=ins + [out],
        out_specs=[out, out, out, pl.BlockSpec((1, 2, 8, width), lambda p: (p, 0, 0, 0))],
        out_shape=[grad, grad, grad, jax.ShapeDtypeStruct((HEADS // 2, 2, 8, width), F32)],
        cost_estimate=pl.CostEstimate(
            flops=10 * seqlen * seqlen * D,
            bytes_accessed=14 * seqlen * D,
            transcendentals=HEADS * seqlen * seqlen,
        ),
        name="attend_back",
    )(prefix, table, projected, projected, projected, upstream)


def where_am_i():
    dp, expert = lax.axis_index("dp"), lax.axis_index("expert")
    return dp // 2, dp % 2, expert // 2, expert % 2


def device_at(z, x, y, core):
    return (2 * z + x, 2 * y + core)


def greet(z, x, y, core):
    barrier = pltpu.get_barrier_semaphore()

    def call(*place):
        pl.semaphore_signal(
            barrier, inc=1, device_id=device_at(*place), device_id_type=pl.DeviceIdType.MESH
        )

    call(z, 1 - x, y, core)
    call(z, x, 1 - y, core)
    call(z, x, y, 1 - core)

    @pl.when(z > 0)
    def _():
        call(z - 1, x, y, core)

    @pl.when(z < 3)
    def _():
        call(z + 1, x, y, core)

    pl.semaphore_wait(barrier, 3 + (z > 0).astype(jnp.int32) + (z < 3).astype(jnp.int32))


def gather_kernel(
    up_ref,
    down_ref,
    dense_ref,
    small_ref,
    tokens_ref,
    hits_ref,
    prefix_ref,
    gate_full,
    up_full,
    down_full,
    dense_full,
    small_full,
    hidden_ref,
    projected_ref,
    attended_ref,
    residual_ref,
    table_ref,
    local_sem,
    z_send,
    z_recv,
    x_send,
    x_recv,
    dz_send,
    dz_recv,
    d_send,
    d_recv,
):
    z, x, y, core = where_am_i()
    greet(z, x, y, core)
    share = dense_ref.shape[1]
    sides = {1: z < 3, -1: z > 0}

    def piece(c, row, column):
        return (gate_full, up_full, down_full)[c].at[2 * row + column]

    def mine(c):
        return up_ref.at[c] if c < 2 else down_ref

    def copy_z(c, row, side, own=False):
        return pltpu.make_async_remote_copy(
            src_ref=mine(c) if own else piece(c, row, x),
            dst_ref=piece(c, row, x),
            send_sem=z_send.at[c, (side + 1) // 2, row],
            recv_sem=z_recv.at[c, row],
            device_id=device_at(z + side, x, y, core),
            device_id_type=pl.DeviceIdType.MESH,
        )

    def copy_x(c, row, own=False):
        return pltpu.make_async_remote_copy(
            src_ref=mine(c) if own else piece(c, row, x),
            dst_ref=piece(c, row, x),
            send_sem=x_send.at[c, row],
            recv_sem=x_recv.at[c, row],
            device_id=device_at(z, 1 - x, y, core),
            device_id_type=pl.DeviceIdType.MESH,
        )

    def send_own(c):
        for side in (1, -1):
            @pl.when(sides[side])
            def _(side=side):
                copy_z(c, z, side, True).start()
        copy_x(c, z, True).start()

    def slot(row, column, line, number):
        return row * 8 + column * 4 + line * 2 + number

    def dense_copies(row, column, line, link, own=False):
        at = slot(row, column, line, core)
        target, sems, index = {
            "right": (device_at(z + 1, x, y, core), dz_send, (1, row)),
            "left": (device_at(z - 1, x, y, core), dz_send, (0, row)),
            "x": (device_at(z, 1 - x, y, core), d_send, (0, row)),
            "y": (device_at(z, x, 1 - y, core), d_send, (1, row * 2 + column)),
            "core": (device_at(z, x, y, 1 - core), d_send, (2, row * 4 + column * 2 + line)),
        }[link]
        if sems is dz_send:
            recv, place = dz_recv, (row,)
        else:
            recv, place = d_recv, index
        rows = pl.ds(pl.multiple_of(at * share, share), share)
        return [
            pltpu.make_async_remote_copy(
                src_ref=dense_ref if own else dense_full.at[:, rows],
                dst_ref=dense_full.at[:, rows],
                send_sem=sems.at[(0,) + index],
                recv_sem=recv.at[(0,) + place],
                device_id=target,
                device_id_type=pl.DeviceIdType.MESH,
            ),
            pltpu.make_async_remote_copy(
                src_ref=small_ref if own else small_full.at[at],
                dst_ref=small_full.at[at],
                send_sem=sems.at[(1,) + index],
                recv_sem=recv.at[(1,) + place],
                device_id=target,
                device_id_type=pl.DeviceIdType.MESH,
            ),
        ]

    def each(copies, step):
        for copy in copies:
            getattr(copy, step)()

    own_at = slot(z, x, y, core)
    own_rows = pl.ds(pl.multiple_of(own_at * share, share), share)
    local = [
        pltpu.make_async_copy(up_ref.at[0], gate_full.at[2 * z + x], local_sem.at[0]),
        pltpu.make_async_copy(up_ref.at[1], up_full.at[2 * z + x], local_sem.at[4]),
        pltpu.make_async_copy(down_ref, down_full.at[2 * z + x], local_sem.at[1]),
        pltpu.make_async_copy(dense_ref, dense_full.at[:, own_rows], local_sem.at[2]),
        pltpu.make_async_copy(small_ref, small_full.at[own_at], local_sem.at[3]),
    ]

    for side, link in ((1, "right"), (-1, "left")):
        @pl.when(sides[side])
        def _(link=link):
            each(dense_copies(z, x, y, link, True), "start")
    for link in ("x", "y", "core"):
        each(dense_copies(z, x, y, link, True), "start")
    send_own(0)
    each(local, "start")

    def x_arrived(row):
        each(dense_copies(row, 1 - x, y, "x"), "wait_recv")
        each(dense_copies(row, 1 - x, y, "y"), "start")
        each(dense_copies(row, 1 - x, y, "core"), "start")

    for s in (1, 2, 3):
        for side, link in ((1, "right"), (-1, "left")):
            row = z - side * s
            there = (z >= s) if side > 0 else (z + s <= 3)

            @pl.when(there)
            def _(row=row, side=side, link=link):
                each(dense_copies(row, x, y, link), "wait_recv")

                @pl.when(sides[side])
                def _():
                    each(dense_copies(row, x, y, link), "start")

                for other in ("x", "y", "core"):
                    each(dense_copies(row, x, y, other), "start")
        if s == 1:
            x_arrived(z)
        if s < 3:
            send_own(s)
    for s in (1, 2, 3):
        for row, there in ((z - s, z >= s), (z + s, z + s <= 3)):
            @pl.when(there)
            def _(row=row):
                x_arrived(row)
    for s in range(4):
        for column in range(2):
            row = lax.rem(z + s, 4)
            each(dense_copies(row, column, 1 - y, "y"), "wait_recv")
            each(dense_copies(row, column, 1 - y, "core"), "start")

    def pass_on(c, s):
        for side in (1, -1):
            row = z - side * s
            there = (z >= s) if side > 0 else (z + s <= 3)

            @pl.when(there)
            def _(row=row, side=side):
                copy_z(c, row, side).wait_recv()

                @pl.when(sides[side])
                def _():
                    copy_z(c, row, side).start()

                copy_x(c, row).start()

    for c in range(3):
        pass_on(c, 1)

    for row in range(4):
        for column in range(2):
            for line in range(2):
                at = slot(row, column, line, 1 - core)
                rows = pl.ds(pl.multiple_of(at * share, share), share)
                index = row * 4 + column * 2 + line
                for part, ref in enumerate((dense_full.at[:, rows], small_full.at[at])):
                    pltpu.make_async_remote_copy(
                        src_ref=ref,
                        dst_ref=ref,
                        send_sem=d_send.at[part, 2, index],
                        recv_sem=d_recv.at[part, 2, index],
                        device_id=device_at(z, x, y, 1 - core),
                        device_id_type=pl.DeviceIdType.MESH,
                    ).wait_recv()
    each(local, "wait")

    width = dense_full.shape[2]
    lane = lax.broadcasted_iota(jnp.int32, (small_full.shape[0], width), 1)
    line_of = lax.broadcasted_iota(jnp.int32, (small_full.shape[0], width), 0)
    gain_parts = small_full[:, 1, 0:share]
    spread = (
        lax.broadcasted_iota(jnp.int32, (share, width), 1) % share
        == lax.broadcasted_iota(jnp.int32, (share, width), 0)
    ).astype(F32)
    wide = jnp.dot(gain_parts, spread, precision=HIGHEST, preferred_element_type=F32)
    gain = jnp.sum(jnp.where(lane // share == line_of, wide, 0.0), 0, keepdims=True)
    bias_parts = small_full[:, 2, 0 : BUCKETS // 2]
    low = jnp.dot(bias_parts, hits_ref[: BUCKETS // 2], precision=HIGHEST, preferred_element_type=F32)
    high = jnp.dot(bias_parts, hits_ref[BUCKETS // 2 :], precision=HIGHEST, preferred_element_type=F32)
    for head in range(HEADS):
        table_ref[head : head + 1] = low[2 * head : 2 * head + 1] + high[2 * head + 1 : 2 * head + 2]
    seqlen = tokens_ref.shape[0]
    step = 128

    @pl.loop(0, seqlen // step)
    def _(i):
        at = pl.ds(pl.multiple_of(i * step, step), step)
        hidden_ref[at] = normed(tokens_ref[at].astype(F32), gain).astype(BF)

    tile = 256
    for part in range(3):
        @pl.loop(0, width // tile)
        def _(n, part=part):
            at = pl.ds(pl.multiple_of(n * tile, tile), tile)
            out = jnp.dot(hidden_ref[...], dense_full[part, :, at], preferred_element_type=F32)
            at = pl.ds(pl.multiple_of(part * width + n * tile, tile), tile)
            projected_ref[:, at] = out.astype(BF)

    prefix = prefix_ref[0]

    @pl.loop(0, HEADS // 2)
    def _(pair):
        def window(part):
            return pl.ds(pl.multiple_of(part * width + pair * 128, 128), 128)

        query_ref = projected_ref.at[:, window(0)]
        key_ref = projected_ref.at[:, window(1)]
        value_ref = projected_ref.at[:, window(2)]
        out_ref = attended_ref.at[:, window(0)]
        for head in range(2):
            lanes = slice(head * HEAD_DIM, (head + 1) * HEAD_DIM)
            rows = bias_rows(table_ref[pl.ds(2 * pair + head, 1), :], seqlen)
            key, value = key_ref[:, lanes], value_ref[:, lanes]
            for block in range(seqlen // 128):
                at = slice(128 * block, 128 * (block + 1))
                probs = probabilities(query_ref[at, lanes], key, rows, prefix, block, seqlen)
                out = jnp.dot(probs.astype(BF), value, preferred_element_type=F32)
                out_ref[at, lanes] = out.astype(BF)

        for c in range(3):
            for s in (2, 3):
                @pl.when(pair == 3 * (s - 2) + c + 1)
                def _(c=c, s=s):
                    pass_on(c, s)

    @pl.loop(0, width // tile)
    def _(n):
        at = pl.ds(pl.multiple_of(n * tile, tile), tile)
        out = jnp.dot(attended_ref[...], dense_full[3, :, at], preferred_element_type=F32)
        residual_ref[:, at] = tokens_ref[:, at].astype(F32) + out

    for row in range(4):
        for column in range(2):
            for line in range(2):
                each(dense_copies(row, column, line, "core"), "wait_send")
        for column in range(2):
            each(dense_copies(row, column, y, "y"), "wait_send")
        each(dense_copies(row, x, y, "x"), "wait_send")
        for side, link in ((1, "right"), (-1, "left")):
            sent = sides[side] & ((row <= z) if side > 0 else (row >= z))

            @pl.when(sent)
            def _(row=row, side=side, link=link):
                each(dense_copies(row, x, y, link), "wait_send")
                for c in range(3):
                    copy_z(c, row, side).wait_send()
        for c in range(3):
            copy_x(c, row).wait_recv()
            copy_x(c, row).wait_send()


def gather_weights(up, down, dense, small, tokens, hits, prefix):
    seqlen, width = tokens.shape
    devices = lax.axis_size(BOTH)
    slices = lax.axis_size("dp")
    vmem, hbm = pl.BlockSpec(memory_space=pltpu.VMEM), pl.BlockSpec(memory_space=pl.ANY)
    dma = pltpu.SemaphoreType.DMA
    return pl.pallas_call(
        gather_kernel,
        in_specs=[vmem] * 6 + [pl.BlockSpec(memory_space=pltpu.SMEM)],
        out_specs=[hbm] * 3 + [vmem] * 7,
        out_shape=[
            jax.ShapeDtypeStruct((slices,) + up.shape[1:], BF),
            jax.ShapeDtypeStruct((slices,) + up.shape[1:], BF),
            jax.ShapeDtypeStruct((slices,) + down.shape, BF),
            jax.ShapeDtypeStruct((dense.shape[0], devices * dense.shape[1], dense.shape[2]), BF),
            jax.ShapeDtypeStruct((devices,) + small.shape, F32),
            jax.ShapeDtypeStruct((seqlen, width), BF),
            jax.ShapeDtypeStruct((seqlen, 3 * width), BF),
            jax.ShapeDtypeStruct((seqlen, width), BF),
            jax.ShapeDtypeStruct((seqlen, width), F32),
            jax.ShapeDtypeStruct((HEADS, hits.shape[1]), F32),
        ],
        scratch_shapes=[
            dma((5,)),
            dma((3, 2, 4)),
            dma((3, 4)),
            dma((3, 4)),
            dma((3, 4)),
            dma((2, 2, 4)),
            dma((2, 4)),
            dma((2, 3, 16)),
            dma((2, 3, 16)),
        ],
        compiler_params=pltpu.CompilerParams(collective_id=1, has_side_effects=True, vmem_limit_bytes=60 * 2**20),
        name="gather_weights",
    )(up, down, dense, small, tokens, hits, prefix)


def reduce_kernel(
    gate_grads,
    up_grads,
    down_grads,
    dense_ref,
    hidden_turned,
    attended_turned,
    branch_ref,
    projected_ref,
    table_ref,
    prefix_ref,
    up_out,
    down_out,
    dense_out,
    hidden_grad,
    bias_ref,
    wide_got,
    tall_got,
    wide_line,
    tall_line,
    wide_own,
    tall_own,
    grads_ref,
    upstream_ref,
    full_ref,
    core_got,
    y_got,
    x_got,
    line_got,
    own_sem,
    x_send,
    x_recv,
    z_send,
    z_recv,
    core_send,
    core_recv,
    y_send,
    y_recv,
    dx_send,
    dx_recv,
):
    z, x, y, core = where_am_i()
    greet(z, x, y, core)
    mesh_id = pl.DeviceIdType.MESH
    share = dense_out.shape[1]
    parts, width = full_ref.shape[0], full_ref.shape[2]
    grads = (gate_grads, up_grads, down_grads)

    def got(c, row):
        return wide_got.at[c, row] if c < 2 else tall_got.at[row] if c == 2 else x_got.at[row]

    def line(c, place):
        return wide_line.at[c, place] if c < 2 else tall_line.at[place] if c == 2 else line_got.at[place]

    def own(c):
        return wide_own.at[c] if c < 2 else tall_own

    def load(c, row):
        return pltpu.make_async_copy(grads[c].at[2 * row + x], own(c), own_sem.at[c])

    def copy_x(c, row):
        return pltpu.make_async_remote_copy(
            src_ref=grads[c].at[2 * row + 1 - x],
            dst_ref=got(c, row),
            send_sem=x_send.at[c, row],
            recv_sem=x_recv.at[c, row],
            device_id=device_at(z, 1 - x, y, core),
            device_id_type=mesh_id,
        )

    def copy_z(c, row, side, place):
        return pltpu.make_async_remote_copy(
            src_ref=got(c, row),
            dst_ref=line(c, place),
            send_sem=z_send.at[c, row],
            recv_sem=z_recv.at[c, place],
            device_id=device_at(z + side, x, y, core),
            device_id_type=mesh_id,
        )

    def add(out, terms):
        shape = out.shape
        if len(shape) == 3:
            @pl.loop(0, shape[0])
            def _(i):
                total = functools.reduce(jnp.add, [term[i].astype(F32) for term in terms])
                out[i] = total.astype(out.dtype)
        else:
            @pl.loop(0, shape[0] // 16)
            def _(i):
                at = pl.ds(pl.multiple_of(i * 16, 16), 16)
                total = functools.reduce(jnp.add, [term[at].astype(F32) for term in terms])
                out[at] = total.astype(out.dtype)

    there = {}
    for s in (3, 2, 1):
        there[s, 1] = z + s <= 3
        there[s, -1] = z >= s
    order = [(s, side) for s in (3, 2, 1) for side in (1, -1)]

    def row_of(s, side):
        return lax.rem(z + side * s + 4, 4)

    def step(c, s, side):
        row = row_of(s, side)

        def run():
            if c < 3:
                copy_x(c, row).wait_recv()
            terms = [got(c, row)] + ([own(c)] if c < 3 else [])
            before = (z > 0) if side > 0 else (z < 3)

            @pl.when(before)
            def _():
                copy_z(c, row, side, row).wait_recv()
                add(got(c, row), terms + [line(c, row)])

            if c < 3:
                @pl.when(jnp.logical_not(before))
                def _():
                    add(got(c, row), terms)

            copy_z(c, row, side, 4 if (s == 1 and side < 0) else row).start()

        if c < 3:
            load(c, row).wait()
        pl.when(there[s, side])(run)
        if c < 3:
            index = order.index((s, side)) + 1
            load(c, row_of(*order[index]) if index < len(order) else z).start()

    def last(c, out):
        if c < 3:
            copy_x(c, z).wait_recv()
            load(c, z).wait()
            add(out, [got(c, z), own(c)])
        else:
            add(out, [got(c, z)])

        @pl.when(z > 0)
        def _():
            copy_z(c, z, 1, z).wait_recv()
            add(out, [out, line(c, z)])

        @pl.when(z < 3)
        def _():
            copy_z(c, z, -1, 4).wait_recv()
            add(out, [out, line(c, 4)])

    for s, side in order:
        @pl.when(there[s, side])
        def _(s=s, side=side):
            for c in range(3):
                copy_x(c, row_of(s, side)).start()
    for c in range(3):
        load(c, row_of(3, 1)).start()

    turned = (((1,), (1,)), ((), ()))
    flip = (((0,), (0,)), ((), ()))
    tile = 256

    @pl.loop(0, width // tile)
    def _(n):
        at = pl.ds(pl.multiple_of(n * tile, tile), tile)
        out = lax.dot_general(
            branch_ref[...], dense_ref[3, at, :], turned, preferred_element_type=F32
        )
        upstream_ref[:, at] = out.astype(BF)
        out = jnp.dot(attended_turned[...], branch_ref[:, at], preferred_element_type=F32)
        full_ref[3, :, at] = out.astype(BF)

    seqlen = projected_ref.shape[0]
    blocks = seqlen // 128
    prefix = prefix_ref[0]

    def attend_pair(pair):
        def window(part):
            return pl.ds(pl.multiple_of(part * width + pair * 128, 128), 128)

        for head in range(2):
            lanes = slice(head * HEAD_DIM, (head + 1) * HEAD_DIM)
            rows = bias_rows(table_ref[pl.ds(2 * pair + head, 1), :], seqlen)
            query = projected_ref.at[:, window(0)][:, lanes]
            key = projected_ref.at[:, window(1)][:, lanes]
            value = projected_ref.at[:, window(2)][:, lanes]
            upstream = upstream_ref.at[:, window(0)][:, lanes]
            probs_low, scores_low, scores = [], [], []
            for block in range(blocks):
                at = slice(128 * block, 128 * (block + 1))
                probs = probabilities(query[at], key, rows, prefix, block, seqlen)
                probs_grad = lax.dot_general(
                    upstream[at], value, turned, preferred_element_type=F32
                )
                inner = jnp.sum(probs * probs_grad, -1, keepdims=True)
                low = (probs * (probs_grad - inner)).astype(BF)
                probs_low.append(probs.astype(BF))
                scores_low.append(low)
                scores.append(low.astype(F32))
                out = jnp.dot(low, key, preferred_element_type=F32) * 0.125
                grads_ref.at[:, window(0)][at, lanes] = out.astype(BF)
            probs_all = jnp.concatenate(probs_low, 0)
            scores_all = jnp.concatenate(scores_low, 0)
            out = lax.dot_general(probs_all, upstream, flip, preferred_element_type=F32)
            grads_ref.at[:, window(2)][:, lanes] = out.astype(BF)
            out = lax.dot_general(scores_all, query, flip, preferred_element_type=F32) * 0.125
            grads_ref.at[:, window(1)][:, lanes] = out.astype(BF)
            bias_ref[pl.ds(2 * pair + head, 1)] = diagonals(scores)[None]

    @pl.loop(0, HEADS // 2)
    def _(pair):
        attend_pair(pair)
        for c, when in ((0, 3), (1, 7)):
            @pl.when(pair == when)
            def _(c=c):
                step(c, 3, 1)
                step(c, 3, -1)

    for part in range(3):
        @pl.loop(0, width // tile)
        def _(n, part=part):
            at = pl.ds(pl.multiple_of(n * tile, tile), tile)
            from_at = pl.ds(pl.multiple_of(part * width + n * tile, tile), tile)
            out = jnp.dot(hidden_turned[...], grads_ref[:, from_at], preferred_element_type=F32)
            full_ref[part, :, at] = out.astype(BF)

    def rows_of(k, number):
        at = (k // 2) * 4 + (k % 2) * 2 + number
        return pl.ds(pl.multiple_of(at * share, share), share)

    def copy_core(k):
        return pltpu.make_async_remote_copy(
            src_ref=full_ref.at[:, rows_of(k, 1 - core)],
            dst_ref=core_got.at[k],
            send_sem=core_send.at[k],
            recv_sem=core_recv.at[k],
            device_id=device_at(z, x, y, 1 - core),
            device_id_type=mesh_id,
        )

    def copy_y(k):
        return pltpu.make_async_remote_copy(
            src_ref=core_got.at[2 * k + 1 - y],
            dst_ref=y_got.at[k],
            send_sem=y_send.at[k],
            recv_sem=y_recv.at[k],
            device_id=device_at(z, x, 1 - y, core),
            device_id_type=mesh_id,
        )

    def copy_dx(row):
        return pltpu.make_async_remote_copy(
            src_ref=y_got.at[2 * row + 1 - x],
            dst_ref=x_got.at[row],
            send_sem=dx_send.at[row],
            recv_sem=dx_recv.at[row],
            device_id=device_at(z, 1 - x, y, core),
            device_id_type=mesh_id,
        )

    @pl.loop(0, 16)
    def _(k):
        copy_core(k).start()

    step(2, 3, 1)
    step(2, 3, -1)

    @pl.loop(0, width // tile)
    def _(n):
        at = pl.ds(pl.multiple_of(n * tile, tile), tile)
        total = None
        for part in range(3):
            out = lax.dot_general(
                grads_ref[:, part * width : (part + 1) * width],
                dense_ref[part, at, :],
                turned,
                preferred_element_type=F32,
            )
            total = out if total is None else total + out
        hidden_grad[:, at] = total

    @pl.loop(0, 8)
    def _(k):
        for line_y in range(2):
            copy_core(2 * k + line_y).wait_recv()
            for part in range(parts):
                mine = full_ref.at[part, rows_of(2 * k + line_y, core)]
                other = core_got.at[2 * k + line_y, part]
                other[...] = (other[...].astype(F32) + mine[...].astype(F32)).astype(BF)
        copy_y(k).start()

    for c in range(3):
        step(c, 2, 1)
        step(c, 2, -1)
    step(0, 1, 1)
    step(0, 1, -1)

    @pl.loop(0, 4)
    def _(row):
        for column in range(2):
            k = 2 * row + column
            copy_y(k).wait_recv()
            for part in range(parts):
                mine, other = core_got.at[2 * k + y, part], y_got.at[k, part]
                other[...] = (other[...].astype(F32) + mine[...].astype(F32)).astype(BF)
        copy_dx(row).start()

    for c in range(3):
        copy_x(c, z).start()
    for c in (1, 2):
        step(c, 1, 1)
        step(c, 1, -1)

    @pl.loop(0, 4)
    def _(row):
        copy_dx(row).wait_recv()
        for part in range(parts):
            mine, other = y_got.at[2 * row + x, part], x_got.at[row, part]
            other[...] = (other[...].astype(F32) + mine[...].astype(F32)).astype(BF)

    for s, side in order:
        step(3, s, side)
    last(0, up_out.at[0])
    last(1, up_out.at[1])
    last(3, dense_out)
    last(2, down_out)

    @pl.loop(0, 16)
    def _(k):
        copy_core(k).wait_send()

    @pl.loop(0, 8)
    def _(k):
        copy_y(k).wait_send()

    @pl.loop(0, 4)
    def _(row):
        copy_dx(row).wait_send()
        for c in range(3):
            copy_x(c, row).wait_send()

    for s, side in order:
        @pl.when(there[s, side])
        def _(s=s, side=side):
            for c in range(4):
                copy_z(c, row_of(s, side), side, row_of(s, side)).wait_send()


def reduce_weights(gate, up, down, dense, hidden, attended, branch, projected, table, prefix):
    seqlen, width = hidden.shape
    share = width // lax.axis_size(BOTH)
    vmem, hbm = pl.BlockSpec(memory_space=pltpu.VMEM), pl.BlockSpec(memory_space=pl.ANY)
    dma = pltpu.SemaphoreType.DMA
    wide, tall = gate.shape[1:], down.shape[1:]
    dense_shape = (dense.shape[0], share, width)
    return pl.pallas_call(
        reduce_kernel,
        in_specs=[hbm] * 3 + [vmem] * 6 + [pl.BlockSpec(memory_space=pltpu.SMEM)],
        out_specs=[vmem] * 5,
        out_shape=[
            jax.ShapeDtypeStruct((2,) + wide, F32),
            jax.ShapeDtypeStruct(tall, F32),
            jax.ShapeDtypeStruct(dense_shape, F32),
            jax.ShapeDtypeStruct((seqlen, width), F32),
            jax.ShapeDtypeStruct((HEADS, 8, table.shape[1]), F32),
        ],
        scratch_shapes=[
            pltpu.VMEM((2, 4) + wide, BF),
            pltpu.VMEM((4,) + tall, BF),
            pltpu.VMEM((2, 5) + wide, BF),
            pltpu.VMEM((5,) + tall, BF),
            pltpu.VMEM((2,) + wide, BF),
            pltpu.VMEM(tall, BF),
            pltpu.VMEM((seqlen, 3 * width), BF),
            pltpu.VMEM((seqlen, width), BF),
            pltpu.VMEM(dense.shape, BF),
            pltpu.VMEM((16,) + dense_shape, BF),
            pltpu.VMEM((8,) + dense_shape, BF),
            pltpu.VMEM((4,) + dense_shape, BF),
            pltpu.VMEM((5,) + dense_shape, BF),
            dma((3,)),
            dma((3, 4)),
            dma((3, 4)),
            dma((4, 4)),
            dma((4, 5)),
            dma((16,)),
            dma((16,)),
            dma((8,)),
            dma((8,)),
            dma((4,)),
            dma((4,)),
        ],
        compiler_params=pltpu.CompilerParams(
            collective_id=2, has_side_effects=True, vmem_limit_bytes=67043328
        ),
        name="reduce_weights",
    )(gate, up, down, dense, hidden.T, attended.T, branch, projected, table, prefix)


def on_device(
    tokens,
    cotangent,
    routes,
    prefix,
    buckets,
    step_count,
    learn_rate,
    weight_decay,
    attend_master,
    attend_first,
    attend_second,
    outward_master,
    outward_first,
    outward_second,
    router_master,
    router_first,
    router_second,
    gains_master,
    gains_first,
    gains_second,
    bias_master,
    bias_first,
    bias_second,
    upward_master,
    upward_first,
    upward_second,
    downward_master,
    downward_first,
    downward_second,
):
    devices = lax.axis_size(BOTH)
    share = attend_master.shape[1]
    seqlen = tokens.shape[0]
    experts = router_master.shape[1]
    capacity = seqlen * TOP * 5 // (4 * experts)

    slices = lax.axis_size("dp")
    router_size, gains_size = router_master.size, gains_master.size
    bucket_hits = (buckets[:, None] == jnp.arange(BUCKETS, dtype=jnp.int32)[None, :]).astype(F32)
    offsets = buckets.shape[0]
    inputs = tokens.astype(F32)
    if is_line():
        hits_wide = jnp.pad(bucket_hits.T, ((0, 0), (0, 2 * seqlen - offsets)))
        small = jnp.concatenate(
            [
                jnp.pad(one.reshape(1, -1), ((0, 0), (0, 128 - one.size)))
                for one in (router_master, gains_master, bias_master)
            ]
            + [jnp.zeros((5, 128), F32)]
        )
        dense = jnp.concatenate([attend_master.astype(BF), outward_master.astype(BF)[None]])
        (
            gate_w,
            up_w,
            downward_w,
            dense_w,
            small,
            hidden_one,
            projected,
            attended,
            residual,
            table,
        ) = gather_weights(
            upward_master[:, 0].astype(BF),
            downward_master[0].astype(BF),
            dense,
            small,
            tokens,
            hits_wide,
            prefix,
        )
        attend_w, outward_w = dense_w[:3], dense_w[3]
        gate_w, up_w = gate_w.reshape(D, FF), up_w.reshape(D, FF)
        downward_w = downward_w.reshape(FF, D)
        router_w = small[:, 0].reshape(D, experts)
        gains_w = small[:, 1, :gains_size].reshape(devices, 2, share).transpose(1, 0, 2).reshape(2, D)
        table = table.reshape(HEADS // 2, 2, 2 * seqlen)
        first_pull = jax.vjp(normed, inputs, gains_w[0])[1]
    else:
        gate_w = gather_dp(upward_master[0, 0].astype(BF)).reshape(D, FF)
        up_w = gather_dp(upward_master[1, 0].astype(BF)).reshape(D, FF)
        downward_w = gather_dp(downward_master[0].astype(BF)).reshape(FF, D)
        attend_w = lax.all_gather(attend_master.astype(BF), BOTH, axis=1, tiled=True)
        outward_w = lax.all_gather(outward_master.astype(BF), BOTH, axis=0, tiled=True)
        router_w = lax.all_gather(router_master, BOTH, axis=0, tiled=True)
        gains_w = lax.all_gather(gains_master, BOTH, axis=1, tiled=True)
        bias_w = lax.all_gather(bias_master, BOTH, axis=0, tiled=True)
        table = jnp.dot(bias_w.reshape(HEADS, BUCKETS), bucket_hits.T, precision=HIGHEST)
        table = jnp.pad(table, ((0, 0), (0, 2 * seqlen - offsets)))
        table = table.reshape(HEADS // 2, 2, 2 * seqlen)
        first_normed, first_pull = jax.vjp(normed, inputs, gains_w[0])
        hidden_one = first_normed.astype(BF)
        projected = jnp.concatenate(
            [
                jnp.dot(hidden_one, attend_w[part], preferred_element_type=F32).astype(BF)
                for part in range(3)
            ],
            1,
        )
        attended = attend(prefix, table, projected)
        residual = inputs + jnp.dot(attended, outward_w, preferred_element_type=F32)

    kinds = jnp.arange(experts, dtype=jnp.int32)
    route_hits = (routes[:, :, None] == kinds[None, None, :]).astype(F32)

    def gate_piece(residual_in, scale_gain, router_in):
        second_normed = normed(residual_in, scale_gain)
        logits = jnp.dot(second_normed, router_in, precision=HIGHEST)
        router_soft = jax.nn.softmax(logits, axis=-1)
        chosen = jnp.sum(router_soft[:, None, :] * route_hits, -1)
        return (second_normed, chosen / jnp.sum(chosen, -1, keepdims=True))

    (second_normed, combine), gate_pull = jax.vjp(gate_piece, residual, gains_w[1], router_w)
    second_low = second_normed.astype(BF)

    hits = jnp.sum(route_hits, 1)
    places = jnp.arange(seqlen, dtype=jnp.int32)
    earlier = (places[None, :] < places[:, None]).astype(BF)
    rank = jnp.dot(earlier, hits.astype(BF), preferred_element_type=F32)
    rank = jnp.where(hits > 0, rank, -1.0).astype(jnp.int32)
    slots = jnp.arange(capacity, dtype=jnp.int32)
    taken = rank.T[:, None, :] == slots[None, :, None]
    choose = taken.astype(BF).reshape(experts * capacity, seqlen)
    weight = jnp.sum(combine[:, :, None] * route_hits, 1)
    slot_weight = jnp.sum(jnp.where(taken, weight.T[:, None, :], 0.0), -1)
    backs = [
        (
            (rank[:, :, None] == slots[None, None, :])
            & (routes[:, k][:, None, None] == kinds[None, :, None])
        )
        .astype(BF)
        .reshape(seqlen, experts * capacity)
        for k in range(TOP)
    ]
    back = (rank[:, :, None] == slots[None, None, :]).astype(BF)
    back = back.reshape(seqlen, experts * capacity)

    def exchange(rows, home):
        if home:
            rows = rows.reshape(1, experts, capacity, D)
            rows = lax.all_to_all(rows, "expert", split_axis=1, concat_axis=0, tiled=True)
        else:
            rows = rows.reshape(experts, 1, capacity, D)
            rows = lax.all_to_all(rows, "expert", split_axis=0, concat_axis=1, tiled=True)
        return rows.reshape(experts * capacity, D)

    sent_rows = jnp.dot(choose, second_low, preferred_element_type=F32).astype(BF)
    upstream_rows = jnp.dot(choose, cotangent, preferred_element_type=F32)
    grad_rows = (slot_weight.reshape(-1, 1) * upstream_rows).astype(BF)
    sent_rows, grad_rows = lax.optimization_barrier((sent_rows, grad_rows))
    arrived = exchange(sent_rows, False)
    grad_arrived = exchange(grad_rows, False)

    gate_value = jnp.dot(arrived, gate_w, preferred_element_type=F32)
    up_value = jnp.dot(arrived, up_w, preferred_element_type=F32)
    gelu_value, gelu_pull = jax.vjp(gelu_tanh, gate_value)
    hidden_mid = (gelu_value * up_value).astype(BF)
    expert_out = jnp.dot(hidden_mid, downward_w, preferred_element_type=F32).astype(BF)
    returned = exchange(expert_out, True)

    turned = (((1,), (1,)), ((), ()))
    flipped = (((0,), (0,)), ((), ()))
    grad_mid = lax.dot_general(grad_arrived, downward_w, turned, preferred_element_type=F32)
    grad_gate = gelu_pull(grad_mid * up_value)[0].astype(BF)
    grad_up = (grad_mid * gelu_value).astype(BF)
    grad_sent = lax.dot_general(grad_gate, gate_w, turned, preferred_element_type=F32)
    grad_sent = grad_sent + lax.dot_general(grad_up, up_w, turned, preferred_element_type=F32)
    grad_sent, returned, grad_gate, grad_up, hidden_mid = lax.optimization_barrier(
        (grad_sent.astype(BF), returned, grad_gate, grad_up, hidden_mid)
    )
    grad_home = exchange(grad_sent, True)


    def weight_grad(left, right):
        full = lax.dot_general(left, right, flipped, preferred_element_type=F32).astype(BF)
        return full.reshape(slices, -1, full.shape[1])

    wide_grads = (
        weight_grad(arrived, grad_gate),
        weight_grad(arrived, grad_up),
        weight_grad(hidden_mid, grad_arrived),
    )

    came_back = jnp.stack(
        [jnp.dot(one, returned, preferred_element_type=F32) for one in backs], 1
    )
    expert_sum = jnp.sum(combine[..., None] * came_back, 1)
    block_output = (residual + expert_sum).astype(BF)
    upstream = cotangent.astype(F32)
    combine_grad = jnp.sum(upstream[:, None, :] * came_back, -1)

    grad_normed = jnp.dot(back, grad_home, preferred_element_type=F32)
    residual_part, gain_two_grad, router_full = gate_pull((grad_normed, combine_grad))
    grad_residual = upstream + residual_part
    grad_branch = grad_residual.astype(BF)
    if is_line():
        upward_g, downward_g, dense_g, grad_hidden_one, bias_parts = reduce_weights(
            *wide_grads,
            dense_w,
            hidden_one,
            attended,
            grad_branch,
            projected,
            table.reshape(HEADS, 2 * seqlen),
            prefix,
        )
        attend_g, outward_g = dense_g[:3], dense_g[3]
        upward_g, downward_g = upward_g[:, None], downward_g[None]
    else:
        upward_g = jnp.stack([scatter_dp(one) for one in wide_grads[:2]])[:, None]
        downward_g = scatter_dp(wide_grads[2])[None]
        outward_full = lax.dot_general(attended, grad_branch, flipped, preferred_element_type=F32)
        outward_g = scatter_all(outward_full.astype(BF).reshape(devices, share, D))
        grad_attended = lax.dot_general(grad_branch, outward_w, turned, preferred_element_type=F32)
        query_grad, key_grad, value_grad, bias_parts = attend_back(
            prefix, table, projected, grad_attended.astype(BF)
        )
        projected_grads = (query_grad, key_grad, value_grad)
        attend_g = scatter_all(
            jnp.concatenate(
                [
                    lax.dot_general(hidden_one, part, flipped, preferred_element_type=F32)
                    .astype(BF)
                    .reshape(devices, share, D)
                    for part in projected_grads
                ],
                1,
            )
        ).reshape(3, share, D)
        grad_hidden_one = functools.reduce(
            jnp.add,
            [
                lax.dot_general(part, attend_w[which], turned, preferred_element_type=F32)
                for which, part in enumerate(projected_grads)
            ],
        )

    inputs_part, gain_one_grad = first_pull(grad_hidden_one)
    input_grad = (grad_residual + inputs_part).astype(BF)

    bias_parts = bias_parts.reshape(HEADS, 8, 2 * seqlen)
    bias_parts = jnp.pad(bias_parts, ((0, 0), (0, 0), (0, 8)))
    per_offset = functools.reduce(
        jnp.add, [bias_parts[:, row, row : row + offsets] for row in range(8)]
    )
    bias_full = jnp.dot(per_offset, bucket_hits, precision=HIGHEST).reshape(-1)

    smalls = sum_all(
        jnp.concatenate([router_full.reshape(-1), gain_one_grad, gain_two_grad, bias_full])
    )
    place = lax.axis_index(BOTH)
    router_g = lax.dynamic_slice(smalls, (place * router_size,), (router_size,))
    router_g = router_g.reshape(share, experts)
    start = D * experts
    gains_g = jnp.stack(
        [
            lax.dynamic_slice(smalls, (start + row * D + place * share,), (share,))
            for row in range(2)
        ]
    )
    bias_g = lax.dynamic_slice(smalls, (start + 2 * D + place * bias_master.size,), bias_master.shape)

    grads_all = (attend_g, outward_g, router_g, gains_g, bias_g, upward_g, downward_g)
    squares = jnp.stack([jnp.sum(member_grad * member_grad) for member_grad in grads_all])
    totals = sum_all(squares)
    counts_all = jnp.array(
        [
            3 * D * D,
            D * D,
            D * experts,
            2 * D,
            HEADS * BUCKETS,
            2 * experts * D * FF,
            experts * FF * D,
        ],
        jnp.float32,
    )
    mean_squares = totals / counts_all
    grad_rms = jnp.sqrt(mean_squares)
    factors = lax.rsqrt(mean_squares + 1e-06)
    step_float = step_count.astype(jnp.float32)
    masters = (
        attend_master,
        outward_master,
        router_master,
        gains_master,
        bias_master,
        upward_master,
        downward_master,
    )
    firsts = (
        attend_first,
        outward_first,
        router_first,
        gains_first,
        bias_first,
        upward_first,
        downward_first,
    )
    seconds = (
        attend_second,
        outward_second,
        router_second,
        gains_second,
        bias_second,
        upward_second,
        downward_second,
    )
    flags = (True, True, True, False, False, True, True)
    updates = [
        adamw_update(
            masters[member],
            firsts[member],
            seconds[member],
            grads_all[member] * factors[member],
            step_float,
            learn_rate,
            weight_decay,
            flags[member],
        )
        for member in range(7)
    ]
    return (
        block_output,
        input_grad,
        grads_all[0],
        updates[0][0],
        updates[0][1],
        updates[0][2],
        grads_all[1],
        updates[1][0],
        updates[1][1],
        updates[1][2],
        grads_all[2],
        updates[2][0],
        updates[2][1],
        updates[2][2],
        grads_all[3],
        updates[3][3],
        updates[3][1],
        updates[3][2],
        grads_all[4],
        updates[4][3],
        updates[4][1],
        updates[4][2],
        grads_all[5],
        updates[5][0],
        updates[5][1],
        updates[5][2],
        grads_all[6],
        updates[6][0],
        updates[6][1],
        updates[6][2],
        grad_rms,
    )


def solution(mesh):
    placed = (
        P(("dp", "expert"), None),
        P(("dp", "expert"), None),
        P(("dp", "expert"), None),
        P(("dp", "expert")),
        P(),
        P(),
        P(),
        P(),
        P(None, ("dp", "expert"), None),
        P(None, ("dp", "expert"), None),
        P(None, ("dp", "expert"), None),
        P(("dp", "expert"), None),
        P(("dp", "expert"), None),
        P(("dp", "expert"), None),
        P(("dp", "expert"), None),
        P(("dp", "expert"), None),
        P(("dp", "expert"), None),
        P(None, ("dp", "expert")),
        P(None, ("dp", "expert")),
        P(None, ("dp", "expert")),
        P(("dp", "expert")),
        P(("dp", "expert")),
        P(("dp", "expert")),
        P(None, "expert", "dp", None),
        P(None, "expert", "dp", None),
        P(None, "expert", "dp", None),
        P("expert", "dp", None),
        P("expert", "dp", None),
        P("expert", "dp", None),
    )
    return jax.shard_map(
        on_device,
        mesh=mesh,
        in_specs=placed,
        out_specs=(
            P(("dp", "expert"), None),
            P(("dp", "expert"), None),
            P(None, ("dp", "expert"), None),
            P(None, ("dp", "expert"), None),
            P(None, ("dp", "expert"), None),
            P(None, ("dp", "expert"), None),
            P(("dp", "expert"), None),
            P(("dp", "expert"), None),
            P(("dp", "expert"), None),
            P(("dp", "expert"), None),
            P(("dp", "expert"), None),
            P(("dp", "expert"), None),
            P(("dp", "expert"), None),
            P(("dp", "expert"), None),
            P(None, ("dp", "expert")),
            P(None, ("dp", "expert")),
            P(None, ("dp", "expert")),
            P(None, ("dp", "expert")),
            P(("dp", "expert")),
            P(("dp", "expert")),
            P(("dp", "expert")),
            P(("dp", "expert")),
            P(None, "expert", "dp", None),
            P(None, "expert", "dp", None),
            P(None, "expert", "dp", None),
            P(None, "expert", "dp", None),
            P("expert", "dp", None),
            P("expert", "dp", None),
            P("expert", "dp", None),
            P("expert", "dp", None),
            P(),
        ),
        check_vma=False,
    )
```

```python
import functools

import jax
import jax.numpy as jnp
from jax import lax
from jax.experimental import pallas as pl
from jax.experimental.pallas import tpu as pltpu
from jax.sharding import PartitionSpec as P

D = 1024
HEADS = 16
HEAD_DIM = 64
FF = 2816
BUCKETS = 32
TOP = 2
BOTH = ("dp", "expert")
BF = jnp.bfloat16
F32 = jnp.float32

HIGHEST = lax.Precision.HIGHEST
MASKED = -1e30


def normed(values, scale_gain):
    return values * lax.rsqrt(jnp.mean(values * values, -1, keepdims=True) + 1e-06) * scale_gain


def gelu_tanh(values):
    return jax.nn.gelu(values, approximate=True)


def adamw_update(
    master, first_moment, second, gradient, step_float, learn_rate, weight_decay, decayed
):
    mean_new = 0.9 * first_moment + 0.1 * gradient
    square_new = 0.95 * second + 0.05 * gradient * gradient
    mean_hat = mean_new / (1.0 - jnp.power(jnp.float32(0.9), step_float))
    square_hat = square_new / (1.0 - jnp.power(jnp.float32(0.95), step_float))
    change = learn_rate * (mean_hat / (jnp.sqrt(square_hat) + 1e-08))
    updated = master - change
    if decayed:
        updated = updated - weight_decay * master
    return (updated, mean_new, square_new, -change)


def is_line():
    return lax.axis_size("dp") == 8 and lax.axis_size("expert") == 4


def gather_dp(shard):
    return lax.all_gather(shard, "dp", axis=0)


def scatter_dp(parts):
    return lax.psum_scatter(parts.astype(F32), "dp", scatter_dimension=0, tiled=False)


def scatter_all(parts):
    return lax.psum_scatter(parts.astype(F32), BOTH, scatter_dimension=0, tiled=False)


def bias_rows(table, seqlen):
    width = table.shape[-1]
    wide = jnp.broadcast_to(table, (128, width))
    return pltpu.roll(wide, width - 127, 1, stride=1, stride_axis=0)


def probabilities(query, key, rows, prefix, block, seqlen):
    blocks = seqlen // 128
    raw = (
        lax.dot_general(query, key, (((1,), (1,)), ((), ())), preferred_element_type=F32) * 0.125
    )
    start = 128 * (blocks - 1 - block)
    raw = raw + rows[:, start : start + seqlen]
    i = lax.broadcasted_iota(jnp.int32, raw.shape, 0) + 128 * block
    j = lax.broadcasted_iota(jnp.int32, raw.shape, 1)
    raw = jnp.where((j <= i) | (j < prefix), raw, MASKED)
    shifted = jnp.exp(raw - jnp.max(raw, -1, keepdims=True))
    return shifted / jnp.sum(shifted, -1, keepdims=True)


def attend_kernel(prefix_ref, table_ref, query_ref, key_ref, value_ref, out_ref):
    seqlen = query_ref.shape[0]
    prefix = prefix_ref[0]
    for head in range(2):
        lanes = slice(head * HEAD_DIM, (head + 1) * HEAD_DIM)
        rows = bias_rows(table_ref[0, head : head + 1, :], seqlen)
        key, value = key_ref[:, lanes], value_ref[:, lanes]
        for block in range(seqlen // 128):
            at = slice(128 * block, 128 * (block + 1))
            probs = probabilities(query_ref[at, lanes], key, rows, prefix, block, seqlen)
            out = jnp.dot(probs.astype(BF), value, preferred_element_type=F32)
            out_ref[at, lanes] = out.astype(BF)


def diagonals(scores):
    blocks = len(scores)
    columns = []
    for column in range(2 * blocks - 1):
        terms = []
        for block in range(blocks):
            piece = column - (blocks - 1 - block)
            if 0 <= piece < blocks:
                terms.append(scores[block][:, 128 * piece : 128 * (piece + 1)])
        columns.append(functools.reduce(jnp.add, terms))
    columns.append(jnp.zeros_like(columns[0]))
    wide = jnp.concatenate(columns, 1)
    total = jnp.zeros((8, wide.shape[1]), F32)
    for group in range(16):
        total = total + pltpu.roll(wide[8 * group : 8 * group + 8], 127 - 8 * group, 1)
    return total


def attend_back_kernel(
    prefix_ref,
    table_ref,
    query_ref,
    key_ref,
    value_ref,
    upstream_ref,
    query_grad_ref,
    key_grad_ref,
    value_grad_ref,
    bias_ref,
):
    seqlen = query_ref.shape[0]
    blocks = seqlen // 128
    prefix = prefix_ref[0]
    flip = (((0,), (0,)), ((), ()))
    for head in range(2):
        lanes = slice(head * HEAD_DIM, (head + 1) * HEAD_DIM)
        rows = bias_rows(table_ref[0, head : head + 1, :], seqlen)
        query, key, value = query_ref[:, lanes], key_ref[:, lanes], value_ref[:, lanes]
        upstream = upstream_ref[:, lanes]
        probs_low, scores_low, scores = [], [], []
        for block in range(blocks):
            at = slice(128 * block, 128 * (block + 1))
            probs = probabilities(query[at], key, rows, prefix, block, seqlen)
            probs_grad = lax.dot_general(
                upstream[at], value, (((1,), (1,)), ((), ())), preferred_element_type=F32
            )
            inner = jnp.sum(probs * probs_grad, -1, keepdims=True)
            low = (probs * (probs_grad - inner)).astype(BF)
            probs_low.append(probs.astype(BF))
            scores_low.append(low)
            scores.append(low.astype(F32))
            out = jnp.dot(low, key, preferred_element_type=F32) * 0.125
            query_grad_ref[at, lanes] = out.astype(BF)
        probs_all = jnp.concatenate(probs_low, 0)
        scores_all = jnp.concatenate(scores_low, 0)
        out = lax.dot_general(probs_all, upstream, flip, preferred_element_type=F32)
        value_grad_ref[:, lanes] = out.astype(BF)
        out = lax.dot_general(scores_all, query, flip, preferred_element_type=F32) * 0.125
        key_grad_ref[:, lanes] = out.astype(BF)
        bias_ref[0, head] = diagonals(scores)


def attention_specs(seqlen, width):
    pairs = HEADS // 2
    table = pl.BlockSpec((1, 2, width), lambda p: (p, 0, 0))
    return (
        [pl.BlockSpec(memory_space=pltpu.SMEM), table]
        + [
            pl.BlockSpec((seqlen, 128), lambda p, part=part: (0, part * pairs + p))
            for part in range(3)
        ],
        pl.BlockSpec((seqlen, 128), lambda p: (0, p)),
    )


def attend(prefix, table, projected):
    seqlen = projected.shape[0]
    ins, out = attention_specs(seqlen, table.shape[-1])
    return pl.pallas_call(
        attend_kernel,
        grid=(HEADS // 2,),
        in_specs=ins,
        out_specs=out,
        out_shape=jax.ShapeDtypeStruct((seqlen, D), BF),
        cost_estimate=pl.CostEstimate(
            flops=4 * seqlen * seqlen * D,
            bytes_accessed=8 * seqlen * D,
            transcendentals=HEADS * seqlen * seqlen,
        ),
        name="attend",
    )(prefix, table, projected, projected, projected)


def attend_back(prefix, table, projected, upstream):
    seqlen = projected.shape[0]
    width = table.shape[-1]
    ins, out = attention_specs(seqlen, width)
    grad = jax.ShapeDtypeStruct((seqlen, D), BF)
    return pl.pallas_call(
        attend_back_kernel,
        grid=(HEADS // 2,),
        in_specs=ins + [out],
        out_specs=[out, out, out, pl.BlockSpec((1, 2, 8, width), lambda p: (p, 0, 0, 0))],
        out_shape=[grad, grad, grad, jax.ShapeDtypeStruct((HEADS // 2, 2, 8, width), F32)],
        cost_estimate=pl.CostEstimate(
            flops=10 * seqlen * seqlen * D,
            bytes_accessed=14 * seqlen * D,
            transcendentals=HEADS * seqlen * seqlen,
        ),
        name="attend_back",
    )(prefix, table, projected, projected, projected, upstream)


def where_am_i():
    dp, expert = lax.axis_index("dp"), lax.axis_index("expert")
    return dp // 2, dp % 2, expert // 2, expert % 2


def device_at(z, x, y, core):
    return (2 * z + x, 2 * y + core)


def greet(z, x, y, core):
    barrier = pltpu.get_barrier_semaphore()

    def call(*place):
        pl.semaphore_signal(
            barrier, inc=1, device_id=device_at(*place), device_id_type=pl.DeviceIdType.MESH
        )

    call(z, 1 - x, y, core)
    call(z, x, 1 - y, core)
    call(z, x, y, 1 - core)
    call(z, x, 1 - y, 1 - core)

    @pl.when(z > 0)
    def _():
        call(z - 1, x, y, core)

    @pl.when(z < 3)
    def _():
        call(z + 1, x, y, core)

    pl.semaphore_wait(barrier, 4 + (z > 0).astype(jnp.int32) + (z < 3).astype(jnp.int32))


def gather_kernel(
    up_ref,
    down_ref,
    dense_ref,
    small_ref,
    tokens_ref,
    cotangent_ref,
    chosen_ref,
    hits_ref,
    prefix_ref,
    gate_full,
    up_full,
    down_full,
    dense_full,
    small_full,
    hidden_ref,
    projected_ref,
    attended_ref,
    residual_ref,
    table_ref,
    arrived_ref,
    grads_ref,
    second_ref,
    rows_ref,
    local_sem,
    z_send,
    z_recv,
    x_send,
    x_recv,
    dz_send,
    dz_recv,
    d_send,
    d_recv,
    turn_send,
    turn_recv,
    a_send,
    a_recv,
):
    z, x, y, core = where_am_i()
    greet(z, x, y, core)
    share = dense_ref.shape[1]
    sides = {1: z < 3, -1: z > 0}

    def piece(c, row, column):
        return (gate_full, up_full, down_full)[c].at[2 * row + column]

    def mine(c):
        return up_ref.at[c] if c < 2 else down_ref

    def copy_z(c, row, side, own=False):
        return pltpu.make_async_remote_copy(
            src_ref=mine(c) if own else piece(c, row, x),
            dst_ref=piece(c, row, x),
            send_sem=z_send.at[c, (side + 1) // 2, row],
            recv_sem=z_recv.at[c, row],
            device_id=device_at(z + side, x, y, core),
            device_id_type=pl.DeviceIdType.MESH,
        )

    def copy_x(c, row, own=False):
        return pltpu.make_async_remote_copy(
            src_ref=mine(c) if own else piece(c, row, x),
            dst_ref=piece(c, row, x),
            send_sem=x_send.at[c, row],
            recv_sem=x_recv.at[c, row],
            device_id=device_at(z, 1 - x, y, core),
            device_id_type=pl.DeviceIdType.MESH,
        )

    inner = (z == 1) | (z == 2)
    inward, outward = jnp.where(z == 1, 1, -1), jnp.where(z == 1, -1, 1)
    outer_row = jnp.where(z == 1, 3, 0)

    def copy_turn(row, side, number):
        return pltpu.make_async_remote_copy(
            src_ref=piece(0, row, 1 - x),
            dst_ref=piece(0, row, 1 - x),
            send_sem=turn_send.at[number],
            recv_sem=turn_recv.at[0],
            device_id=device_at(z + side, x, y, core),
            device_id_type=pl.DeviceIdType.MESH,
        )

    def send_own(c):
        for side in (1, -1):
            @pl.when(sides[side])
            def _(side=side):
                copy_z(c, z, side, True).start()
        copy_x(c, z, True).start()

    def slot(row, column, line, number):
        return row * 8 + column * 4 + line * 2 + number

    def dense_copies(row, column, line, link, own=False):
        at = slot(row, column, line, core)
        target, sems, index = {
            "right": (device_at(z + 1, x, y, core), dz_send, (1, row)),
            "left": (device_at(z - 1, x, y, core), dz_send, (0, row)),
            "x": (device_at(z, 1 - x, y, core), d_send, (0, row)),
            "y": (device_at(z, x, 1 - y, core), d_send, (1, row * 2 + column)),
            "core": (device_at(z, x, y, 1 - core), d_send, (2, row * 4 + column * 2 + line)),
        }[link]
        if sems is dz_send:
            recv, place = dz_recv, (row,)
        else:
            recv, place = d_recv, index
        rows = pl.ds(pl.multiple_of(at * share, share), share)
        return [
            pltpu.make_async_remote_copy(
                src_ref=dense_ref if own else dense_full.at[:, rows],
                dst_ref=dense_full.at[:, rows],
                send_sem=sems.at[(0,) + index],
                recv_sem=recv.at[(0,) + place],
                device_id=target,
                device_id_type=pl.DeviceIdType.MESH,
            ),
            pltpu.make_async_remote_copy(
                src_ref=small_ref if own else small_full.at[at],
                dst_ref=small_full.at[at],
                send_sem=sems.at[(1,) + index],
                recv_sem=recv.at[(1,) + place],
                device_id=target,
                device_id_type=pl.DeviceIdType.MESH,
            ),
        ]

    def each(copies, step):
        for copy in copies:
            getattr(copy, step)()

    own_at = slot(z, x, y, core)
    own_rows = pl.ds(pl.multiple_of(own_at * share, share), share)
    local = [
        pltpu.make_async_copy(up_ref.at[0], gate_full.at[2 * z + x], local_sem.at[0]),
        pltpu.make_async_copy(up_ref.at[1], up_full.at[2 * z + x], local_sem.at[4]),
        pltpu.make_async_copy(down_ref, down_full.at[2 * z + x], local_sem.at[1]),
        pltpu.make_async_copy(dense_ref, dense_full.at[:, own_rows], local_sem.at[2]),
        pltpu.make_async_copy(small_ref, small_full.at[own_at], local_sem.at[3]),
    ]

    for side, link in ((1, "right"), (-1, "left")):
        @pl.when(sides[side])
        def _(link=link):
            each(dense_copies(z, x, y, link, True), "start")
    for link in ("x", "y", "core"):
        each(dense_copies(z, x, y, link, True), "start")
    send_own(0)
    each(local, "start")

    def x_arrived(row):
        each(dense_copies(row, 1 - x, y, "x"), "wait_recv")
        each(dense_copies(row, 1 - x, y, "y"), "start")
        each(dense_copies(row, 1 - x, y, "core"), "start")

    for s in (1, 2, 3):
        for side, link in ((1, "right"), (-1, "left")):
            row = z - side * s
            there = (z >= s) if side > 0 else (z + s <= 3)

            @pl.when(there)
            def _(row=row, side=side, link=link):
                each(dense_copies(row, x, y, link), "wait_recv")

                @pl.when(sides[side])
                def _():
                    each(dense_copies(row, x, y, link), "start")

                for other in ("x", "y", "core"):
                    each(dense_copies(row, x, y, other), "start")
        if s == 1:
            x_arrived(z)
        if s < 3:
            send_own(s)
    for s in (1, 2, 3):
        for row, there in ((z - s, z >= s), (z + s, z + s <= 3)):
            @pl.when(there)
            def _(row=row):
                x_arrived(row)
    for s in range(4):
        for column in range(2):
            row = lax.rem(z + s, 4)
            each(dense_copies(row, column, 1 - y, "y"), "wait_recv")
            each(dense_copies(row, column, 1 - y, "core"), "start")

    def pass_on(c, s):
        for side in (1, -1):
            row = z - side * s
            there = (z >= s) if side > 0 else (z + s <= 3)

            @pl.when(there)
            def _(row=row, side=side):
                copy_z(c, row, side).wait_recv()

                @pl.when(sides[side])
                def _():
                    copy_z(c, row, side).start()

                if c == 0:
                    @pl.when(row != 3 - z)
                    def _():
                        copy_x(c, row).start()
                else:
                    copy_x(c, row).start()

    for c in range(3):
        pass_on(c, 1)

    @pl.when(inner)
    def _():
        copy_x(0, z).wait_recv()
        copy_turn(z, inward, 0).start()

    for row in range(4):
        for column in range(2):
            for line in range(2):
                at = slot(row, column, line, 1 - core)
                rows = pl.ds(pl.multiple_of(at * share, share), share)
                index = row * 4 + column * 2 + line
                for part, ref in enumerate((dense_full.at[:, rows], small_full.at[at])):
                    pltpu.make_async_remote_copy(
                        src_ref=ref,
                        dst_ref=ref,
                        send_sem=d_send.at[part, 2, index],
                        recv_sem=d_recv.at[part, 2, index],
                        device_id=device_at(z, x, y, 1 - core),
                        device_id_type=pl.DeviceIdType.MESH,
                    ).wait_recv()
    each(local, "wait")

    width = dense_full.shape[2]
    lane = lax.broadcasted_iota(jnp.int32, (small_full.shape[0], width), 1)
    line_of = lax.broadcasted_iota(jnp.int32, (small_full.shape[0], width), 0)
    spread = (
        lax.broadcasted_iota(jnp.int32, (share, width), 1) % share
        == lax.broadcasted_iota(jnp.int32, (share, width), 0)
    ).astype(F32)

    def whole_row(row, start):
        shares = small_full[:, row, start : start + share]
        wide = jnp.dot(shares, spread, precision=HIGHEST, preferred_element_type=F32)
        return jnp.sum(jnp.where(lane // share == line_of, wide, 0.0), 0, keepdims=True)

    gain = whole_row(1, 0)
    bias_parts = small_full[:, 2, 0 : BUCKETS // 2]
    low = jnp.dot(bias_parts, hits_ref[: BUCKETS // 2], precision=HIGHEST, preferred_element_type=F32)
    high = jnp.dot(bias_parts, hits_ref[BUCKETS // 2 :], precision=HIGHEST, preferred_element_type=F32)
    for head in range(HEADS):
        table_ref[head : head + 1] = low[2 * head : 2 * head + 1] + high[2 * head + 1 : 2 * head + 2]
    seqlen = tokens_ref.shape[0]
    step = 128

    @pl.loop(0, seqlen // step)
    def _(i):
        at = pl.ds(pl.multiple_of(i * step, step), step)
        hidden_ref[at] = normed(tokens_ref[at].astype(F32), gain).astype(BF)

    tile = 256
    for part in range(3):
        @pl.loop(0, width // tile)
        def _(n, part=part):
            at = pl.ds(pl.multiple_of(n * tile, tile), tile)
            out = jnp.dot(hidden_ref[...], dense_full[part, :, at], preferred_element_type=F32)
            at = pl.ds(pl.multiple_of(part * width + n * tile, tile), tile)
            projected_ref[:, at] = out.astype(BF)

    prefix = prefix_ref[0]

    @pl.loop(0, HEADS // 2)
    def _(pair):
        def window(part):
            return pl.ds(pl.multiple_of(part * width + pair * 128, 128), 128)

        query_ref = projected_ref.at[:, window(0)]
        key_ref = projected_ref.at[:, window(1)]
        value_ref = projected_ref.at[:, window(2)]
        out_ref = attended_ref.at[:, window(0)]
        for head in range(2):
            lanes = slice(head * HEAD_DIM, (head + 1) * HEAD_DIM)
            rows = bias_rows(table_ref[pl.ds(2 * pair + head, 1), :], seqlen)
            key, value = key_ref[:, lanes], value_ref[:, lanes]
            for block in range(seqlen // 128):
                at = slice(128 * block, 128 * (block + 1))
                probs = probabilities(query_ref[at, lanes], key, rows, prefix, block, seqlen)
                out = jnp.dot(probs.astype(BF), value, preferred_element_type=F32)
                out_ref[at, lanes] = out.astype(BF)

        for c in range(3):
            @pl.when(pair == 3 * c + 1)
            def _(c=c):
                pass_on(c, 2)

    @pl.loop(0, width // tile)
    def _(n):
        at = pl.ds(pl.multiple_of(n * tile, tile), tile)
        out = jnp.dot(attended_ref[...], dense_full[3, :, at], preferred_element_type=F32)
        residual_ref[:, at] = tokens_ref[:, at].astype(F32) + out

    gain = whole_row(1, share)
    experts, capacity = arrived_ref.shape[0], arrived_ref.shape[1]
    router = [whole_row(0, share * number) for number in range(experts)]
    router = jnp.concatenate(router + [jnp.zeros((8 - experts, width), F32)], 0)
    logits = []
    for i in range(seqlen // step):
        at = slice(i * step, (i + 1) * step)
        second = normed(residual_ref[at], gain)
        second_ref[at] = second.astype(BF)
        logits.append(
            lax.dot_general(
                router,
                second,
                (((1,), (1,)), ((), ())),
                precision=HIGHEST,
                preferred_element_type=F32,
            )
        )
    logits = jnp.concatenate(logits, 1)[:experts]
    shifted = jnp.exp(logits - jnp.max(logits, 0, keepdims=True))
    soft = shifted / jnp.sum(shifted, 0, keepdims=True)
    chosen = chosen_ref[...]
    weight = soft * chosen[:experts].astype(F32)
    weight = weight / jnp.sum(weight, 0, keepdims=True)
    earlier = (
        lax.broadcasted_iota(jnp.int32, (seqlen, seqlen), 0)
        < lax.broadcasted_iota(jnp.int32, (seqlen, seqlen), 1)
    ).astype(F32)
    rank = jnp.dot(chosen, earlier.astype(BF), preferred_element_type=F32)
    rank = jnp.where(chosen.astype(F32) > 0.0, rank, -1.0).astype(jnp.int32)
    me = 2 * y + core

    def copy_rows(which, number):
        return pltpu.make_async_remote_copy(
            src_ref=rows_ref.at[which, number],
            dst_ref=(arrived_ref, grads_ref)[which].at[me],
            send_sem=a_send.at[which, number],
            recv_sem=a_recv.at[which, me],
            device_id=device_at(z, x, number // 2, number % 2),
            device_id_type=pl.DeviceIdType.MESH,
        )

    def keep_rows(which, number):
        return pltpu.make_async_copy(
            rows_ref.at[which, number],
            (arrived_ref, grads_ref)[which].at[number],
            a_send.at[which, number],
        )

    for number in range(experts):
        taken = (
            lax.broadcasted_iota(jnp.int32, (capacity, seqlen), 0) == rank[number : number + 1]
        ).astype(F32)
        slot_weight = jnp.sum(taken * weight[number : number + 1], 1, keepdims=True)
        pick = taken.astype(BF)

        @pl.loop(0, width // tile)
        def _(n, number=number, pick=pick, slot_weight=slot_weight):
            at = pl.ds(pl.multiple_of(n * tile, tile), tile)
            out = jnp.dot(pick, second_ref[:, at], preferred_element_type=F32)
            rows_ref[0, number, :, at] = out.astype(BF)
            out = jnp.dot(pick, cotangent_ref[:, at], preferred_element_type=F32)
            rows_ref[1, number, :, at] = (slot_weight * out).astype(BF)

        for which in range(2):
            @pl.when(me == number)
            def _(which=which, number=number):
                keep_rows(which, number).start()

            @pl.when(me != number)
            def _(which=which, number=number):
                copy_rows(which, number).start()

    for c in range(3):
        pass_on(c, 3)

    @pl.when(inner)
    def _():
        copy_x(0, outer_row).wait_recv()
        copy_turn(outer_row, outward, 1).start()

    for number in range(experts):
        for which in range(2):
            @pl.when(me == number)
            def _(which=which, number=number):
                keep_rows(which, number).wait()

            @pl.when(me != number)
            def _(which=which, number=number):
                copy_rows(which, number).wait_send()
                pltpu.make_async_remote_copy(
                    src_ref=rows_ref.at[which, number],
                    dst_ref=(arrived_ref, grads_ref)[which].at[number],
                    send_sem=a_send.at[which, number],
                    recv_sem=a_recv.at[which, number],
                    device_id=device_at(z, x, number // 2, number % 2),
                    device_id_type=pl.DeviceIdType.MESH,
                ).wait_recv()

    for row in range(4):
        for column in range(2):
            for line in range(2):
                each(dense_copies(row, column, line, "core"), "wait_send")
        for column in range(2):
            each(dense_copies(row, column, y, "y"), "wait_send")
        each(dense_copies(row, x, y, "x"), "wait_send")
        for side, link in ((1, "right"), (-1, "left")):
            sent = sides[side] & ((row <= z) if side > 0 else (row >= z))

            @pl.when(sent)
            def _(row=row, side=side, link=link):
                each(dense_copies(row, x, y, link), "wait_send")
                for c in range(3):
                    copy_z(c, row, side).wait_send()
        for c in (1, 2):
            copy_x(c, row).wait_recv()
            copy_x(c, row).wait_send()

        @pl.when(z != 3 - row)
        def _(row=row):
            copy_x(0, row).wait_send()

            @pl.when(jnp.logical_not(inner & ((z == row) | (outer_row == row))))
            def _():
                copy_x(0, row).wait_recv()

    copy_turn(3 - z, 0, 0).wait_recv()

    @pl.when(inner)
    def _():
        copy_turn(z, inward, 0).wait_send()
        copy_turn(outer_row, outward, 1).wait_send()


def gather_weights(up, down, dense, small, tokens, cotangent, chosen, hits, prefix, capacity):
    seqlen, width = tokens.shape
    devices = lax.axis_size(BOTH)
    slices, experts = lax.axis_size("dp"), lax.axis_size("expert")
    vmem, hbm = pl.BlockSpec(memory_space=pltpu.VMEM), pl.BlockSpec(memory_space=pl.ANY)
    dma = pltpu.SemaphoreType.DMA
    return pl.pallas_call(
        gather_kernel,
        in_specs=[vmem] * 8 + [pl.BlockSpec(memory_space=pltpu.SMEM)],
        out_specs=[hbm] * 3 + [vmem] * 7 + [hbm] * 2,
        out_shape=[
            jax.ShapeDtypeStruct((slices,) + up.shape[1:], BF),
            jax.ShapeDtypeStruct((slices,) + up.shape[1:], BF),
            jax.ShapeDtypeStruct((slices,) + down.shape, BF),
            jax.ShapeDtypeStruct((dense.shape[0], devices * dense.shape[1], dense.shape[2]), BF),
            jax.ShapeDtypeStruct((devices,) + small.shape, F32),
            jax.ShapeDtypeStruct((seqlen, width), BF),
            jax.ShapeDtypeStruct((seqlen, 3 * width), BF),
            jax.ShapeDtypeStruct((seqlen, width), BF),
            jax.ShapeDtypeStruct((seqlen, width), F32),
            jax.ShapeDtypeStruct((HEADS, hits.shape[1]), F32),
            jax.ShapeDtypeStruct((experts, capacity, width), BF),
            jax.ShapeDtypeStruct((experts, capacity, width), BF),
        ],
        scratch_shapes=[
            pltpu.VMEM((seqlen, width), BF),
            pltpu.VMEM((2, experts, capacity, width), BF),
            dma((5,)),
            dma((3, 2, 4)),
            dma((3, 4)),
            dma((3, 4)),
            dma((3, 4)),
            dma((2, 2, 4)),
            dma((2, 4)),
            dma((2, 3, 16)),
            dma((2, 3, 16)),
            dma((2,)),
            dma((1,)),
            dma((2, experts)),
            dma((2, experts)),
        ],
        compiler_params=pltpu.CompilerParams(collective_id=1, has_side_effects=True, vmem_limit_bytes=60 * 2**20),
        name="gather_weights",
    )(up, down, dense, small, tokens, cotangent, chosen, hits, prefix)


def reduce_kernel(
    gate_grads,
    up_grads,
    down_grads,
    dense_ref,
    hidden_turned,
    attended_turned,
    branch_ref,
    projected_ref,
    table_ref,
    prefix_ref,
    up_out,
    down_out,
    dense_out,
    hidden_grad,
    bias_ref,
    wide_got,
    tall_got,
    wide_line,
    tall_line,
    wide_own,
    tall_own,
    grads_ref,
    upstream_ref,
    full_ref,
    core_got,
    y_got,
    x_got,
    line_got,
    own_sem,
    x_send,
    x_recv,
    z_send,
    z_recv,
    core_send,
    core_recv,
    y_send,
    y_recv,
    dx_send,
    dx_recv,
):
    z, x, y, core = where_am_i()
    greet(z, x, y, core)
    mesh_id = pl.DeviceIdType.MESH
    share = dense_out.shape[1]
    parts, width = full_ref.shape[0], full_ref.shape[2]
    grads = (gate_grads, up_grads, down_grads)

    def got(c, row):
        return wide_got.at[c, row] if c < 2 else tall_got.at[row] if c == 2 else x_got.at[row]

    def line(c, place):
        return wide_line.at[c, place] if c < 2 else tall_line.at[place] if c == 2 else line_got.at[place]

    def own(c):
        return wide_own.at[c] if c < 2 else tall_own

    def load(c, row):
        return pltpu.make_async_copy(grads[c].at[2 * row + x], own(c), own_sem.at[c])

    def copy_x(c, row):
        return pltpu.make_async_remote_copy(
            src_ref=grads[c].at[2 * row + 1 - x],
            dst_ref=got(c, row),
            send_sem=x_send.at[c, row],
            recv_sem=x_recv.at[c, row],
            device_id=device_at(z, 1 - x, y, core),
            device_id_type=mesh_id,
        )

    def copy_z(c, row, side, place):
        return pltpu.make_async_remote_copy(
            src_ref=got(c, row),
            dst_ref=line(c, place),
            send_sem=z_send.at[c, row],
            recv_sem=z_recv.at[c, place],
            device_id=device_at(z + side, x, y, core),
            device_id_type=mesh_id,
        )

    def add(out, terms):
        shape = out.shape
        if len(shape) == 3:
            @pl.loop(0, shape[0])
            def _(i):
                total = functools.reduce(jnp.add, [term[i].astype(F32) for term in terms])
                out[i] = total.astype(out.dtype)
        else:
            @pl.loop(0, shape[0] // 16)
            def _(i):
                at = pl.ds(pl.multiple_of(i * 16, 16), 16)
                total = functools.reduce(jnp.add, [term[at].astype(F32) for term in terms])
                out[at] = total.astype(out.dtype)

    there = {}
    for s in (3, 2, 1):
        there[s, 1] = z + s <= 3
        there[s, -1] = z >= s
    order = [(s, side) for s in (3, 2, 1) for side in (1, -1)]

    def row_of(s, side):
        return lax.rem(z + side * s + 4, 4)

    def step(c, s, side):
        row = row_of(s, side)

        def run():
            if c < 3:
                copy_x(c, row).wait_recv()
            terms = [got(c, row)] + ([own(c)] if c < 3 else [])
            before = (z > 0) if side > 0 else (z < 3)

            @pl.when(before)
            def _():
                copy_z(c, row, side, row).wait_recv()
                add(got(c, row), terms + [line(c, row)])

            if c < 3:
                @pl.when(jnp.logical_not(before))
                def _():
                    add(got(c, row), terms)

            copy_z(c, row, side, 4 if (s == 1 and side < 0) else row).start()

        if c < 3:
            load(c, row).wait()
        pl.when(there[s, side])(run)
        if c < 3:
            index = order.index((s, side)) + 1
            load(c, row_of(*order[index]) if index < len(order) else z).start()

    def last(c, out):
        if c < 3:
            copy_x(c, z).wait_recv()
            load(c, z).wait()
            add(out, [got(c, z), own(c)])
        else:
            add(out, [got(c, z)])

        @pl.when(z > 0)
        def _():
            copy_z(c, z, 1, z).wait_recv()
            add(out, [out, line(c, z)])

        @pl.when(z < 3)
        def _():
            copy_z(c, z, -1, 4).wait_recv()
            add(out, [out, line(c, 4)])

    for s, side in order:
        @pl.when(there[s, side])
        def _(s=s, side=side):
            for c in range(3):
                copy_x(c, row_of(s, side)).start()
    for c in range(3):
        load(c, row_of(3, 1)).start()

    turned = (((1,), (1,)), ((), ()))
    flip = (((0,), (0,)), ((), ()))
    tile = 256

    @pl.loop(0, width // tile)
    def _(n):
        at = pl.ds(pl.multiple_of(n * tile, tile), tile)
        out = lax.dot_general(
            branch_ref[...], dense_ref[3, at, :], turned, preferred_element_type=F32
        )
        upstream_ref[:, at] = out.astype(BF)
        out = jnp.dot(attended_turned[...], branch_ref[:, at], preferred_element_type=F32)
        full_ref[3, :, at] = out.astype(BF)

    seqlen = projected_ref.shape[0]
    blocks = seqlen // 128
    prefix = prefix_ref[0]

    def attend_pair(pair):
        def window(part):
            return pl.ds(pl.multiple_of(part * width + pair * 128, 128), 128)

        for head in range(2):
            lanes = slice(head * HEAD_DIM, (head + 1) * HEAD_DIM)
            rows = bias_rows(table_ref[pl.ds(2 * pair + head, 1), :], seqlen)
            query = projected_ref.at[:, window(0)][:, lanes]
            key = projected_ref.at[:, window(1)][:, lanes]
            value = projected_ref.at[:, window(2)][:, lanes]
            upstream = upstream_ref.at[:, window(0)][:, lanes]
            probs_low, scores_low, scores = [], [], []
            for block in range(blocks):
                at = slice(128 * block, 128 * (block + 1))
                probs = probabilities(query[at], key, rows, prefix, block, seqlen)
                probs_grad = lax.dot_general(
                    upstream[at], value, turned, preferred_element_type=F32
                )
                inner = jnp.sum(probs * probs_grad, -1, keepdims=True)
                low = (probs * (probs_grad - inner)).astype(BF)
                probs_low.append(probs.astype(BF))
                scores_low.append(low)
                scores.append(low.astype(F32))
                out = jnp.dot(low, key, preferred_element_type=F32) * 0.125
                grads_ref.at[:, window(0)][at, lanes] = out.astype(BF)
            probs_all = jnp.concatenate(probs_low, 0)
            scores_all = jnp.concatenate(scores_low, 0)
            out = lax.dot_general(probs_all, upstream, flip, preferred_element_type=F32)
            grads_ref.at[:, window(2)][:, lanes] = out.astype(BF)
            out = lax.dot_general(scores_all, query, flip, preferred_element_type=F32) * 0.125
            grads_ref.at[:, window(1)][:, lanes] = out.astype(BF)
            bias_ref[pl.ds(2 * pair + head, 1)] = diagonals(scores)[None]

    @pl.loop(0, HEADS // 2)
    def _(pair):
        attend_pair(pair)
        for c, when in ((0, 3), (1, 7)):
            @pl.when(pair == when)
            def _(c=c):
                step(c, 3, 1)
                step(c, 3, -1)

    for part in range(3):
        @pl.loop(0, width // tile)
        def _(n, part=part):
            at = pl.ds(pl.multiple_of(n * tile, tile), tile)
            from_at = pl.ds(pl.multiple_of(part * width + n * tile, tile), tile)
            out = jnp.dot(hidden_turned[...], grads_ref[:, from_at], preferred_element_type=F32)
            full_ref[part, :, at] = out.astype(BF)

    def rows_of(k, number):
        at = (k // 2) * 4 + (k % 2) * 2 + number
        return pl.ds(pl.multiple_of(at * share, share), share)

    def copy_core(k):
        return pltpu.make_async_remote_copy(
            src_ref=full_ref.at[:, rows_of(k, 1 - core)],
            dst_ref=core_got.at[k],
            send_sem=core_send.at[k],
            recv_sem=core_recv.at[k],
            device_id=device_at(z, x, y, 1 - core),
            device_id_type=mesh_id,
        )

    def copy_y(k):
        return pltpu.make_async_remote_copy(
            src_ref=core_got.at[2 * k + 1 - y],
            dst_ref=y_got.at[k],
            send_sem=y_send.at[k],
            recv_sem=y_recv.at[k],
            device_id=device_at(z, x, 1 - y, core),
            device_id_type=mesh_id,
        )

    def copy_dx(row):
        return pltpu.make_async_remote_copy(
            src_ref=y_got.at[2 * row + 1 - x],
            dst_ref=x_got.at[row],
            send_sem=dx_send.at[row],
            recv_sem=dx_recv.at[row],
            device_id=device_at(z, 1 - x, y, core),
            device_id_type=mesh_id,
        )

    @pl.loop(0, 16)
    def _(k):
        copy_core(k).start()

    step(2, 3, 1)
    step(2, 3, -1)

    @pl.loop(0, width // tile)
    def _(n):
        at = pl.ds(pl.multiple_of(n * tile, tile), tile)
        total = None
        for part in range(3):
            out = lax.dot_general(
                grads_ref[:, part * width : (part + 1) * width],
                dense_ref[part, at, :],
                turned,
                preferred_element_type=F32,
            )
            total = out if total is None else total + out
        hidden_grad[:, at] = total

    @pl.loop(0, 8)
    def _(k):
        for line_y in range(2):
            copy_core(2 * k + line_y).wait_recv()
            for part in range(parts):
                mine = full_ref.at[part, rows_of(2 * k + line_y, core)]
                other = core_got.at[2 * k + line_y, part]
                other[...] = (other[...].astype(F32) + mine[...].astype(F32)).astype(BF)
        copy_y(k).start()

    for c in range(3):
        step(c, 2, 1)
        step(c, 2, -1)
    step(0, 1, 1)
    step(0, 1, -1)

    @pl.loop(0, 4)
    def _(row):
        for column in range(2):
            k = 2 * row + column
            copy_y(k).wait_recv()
            for part in range(parts):
                mine, other = core_got.at[2 * k + y, part], y_got.at[k, part]
                other[...] = (other[...].astype(F32) + mine[...].astype(F32)).astype(BF)
        copy_dx(row).start()

    for c in range(3):
        copy_x(c, z).start()
    for c in (1, 2):
        step(c, 1, 1)
        step(c, 1, -1)

    @pl.loop(0, 4)
    def _(row):
        copy_dx(row).wait_recv()
        for part in range(parts):
            mine, other = y_got.at[2 * row + x, part], x_got.at[row, part]
            other[...] = (other[...].astype(F32) + mine[...].astype(F32)).astype(BF)

    for s, side in order:
        step(3, s, side)
    last(0, up_out.at[0])
    last(1, up_out.at[1])
    last(3, dense_out)
    last(2, down_out)

    @pl.loop(0, 16)
    def _(k):
        copy_core(k).wait_send()

    @pl.loop(0, 8)
    def _(k):
        copy_y(k).wait_send()

    @pl.loop(0, 4)
    def _(row):
        copy_dx(row).wait_send()
        for c in range(3):
            copy_x(c, row).wait_send()

    for s, side in order:
        @pl.when(there[s, side])
        def _(s=s, side=side):
            for c in range(4):
                copy_z(c, row_of(s, side), side, row_of(s, side)).wait_send()


def reduce_weights(gate, up, down, dense, hidden, attended, branch, projected, table, prefix):
    seqlen, width = hidden.shape
    share = width // lax.axis_size(BOTH)
    vmem, hbm = pl.BlockSpec(memory_space=pltpu.VMEM), pl.BlockSpec(memory_space=pl.ANY)
    dma = pltpu.SemaphoreType.DMA
    wide, tall = gate.shape[1:], down.shape[1:]
    dense_shape = (dense.shape[0], share, width)
    return pl.pallas_call(
        reduce_kernel,
        in_specs=[hbm] * 3 + [vmem] * 6 + [pl.BlockSpec(memory_space=pltpu.SMEM)],
        out_specs=[vmem] * 5,
        out_shape=[
            jax.ShapeDtypeStruct((2,) + wide, F32),
            jax.ShapeDtypeStruct(tall, F32),
            jax.ShapeDtypeStruct(dense_shape, F32),
            jax.ShapeDtypeStruct((seqlen, width), F32),
            jax.ShapeDtypeStruct((HEADS, 8, table.shape[1]), F32),
        ],
        scratch_shapes=[
            pltpu.VMEM((2, 4) + wide, BF),
            pltpu.VMEM((4,) + tall, BF),
            pltpu.VMEM((2, 5) + wide, BF),
            pltpu.VMEM((5,) + tall, BF),
            pltpu.VMEM((2,) + wide, BF),
            pltpu.VMEM(tall, BF),
            pltpu.VMEM((seqlen, 3 * width), BF),
            pltpu.VMEM((seqlen, width), BF),
            pltpu.VMEM(dense.shape, BF),
            pltpu.VMEM((16,) + dense_shape, BF),
            pltpu.VMEM((8,) + dense_shape, BF),
            pltpu.VMEM((4,) + dense_shape, BF),
            pltpu.VMEM((5,) + dense_shape, BF),
            dma((3,)),
            dma((3, 4)),
            dma((3, 4)),
            dma((4, 4)),
            dma((4, 5)),
            dma((16,)),
            dma((16,)),
            dma((8,)),
            dma((8,)),
            dma((4,)),
            dma((4,)),
        ],
        compiler_params=pltpu.CompilerParams(
            collective_id=2, has_side_effects=True, vmem_limit_bytes=67043328
        ),
        name="reduce_weights",
    )(gate, up, down, dense, hidden.T, attended.T, branch, projected, table, prefix)


def sum_kernel(array_ref, out_ref, sent, got, send_sem, recv_sem):
    z, x, y, core = where_am_i()
    barrier = pltpu.get_barrier_semaphore()
    pairs = [(z, x, y, 1 - core), (z, x, 1 - y, core), (z, 1 - x, y, core)]
    lines = [(lax.rem(z + s, 4), x, y, core) for s in (1, 2, 3)]
    for place in pairs + lines:
        pl.semaphore_signal(
            barrier, inc=1, device_id=device_at(*place), device_id_type=pl.DeviceIdType.MESH
        )
    pl.semaphore_wait(barrier, 6)

    def copy(stage, number, slot, place):
        return pltpu.make_async_remote_copy(
            src_ref=sent.at[stage],
            dst_ref=got.at[slot],
            send_sem=send_sem.at[number],
            recv_sem=recv_sem.at[slot],
            device_id=device_at(*place),
            device_id_type=pl.DeviceIdType.MESH,
        )

    total = array_ref[...]
    for stage, place in enumerate(pairs):
        sent[stage] = total
        move = copy(stage, stage, stage, place)
        move.start()
        move.wait()
        total = total + got[stage]
    sent[3] = total
    moves = [copy(3, 3 + number, 3 + z, place) for number, place in enumerate(lines)]
    for move in moves:
        move.start()
    for row in range(4):
        @pl.when(z == row)
        def _(row=row):
            got[3 + row] = sent[3]

        @pl.when(z != row)
        def _(row=row):
            copy(3, 3, 3 + row, lines[0]).wait_recv()
    out_ref[...] = got[3] + got[4] + got[5] + got[6]
    for move in moves:
        move.wait_send()


def sum_all(array):
    if not is_line():
        return lax.psum(array, BOTH)
    vmem = pl.BlockSpec(memory_space=pltpu.VMEM)
    dma = pltpu.SemaphoreType.DMA
    return pl.pallas_call(
        sum_kernel,
        in_specs=[vmem],
        out_specs=vmem,
        out_shape=jax.ShapeDtypeStruct(array.shape, F32),
        scratch_shapes=[
            pltpu.VMEM((4,) + array.shape, F32),
            pltpu.VMEM((7,) + array.shape, F32),
            dma((6,)),
            dma((7,)),
        ],
        compiler_params=pltpu.CompilerParams(collective_id=3, has_side_effects=True),
        name="sum_all",
    )(array)


def on_device(
    tokens,
    cotangent,
    routes,
    prefix,
    buckets,
    step_count,
    learn_rate,
    weight_decay,
    attend_master,
    attend_first,
    attend_second,
    outward_master,
    outward_first,
    outward_second,
    router_master,
    router_first,
    router_second,
    gains_master,
    gains_first,
    gains_second,
    bias_master,
    bias_first,
    bias_second,
    upward_master,
    upward_first,
    upward_second,
    downward_master,
    downward_first,
    downward_second,
):
    devices = lax.axis_size(BOTH)
    share = attend_master.shape[1]
    seqlen = tokens.shape[0]
    experts = router_master.shape[1]
    capacity = seqlen * TOP * 5 // (4 * experts)

    slices = lax.axis_size("dp")
    router_size, gains_size = router_master.size, gains_master.size
    bucket_hits = (buckets[:, None] == jnp.arange(BUCKETS, dtype=jnp.int32)[None, :]).astype(F32)
    offsets = buckets.shape[0]
    inputs = tokens.astype(F32)
    kinds = jnp.arange(experts, dtype=jnp.int32)
    route_hits = (routes[:, :, None] == kinds[None, None, :]).astype(F32)
    hits = jnp.sum(route_hits, 1)
    if is_line():
        chosen = jnp.sum((routes.T[:, None, :] == jnp.arange(8)[None, :, None]).astype(F32), 0)
        hits_wide = jnp.pad(bucket_hits.T, ((0, 0), (0, 2 * seqlen - offsets)))
        small = jnp.concatenate(
            [
                jnp.pad(one.reshape(1, -1), ((0, 0), (0, 128 - one.size)))
                for one in (router_master.T, gains_master, bias_master)
            ]
            + [jnp.zeros((5, 128), F32)]
        )
        dense = jnp.concatenate([attend_master.astype(BF), outward_master.astype(BF)[None]])
        (
            gate_w,
            up_w,
            downward_w,
            dense_w,
            small,
            hidden_one,
            projected,
            attended,
            residual,
            table,
            arrived,
            grad_arrived,
        ) = gather_weights(
            upward_master[:, 0].astype(BF),
            downward_master[0].astype(BF),
            dense,
            small,
            tokens,
            cotangent,
            chosen.astype(BF),
            hits_wide,
            prefix,
            capacity,
        )
        attend_w, outward_w = dense_w[:3], dense_w[3]
        gate_w, up_w = gate_w.reshape(D, FF), up_w.reshape(D, FF)
        downward_w = downward_w.reshape(FF, D)
        router_w = small[:, 0].reshape(devices, experts, share).transpose(0, 2, 1).reshape(D, experts)
        gains_w = small[:, 1, :gains_size].reshape(devices, 2, share).transpose(1, 0, 2).reshape(2, D)
        table = table.reshape(HEADS // 2, 2, 2 * seqlen)
        first_pull = jax.vjp(normed, inputs, gains_w[0])[1]
    else:
        gate_w = gather_dp(upward_master[0, 0].astype(BF)).reshape(D, FF)
        up_w = gather_dp(upward_master[1, 0].astype(BF)).reshape(D, FF)
        downward_w = gather_dp(downward_master[0].astype(BF)).reshape(FF, D)
        attend_w = lax.all_gather(attend_master.astype(BF), BOTH, axis=1, tiled=True)
        outward_w = lax.all_gather(outward_master.astype(BF), BOTH, axis=0, tiled=True)
        router_w = lax.all_gather(router_master, BOTH, axis=0, tiled=True)
        gains_w = lax.all_gather(gains_master, BOTH, axis=1, tiled=True)
        bias_w = lax.all_gather(bias_master, BOTH, axis=0, tiled=True)
        table = jnp.dot(bias_w.reshape(HEADS, BUCKETS), bucket_hits.T, precision=HIGHEST)
        table = jnp.pad(table, ((0, 0), (0, 2 * seqlen - offsets)))
        table = table.reshape(HEADS // 2, 2, 2 * seqlen)
        first_normed, first_pull = jax.vjp(normed, inputs, gains_w[0])
        hidden_one = first_normed.astype(BF)
        projected = jnp.concatenate(
            [
                jnp.dot(hidden_one, attend_w[part], preferred_element_type=F32).astype(BF)
                for part in range(3)
            ],
            1,
        )
        attended = attend(prefix, table, projected)
        residual = inputs + jnp.dot(attended, outward_w, preferred_element_type=F32)

    def gate_piece(residual_in, scale_gain, router_in):
        second_normed = normed(residual_in, scale_gain)
        logits = jnp.dot(second_normed, router_in, precision=HIGHEST)
        router_soft = jax.nn.softmax(logits, axis=-1)
        chosen = jnp.sum(router_soft[:, None, :] * route_hits, -1)
        return (second_normed, chosen / jnp.sum(chosen, -1, keepdims=True))

    (second_normed, combine), gate_pull = jax.vjp(gate_piece, residual, gains_w[1], router_w)
    second_low = second_normed.astype(BF)

    places = jnp.arange(seqlen, dtype=jnp.int32)
    earlier = (places[None, :] < places[:, None]).astype(BF)
    rank = jnp.dot(earlier, hits.astype(BF), preferred_element_type=F32)
    rank = jnp.where(hits > 0, rank, -1.0).astype(jnp.int32)
    slots = jnp.arange(capacity, dtype=jnp.int32)
    taken = rank.T[:, None, :] == slots[None, :, None]
    choose = taken.astype(BF).reshape(experts * capacity, seqlen)
    weight = jnp.sum(combine[:, :, None] * route_hits, 1)
    slot_weight = jnp.sum(jnp.where(taken, weight.T[:, None, :], 0.0), -1)
    backs = [
        (
            (rank[:, :, None] == slots[None, None, :])
            & (routes[:, k][:, None, None] == kinds[None, :, None])
        )
        .astype(BF)
        .reshape(seqlen, experts * capacity)
        for k in range(TOP)
    ]
    back = (rank[:, :, None] == slots[None, None, :]).astype(BF)
    back = back.reshape(seqlen, experts * capacity)

    def exchange(rows, home):
        if home:
            rows = rows.reshape(1, experts, capacity, D)
            rows = lax.all_to_all(rows, "expert", split_axis=1, concat_axis=0, tiled=True)
        else:
            rows = rows.reshape(experts, 1, capacity, D)
            rows = lax.all_to_all(rows, "expert", split_axis=0, concat_axis=1, tiled=True)
        return rows.reshape(experts * capacity, D)

    if is_line():
        arrived = arrived.reshape(experts * capacity, D)
        grad_arrived = grad_arrived.reshape(experts * capacity, D)
    else:
        sent_rows = jnp.dot(choose, second_low, preferred_element_type=F32).astype(BF)
        upstream_rows = jnp.dot(choose, cotangent, preferred_element_type=F32)
        grad_rows = (slot_weight.reshape(-1, 1) * upstream_rows).astype(BF)
        sent_rows, grad_rows = lax.optimization_barrier((sent_rows, grad_rows))
        arrived = exchange(sent_rows, False)
        grad_arrived = exchange(grad_rows, False)

    gate_value = jnp.dot(arrived, gate_w, preferred_element_type=F32)
    up_value = jnp.dot(arrived, up_w, preferred_element_type=F32)
    gelu_value, gelu_pull = jax.vjp(gelu_tanh, gate_value)
    hidden_mid = (gelu_value * up_value).astype(BF)
    expert_out = jnp.dot(hidden_mid, downward_w, preferred_element_type=F32).astype(BF)
    returned = exchange(expert_out, True)

    turned = (((1,), (1,)), ((), ()))
    flipped = (((0,), (0,)), ((), ()))
    grad_mid = lax.dot_general(grad_arrived, downward_w, turned, preferred_element_type=F32)
    grad_gate = gelu_pull(grad_mid * up_value)[0].astype(BF)
    grad_up = (grad_mid * gelu_value).astype(BF)
    grad_sent = lax.dot_general(grad_gate, gate_w, turned, preferred_element_type=F32)
    grad_sent = grad_sent + lax.dot_general(grad_up, up_w, turned, preferred_element_type=F32)
    grad_sent, returned, grad_gate, grad_up, hidden_mid = lax.optimization_barrier(
        (grad_sent.astype(BF), returned, grad_gate, grad_up, hidden_mid)
    )
    grad_home = exchange(grad_sent, True)


    def weight_grad(left, right):
        full = lax.dot_general(left, right, flipped, preferred_element_type=F32).astype(BF)
        return full.reshape(slices, -1, full.shape[1])

    wide_grads = (
        weight_grad(arrived, grad_gate),
        weight_grad(arrived, grad_up),
        weight_grad(hidden_mid, grad_arrived),
    )

    came_back = jnp.stack(
        [jnp.dot(one, returned, preferred_element_type=F32) for one in backs], 1
    )
    expert_sum = jnp.sum(combine[..., None] * came_back, 1)
    block_output = (residual + expert_sum).astype(BF)
    upstream = cotangent.astype(F32)
    combine_grad = jnp.sum(upstream[:, None, :] * came_back, -1)

    grad_normed = jnp.dot(back, grad_home, preferred_element_type=F32)
    residual_part, gain_two_grad, router_full = gate_pull((grad_normed, combine_grad))
    grad_residual = upstream + residual_part
    grad_branch = grad_residual.astype(BF)
    if is_line():
        upward_g, downward_g, dense_g, grad_hidden_one, bias_parts = reduce_weights(
            *wide_grads,
            dense_w,
            hidden_one,
            attended,
            grad_branch,
            projected,
            table.reshape(HEADS, 2 * seqlen),
            prefix,
        )
        attend_g, outward_g = dense_g[:3], dense_g[3]
        upward_g, downward_g = upward_g[:, None], downward_g[None]
    else:
        upward_g = jnp.stack([scatter_dp(one) for one in wide_grads[:2]])[:, None]
        downward_g = scatter_dp(wide_grads[2])[None]
        outward_full = lax.dot_general(attended, grad_branch, flipped, preferred_element_type=F32)
        outward_g = scatter_all(outward_full.astype(BF).reshape(devices, share, D))
        grad_attended = lax.dot_general(grad_branch, outward_w, turned, preferred_element_type=F32)
        query_grad, key_grad, value_grad, bias_parts = attend_back(
            prefix, table, projected, grad_attended.astype(BF)
        )
        projected_grads = (query_grad, key_grad, value_grad)
        attend_g = scatter_all(
            jnp.concatenate(
                [
                    lax.dot_general(hidden_one, part, flipped, preferred_element_type=F32)
                    .astype(BF)
                    .reshape(devices, share, D)
                    for part in projected_grads
                ],
                1,
            )
        ).reshape(3, share, D)
        grad_hidden_one = functools.reduce(
            jnp.add,
            [
                lax.dot_general(part, attend_w[which], turned, preferred_element_type=F32)
                for which, part in enumerate(projected_grads)
            ],
        )

    inputs_part, gain_one_grad = first_pull(grad_hidden_one)
    input_grad = (grad_residual + inputs_part).astype(BF)

    bias_parts = bias_parts.reshape(HEADS, 8, 2 * seqlen)
    bias_parts = jnp.pad(bias_parts, ((0, 0), (0, 0), (0, 8)))
    per_offset = functools.reduce(
        jnp.add, [bias_parts[:, row, row : row + offsets] for row in range(8)]
    )
    bias_full = jnp.dot(per_offset, bucket_hits, precision=HIGHEST).reshape(-1)

    lanes = jnp.arange(128, dtype=jnp.int32)

    def in_lanes(values):
        return functools.reduce(
            jnp.add, [jnp.where(lanes == which, value, 0.0) for which, value in values.items()]
        )

    def square(array):
        return jnp.sum(array * array)

    big = in_lanes(
        {0: square(attend_g), 1: square(outward_g), 5: square(upward_g), 6: square(downward_g)}
    )
    parts = (router_full.reshape(-1), gain_one_grad, gain_two_grad, bias_full)
    length = sum(one.size for one in parts)
    padding = jnp.zeros((-length - 128) % 1024, F32)
    sums = sum_all(jnp.concatenate(parts + (padding, big)).reshape(-1, 128))
    smalls = sums.reshape(-1)[:length]
    place = lax.axis_index(BOTH)
    router_g = lax.dynamic_slice(smalls, (place * router_size,), (router_size,))
    router_g = router_g.reshape(share, experts)
    start = D * experts
    gains_g = jnp.stack(
        [
            lax.dynamic_slice(smalls, (start + row * D + place * share,), (share,))
            for row in range(2)
        ]
    )
    bias_g = lax.dynamic_slice(smalls, (start + 2 * D + place * bias_master.size,), bias_master.shape)

    grads_all = (attend_g, outward_g, router_g, gains_g, bias_g, upward_g, downward_g)
    start = D * experts
    totals = sums[-1] + in_lanes(
        {
            2: square(smalls[:start]),
            3: square(smalls[start : start + 2 * D]),
            4: square(smalls[start + 2 * D :]),
        }
    )
    totals = totals[:7]
    counts_all = jnp.array(
        [
            3 * D * D,
            D * D,
            D * experts,
            2 * D,
            HEADS * BUCKETS,
            2 * experts * D * FF,
            experts * FF * D,
        ],
        jnp.float32,
    )
    mean_squares = totals / counts_all
    grad_rms = jnp.sqrt(mean_squares)
    factors = lax.rsqrt(mean_squares + 1e-06)
    step_float = step_count.astype(jnp.float32)
    masters = (
        attend_master,
        outward_master,
        router_master,
        gains_master,
        bias_master,
        upward_master,
        downward_master,
    )
    firsts = (
        attend_first,
        outward_first,
        router_first,
        gains_first,
        bias_first,
        upward_first,
        downward_first,
    )
    seconds = (
        attend_second,
        outward_second,
        router_second,
        gains_second,
        bias_second,
        upward_second,
        downward_second,
    )
    flags = (True, True, True, False, False, True, True)
    updates = [
        adamw_update(
            masters[member],
            firsts[member],
            seconds[member],
            grads_all[member] * factors[member],
            step_float,
            learn_rate,
            weight_decay,
            flags[member],
        )
        for member in range(7)
    ]
    return (
        block_output,
        input_grad,
        grads_all[0],
        updates[0][0],
        updates[0][1],
        updates[0][2],
        grads_all[1],
        updates[1][0],
        updates[1][1],
        updates[1][2],
        grads_all[2],
        updates[2][0],
        updates[2][1],
        updates[2][2],
        grads_all[3],
        updates[3][3],
        updates[3][1],
        updates[3][2],
        grads_all[4],
        updates[4][3],
        updates[4][1],
        updates[4][2],
        grads_all[5],
        updates[5][0],
        updates[5][1],
        updates[5][2],
        grads_all[6],
        updates[6][0],
        updates[6][1],
        updates[6][2],
        grad_rms,
    )


def solution(mesh):
    placed = (
        P(("dp", "expert"), None),
        P(("dp", "expert"), None),
        P(("dp", "expert"), None),
        P(("dp", "expert")),
        P(),
        P(),
        P(),
        P(),
        P(None, ("dp", "expert"), None),
        P(None, ("dp", "expert"), None),
        P(None, ("dp", "expert"), None),
        P(("dp", "expert"), None),
        P(("dp", "expert"), None),
        P(("dp", "expert"), None),
        P(("dp", "expert"), None),
        P(("dp", "expert"), None),
        P(("dp", "expert"), None),
        P(None, ("dp", "expert")),
        P(None, ("dp", "expert")),
        P(None, ("dp", "expert")),
        P(("dp", "expert")),
        P(("dp", "expert")),
        P(("dp", "expert")),
        P(None, "expert", "dp", None),
        P(None, "expert", "dp", None),
        P(None, "expert", "dp", None),
        P("expert", "dp", None),
        P("expert", "dp", None),
        P("expert", "dp", None),
    )
    return jax.shard_map(
        on_device,
        mesh=mesh,
        in_specs=placed,
        out_specs=(
            P(("dp", "expert"), None),
            P(("dp", "expert"), None),
            P(None, ("dp", "expert"), None),
            P(None, ("dp", "expert"), None),
            P(None, ("dp", "expert"), None),
            P(None, ("dp", "expert"), None),
            P(("dp", "expert"), None),
            P(("dp", "expert"), None),
            P(("dp", "expert"), None),
            P(("dp", "expert"), None),
            P(("dp", "expert"), None),
            P(("dp", "expert"), None),
            P(("dp", "expert"), None),
            P(("dp", "expert"), None),
            P(None, ("dp", "expert")),
            P(None, ("dp", "expert")),
            P(None, ("dp", "expert")),
            P(None, ("dp", "expert")),
            P(("dp", "expert")),
            P(("dp", "expert")),
            P(("dp", "expert")),
            P(("dp", "expert")),
            P(None, "expert", "dp", None),
            P(None, "expert", "dp", None),
            P(None, "expert", "dp", None),
            P(None, "expert", "dp", None),
            P("expert", "dp", None),
            P("expert", "dp", None),
            P("expert", "dp", None),
            P("expert", "dp", None),
            P(),
        ),
        check_vma=False,
    )
```

```python
import functools

import jax
import jax.numpy as jnp
from jax import lax
from jax.experimental import pallas as pl
from jax.experimental.pallas import tpu as pltpu
from jax.sharding import PartitionSpec as P

D = 1024
HEADS = 16
HEAD_DIM = 64
FF = 2816
BUCKETS = 32
TOP = 2
BOTH = ("dp", "expert")
BF = jnp.bfloat16
F32 = jnp.float32

HIGHEST = lax.Precision.HIGHEST
MASKED = -1e30


def normed(values, scale_gain):
    return values * lax.rsqrt(jnp.mean(values * values, -1, keepdims=True) + 1e-06) * scale_gain


def gelu_both(values):
    scale = 0.7978845608028654
    square = values * values
    half = 0.5 + 0.5 * jnp.tanh(values * (scale + (scale * 0.044715) * square))
    value = values * half
    slope = half + value * (1.0 - half) * (2.0 * scale + (6.0 * scale * 0.044715) * square)
    return value, slope


def adamw_update(
    master, first_moment, second, gradient, step_float, learn_rate, weight_decay, decayed
):
    mean_new = 0.9 * first_moment + 0.1 * gradient
    square_new = 0.95 * second + 0.05 * gradient * gradient
    mean_hat = mean_new / (1.0 - jnp.power(jnp.float32(0.9), step_float))
    square_hat = square_new / (1.0 - jnp.power(jnp.float32(0.95), step_float))
    change = learn_rate * (mean_hat / (jnp.sqrt(square_hat) + 1e-08))
    updated = master - change
    if decayed:
        updated = updated - weight_decay * master
    return (updated, mean_new, square_new, -change)


def is_line():
    return lax.axis_size("dp") == 8 and lax.axis_size("expert") == 4


def gather_dp(shard):
    return lax.all_gather(shard, "dp", axis=0)


def scatter_dp(parts):
    return lax.psum_scatter(parts.astype(F32), "dp", scatter_dimension=0, tiled=False)


def scatter_all(parts):
    return lax.psum_scatter(parts.astype(F32), BOTH, scatter_dimension=0, tiled=False)


def bias_rows(table, seqlen):
    width = table.shape[-1]
    wide = jnp.broadcast_to(table, (128, width))
    return pltpu.roll(wide, width - 127, 1, stride=1, stride_axis=0)


def probabilities(query, key, rows, prefix, block, seqlen):
    blocks = seqlen // 128
    raw = (
        lax.dot_general(query, key, (((1,), (1,)), ((), ())), preferred_element_type=F32) * 0.125
    )
    start = 128 * (blocks - 1 - block)
    raw = raw + rows[:, start : start + seqlen]
    i = lax.broadcasted_iota(jnp.int32, raw.shape, 0) + 128 * block
    j = lax.broadcasted_iota(jnp.int32, raw.shape, 1)
    raw = jnp.where((j <= i) | (j < prefix), raw, MASKED)
    shifted = jnp.exp(raw - jnp.max(raw, -1, keepdims=True))
    return shifted / jnp.sum(shifted, -1, keepdims=True)


def attend_kernel(prefix_ref, table_ref, query_ref, key_ref, value_ref, out_ref):
    seqlen = query_ref.shape[0]
    prefix = prefix_ref[0]
    for head in range(2):
        lanes = slice(head * HEAD_DIM, (head + 1) * HEAD_DIM)
        rows = bias_rows(table_ref[0, head : head + 1, :], seqlen)
        key, value = key_ref[:, lanes], value_ref[:, lanes]
        for block in range(seqlen // 128):
            at = slice(128 * block, 128 * (block + 1))
            probs = probabilities(query_ref[at, lanes], key, rows, prefix, block, seqlen)
            out = jnp.dot(probs.astype(BF), value, preferred_element_type=F32)
            out_ref[at, lanes] = out.astype(BF)


def diagonals(scores):
    blocks = len(scores)
    columns = []
    for column in range(2 * blocks - 1):
        terms = []
        for block in range(blocks):
            piece = column - (blocks - 1 - block)
            if 0 <= piece < blocks:
                terms.append(scores[block][:, 128 * piece : 128 * (piece + 1)])
        columns.append(functools.reduce(jnp.add, terms))
    columns.append(jnp.zeros_like(columns[0]))
    wide = jnp.concatenate(columns, 1)
    total = jnp.zeros((8, wide.shape[1]), F32)
    for group in range(16):
        total = total + pltpu.roll(wide[8 * group : 8 * group + 8], 127 - 8 * group, 1)
    return total


def attend_back_kernel(
    prefix_ref,
    table_ref,
    query_ref,
    key_ref,
    value_ref,
    upstream_ref,
    query_grad_ref,
    key_grad_ref,
    value_grad_ref,
    bias_ref,
):
    seqlen = query_ref.shape[0]
    blocks = seqlen // 128
    prefix = prefix_ref[0]
    flip = (((0,), (0,)), ((), ()))
    for head in range(2):
        lanes = slice(head * HEAD_DIM, (head + 1) * HEAD_DIM)
        rows = bias_rows(table_ref[0, head : head + 1, :], seqlen)
        query, key, value = query_ref[:, lanes], key_ref[:, lanes], value_ref[:, lanes]
        upstream = upstream_ref[:, lanes]
        probs_low, scores_low, scores = [], [], []
        for block in range(blocks):
            at = slice(128 * block, 128 * (block + 1))
            probs = probabilities(query[at], key, rows, prefix, block, seqlen)
            probs_grad = lax.dot_general(
                upstream[at], value, (((1,), (1,)), ((), ())), preferred_element_type=F32
            )
            inner = jnp.sum(probs * probs_grad, -1, keepdims=True)
            low = (probs * (probs_grad - inner)).astype(BF)
            probs_low.append(probs.astype(BF))
            scores_low.append(low)
            scores.append(low.astype(F32))
            out = jnp.dot(low, key, preferred_element_type=F32) * 0.125
            query_grad_ref[at, lanes] = out.astype(BF)
        probs_all = jnp.concatenate(probs_low, 0)
        scores_all = jnp.concatenate(scores_low, 0)
        out = lax.dot_general(probs_all, upstream, flip, preferred_element_type=F32)
        value_grad_ref[:, lanes] = out.astype(BF)
        out = lax.dot_general(scores_all, query, flip, preferred_element_type=F32) * 0.125
        key_grad_ref[:, lanes] = out.astype(BF)
        bias_ref[0, head] = diagonals(scores)


def attention_specs(seqlen, width):
    pairs = HEADS // 2
    table = pl.BlockSpec((1, 2, width), lambda p: (p, 0, 0))
    return (
        [pl.BlockSpec(memory_space=pltpu.SMEM), table]
        + [
            pl.BlockSpec((seqlen, 128), lambda p, part=part: (0, part * pairs + p))
            for part in range(3)
        ],
        pl.BlockSpec((seqlen, 128), lambda p: (0, p)),
    )


def attend(prefix, table, projected):
    seqlen = projected.shape[0]
    ins, out = attention_specs(seqlen, table.shape[-1])
    return pl.pallas_call(
        attend_kernel,
        grid=(HEADS // 2,),
        in_specs=ins,
        out_specs=out,
        out_shape=jax.ShapeDtypeStruct((seqlen, D), BF),
        cost_estimate=pl.CostEstimate(
            flops=4 * seqlen * seqlen * D,
            bytes_accessed=8 * seqlen * D,
            transcendentals=HEADS * seqlen * seqlen,
        ),
        name="attend",
    )(prefix, table, projected, projected, projected)


def attend_back(prefix, table, projected, upstream):
    seqlen = projected.shape[0]
    width = table.shape[-1]
    ins, out = attention_specs(seqlen, width)
    grad = jax.ShapeDtypeStruct((seqlen, D), BF)
    return pl.pallas_call(
        attend_back_kernel,
        grid=(HEADS // 2,),
        in_specs=ins + [out],
        out_specs=[out, out, out, pl.BlockSpec((1, 2, 8, width), lambda p: (p, 0, 0, 0))],
        out_shape=[grad, grad, grad, jax.ShapeDtypeStruct((HEADS // 2, 2, 8, width), F32)],
        cost_estimate=pl.CostEstimate(
            flops=10 * seqlen * seqlen * D,
            bytes_accessed=14 * seqlen * D,
            transcendentals=HEADS * seqlen * seqlen,
        ),
        name="attend_back",
    )(prefix, table, projected, projected, projected, upstream)


def where_am_i():
    dp, expert = lax.axis_index("dp"), lax.axis_index("expert")
    return dp // 2, dp % 2, expert // 2, expert % 2


def device_at(z, x, y, core):
    return (2 * z + x, 2 * y + core)


def greet(z, x, y, core):
    barrier = pltpu.get_barrier_semaphore()

    def call(*place):
        pl.semaphore_signal(
            barrier, inc=1, device_id=device_at(*place), device_id_type=pl.DeviceIdType.MESH
        )

    call(z, 1 - x, y, core)
    call(z, x, 1 - y, core)
    call(z, x, y, 1 - core)
    call(z, x, 1 - y, 1 - core)

    @pl.when(z > 0)
    def _():
        call(z - 1, x, y, core)

    @pl.when(z < 3)
    def _():
        call(z + 1, x, y, core)

    pl.semaphore_wait(barrier, 4 + (z > 0).astype(jnp.int32) + (z < 3).astype(jnp.int32))


def gather_kernel(
    up_ref,
    down_ref,
    dense_ref,
    small_ref,
    tokens_ref,
    cotangent_ref,
    chosen_ref,
    hits_ref,
    prefix_ref,
    gate_full,
    up_full,
    down_full,
    dense_full,
    small_full,
    hidden_ref,
    projected_ref,
    attended_ref,
    residual_ref,
    table_ref,
    arrived_ref,
    grads_ref,
    second_ref,
    rows_ref,
    local_sem,
    z_send,
    z_recv,
    x_send,
    x_recv,
    dz_send,
    dz_recv,
    d_send,
    d_recv,
    turn_send,
    turn_recv,
    a_send,
    a_recv,
):
    z, x, y, core = where_am_i()
    greet(z, x, y, core)
    share = dense_ref.shape[1]
    sides = {1: z < 3, -1: z > 0}

    def piece(c, row, column):
        return (gate_full, up_full, down_full)[c].at[2 * row + column]

    def mine(c):
        return up_ref.at[c] if c < 2 else down_ref

    def copy_z(c, row, side, own=False):
        return pltpu.make_async_remote_copy(
            src_ref=mine(c) if own else piece(c, row, x),
            dst_ref=piece(c, row, x),
            send_sem=z_send.at[c, (side + 1) // 2, row],
            recv_sem=z_recv.at[c, row],
            device_id=device_at(z + side, x, y, core),
            device_id_type=pl.DeviceIdType.MESH,
        )

    def copy_x(c, row, own=False):
        return pltpu.make_async_remote_copy(
            src_ref=mine(c) if own else piece(c, row, x),
            dst_ref=piece(c, row, x),
            send_sem=x_send.at[c, row],
            recv_sem=x_recv.at[c, row],
            device_id=device_at(z, 1 - x, y, core),
            device_id_type=pl.DeviceIdType.MESH,
        )

    inner = (z == 1) | (z == 2)
    inward, outward = jnp.where(z == 1, 1, -1), jnp.where(z == 1, -1, 1)
    outer_row = jnp.where(z == 1, 3, 0)

    def copy_turn(row, side, number):
        return pltpu.make_async_remote_copy(
            src_ref=piece(0, row, 1 - x),
            dst_ref=piece(0, row, 1 - x),
            send_sem=turn_send.at[number],
            recv_sem=turn_recv.at[0],
            device_id=device_at(z + side, x, y, core),
            device_id_type=pl.DeviceIdType.MESH,
        )

    def send_own(c):
        for side in (1, -1):
            @pl.when(sides[side])
            def _(side=side):
                copy_z(c, z, side, True).start()
        copy_x(c, z, True).start()

    def slot(row, column, line, number):
        return row * 8 + column * 4 + line * 2 + number

    def dense_copies(row, column, line, link, own=False):
        at = slot(row, column, line, core)
        target, sems, index = {
            "right": (device_at(z + 1, x, y, core), dz_send, (1, row)),
            "left": (device_at(z - 1, x, y, core), dz_send, (0, row)),
            "x": (device_at(z, 1 - x, y, core), d_send, (0, row)),
            "y": (device_at(z, x, 1 - y, core), d_send, (1, row * 2 + column)),
            "core": (device_at(z, x, y, 1 - core), d_send, (2, row * 4 + column * 2 + line)),
        }[link]
        if sems is dz_send:
            recv, place = dz_recv, (row,)
        else:
            recv, place = d_recv, index
        rows = pl.ds(pl.multiple_of(at * share, share), share)
        return [
            pltpu.make_async_remote_copy(
                src_ref=dense_ref if own else dense_full.at[:, rows],
                dst_ref=dense_full.at[:, rows],
                send_sem=sems.at[(0,) + index],
                recv_sem=recv.at[(0,) + place],
                device_id=target,
                device_id_type=pl.DeviceIdType.MESH,
            ),
            pltpu.make_async_remote_copy(
                src_ref=small_ref if own else small_full.at[at],
                dst_ref=small_full.at[at],
                send_sem=sems.at[(1,) + index],
                recv_sem=recv.at[(1,) + place],
                device_id=target,
                device_id_type=pl.DeviceIdType.MESH,
            ),
        ]

    def each(copies, step):
        for copy in copies:
            getattr(copy, step)()

    own_at = slot(z, x, y, core)
    own_rows = pl.ds(pl.multiple_of(own_at * share, share), share)
    local = [
        pltpu.make_async_copy(up_ref.at[0], gate_full.at[2 * z + x], local_sem.at[0]),
        pltpu.make_async_copy(up_ref.at[1], up_full.at[2 * z + x], local_sem.at[4]),
        pltpu.make_async_copy(down_ref, down_full.at[2 * z + x], local_sem.at[1]),
        pltpu.make_async_copy(dense_ref, dense_full.at[:, own_rows], local_sem.at[2]),
        pltpu.make_async_copy(small_ref, small_full.at[own_at], local_sem.at[3]),
    ]

    for side, link in ((1, "right"), (-1, "left")):
        @pl.when(sides[side])
        def _(link=link):
            each(dense_copies(z, x, y, link, True), "start")
    for link in ("x", "y", "core"):
        each(dense_copies(z, x, y, link, True), "start")
    send_own(0)
    each(local, "start")

    def x_arrived(row):
        each(dense_copies(row, 1 - x, y, "x"), "wait_recv")
        each(dense_copies(row, 1 - x, y, "y"), "start")
        each(dense_copies(row, 1 - x, y, "core"), "start")

    for s in (1, 2, 3):
        for side, link in ((1, "right"), (-1, "left")):
            row = z - side * s
            there = (z >= s) if side > 0 else (z + s <= 3)

            @pl.when(there)
            def _(row=row, side=side, link=link):
                each(dense_copies(row, x, y, link), "wait_recv")

                @pl.when(sides[side])
                def _():
                    each(dense_copies(row, x, y, link), "start")

                for other in ("x", "y", "core"):
                    each(dense_copies(row, x, y, other), "start")
        if s == 1:
            x_arrived(z)
        if s < 3:
            send_own(s)
    for s in (1, 2, 3):
        for row, there in ((z - s, z >= s), (z + s, z + s <= 3)):
            @pl.when(there)
            def _(row=row):
                x_arrived(row)
    for s in range(4):
        for column in range(2):
            row = lax.rem(z + s, 4)
            each(dense_copies(row, column, 1 - y, "y"), "wait_recv")
            each(dense_copies(row, column, 1 - y, "core"), "start")

    def pass_on(c, s):
        for side in (1, -1):
            row = z - side * s
            there = (z >= s) if side > 0 else (z + s <= 3)

            @pl.when(there)
            def _(row=row, side=side):
                copy_z(c, row, side).wait_recv()

                @pl.when(sides[side])
                def _():
                    copy_z(c, row, side).start()

                if c == 0:
                    @pl.when(row != 3 - z)
                    def _():
                        copy_x(c, row).start()
                else:
                    copy_x(c, row).start()

    for c in range(3):
        pass_on(c, 1)

    @pl.when(inner)
    def _():
        copy_x(0, z).wait_recv()
        copy_turn(z, inward, 0).start()

    for row in range(4):
        for column in range(2):
            for line in range(2):
                at = slot(row, column, line, 1 - core)
                rows = pl.ds(pl.multiple_of(at * share, share), share)
                index = row * 4 + column * 2 + line
                for part, ref in enumerate((dense_full.at[:, rows], small_full.at[at])):
                    pltpu.make_async_remote_copy(
                        src_ref=ref,
                        dst_ref=ref,
                        send_sem=d_send.at[part, 2, index],
                        recv_sem=d_recv.at[part, 2, index],
                        device_id=device_at(z, x, y, 1 - core),
                        device_id_type=pl.DeviceIdType.MESH,
                    ).wait_recv()
    each(local, "wait")

    width = dense_full.shape[2]
    lane = lax.broadcasted_iota(jnp.int32, (small_full.shape[0], width), 1)
    line_of = lax.broadcasted_iota(jnp.int32, (small_full.shape[0], width), 0)
    spread = (
        lax.broadcasted_iota(jnp.int32, (share, width), 1) % share
        == lax.broadcasted_iota(jnp.int32, (share, width), 0)
    ).astype(F32)

    def whole_row(row, start):
        shares = small_full[:, row, start : start + share]
        wide = jnp.dot(shares, spread, precision=HIGHEST, preferred_element_type=F32)
        return jnp.sum(jnp.where(lane // share == line_of, wide, 0.0), 0, keepdims=True)

    gain = whole_row(1, 0)
    bias_parts = small_full[:, 2, 0 : BUCKETS // 2]
    low = jnp.dot(bias_parts, hits_ref[: BUCKETS // 2], precision=HIGHEST, preferred_element_type=F32)
    high = jnp.dot(bias_parts, hits_ref[BUCKETS // 2 :], precision=HIGHEST, preferred_element_type=F32)
    for head in range(HEADS):
        table_ref[head : head + 1] = low[2 * head : 2 * head + 1] + high[2 * head + 1 : 2 * head + 2]
    seqlen = tokens_ref.shape[0]
    step = 128

    @pl.loop(0, seqlen // step)
    def _(i):
        at = pl.ds(pl.multiple_of(i * step, step), step)
        hidden_ref[at] = normed(tokens_ref[at].astype(F32), gain).astype(BF)

    tile = 256
    for part in range(3):
        @pl.loop(0, width // tile)
        def _(n, part=part):
            at = pl.ds(pl.multiple_of(n * tile, tile), tile)
            out = jnp.dot(hidden_ref[...], dense_full[part, :, at], preferred_element_type=F32)
            at = pl.ds(pl.multiple_of(part * width + n * tile, tile), tile)
            projected_ref[:, at] = out.astype(BF)

    prefix = prefix_ref[0]

    @pl.loop(0, HEADS // 2)
    def _(pair):
        def window(part):
            return pl.ds(pl.multiple_of(part * width + pair * 128, 128), 128)

        query_ref = projected_ref.at[:, window(0)]
        key_ref = projected_ref.at[:, window(1)]
        value_ref = projected_ref.at[:, window(2)]
        out_ref = attended_ref.at[:, window(0)]
        for head in range(2):
            lanes = slice(head * HEAD_DIM, (head + 1) * HEAD_DIM)
            rows = bias_rows(table_ref[pl.ds(2 * pair + head, 1), :], seqlen)
            key, value = key_ref[:, lanes], value_ref[:, lanes]
            for block in range(seqlen // 128):
                at = slice(128 * block, 128 * (block + 1))
                probs = probabilities(query_ref[at, lanes], key, rows, prefix, block, seqlen)
                out = jnp.dot(probs.astype(BF), value, preferred_element_type=F32)
                out_ref[at, lanes] = out.astype(BF)

        for c in range(3):
            @pl.when(pair == 3 * c + 1)
            def _(c=c):
                pass_on(c, 2)

    @pl.loop(0, width // tile)
    def _(n):
        at = pl.ds(pl.multiple_of(n * tile, tile), tile)
        out = jnp.dot(attended_ref[...], dense_full[3, :, at], preferred_element_type=F32)
        residual_ref[:, at] = tokens_ref[:, at].astype(F32) + out

    gain = whole_row(1, share)
    experts, capacity = arrived_ref.shape[0], arrived_ref.shape[1]
    router = [whole_row(0, share * number) for number in range(experts)]
    router = jnp.concatenate(router + [jnp.zeros((8 - experts, width), F32)], 0)
    logits = []
    for i in range(seqlen // step):
        at = slice(i * step, (i + 1) * step)
        second = normed(residual_ref[at], gain)
        second_ref[at] = second.astype(BF)
        logits.append(
            lax.dot_general(
                router,
                second,
                (((1,), (1,)), ((), ())),
                precision=HIGHEST,
                preferred_element_type=F32,
            )
        )
    logits = jnp.concatenate(logits, 1)[:experts]
    shifted = jnp.exp(logits - jnp.max(logits, 0, keepdims=True))
    soft = shifted / jnp.sum(shifted, 0, keepdims=True)
    chosen = chosen_ref[...]
    weight = soft * chosen[:experts].astype(F32)
    weight = weight / jnp.sum(weight, 0, keepdims=True)
    earlier = (
        lax.broadcasted_iota(jnp.int32, (seqlen, seqlen), 0)
        < lax.broadcasted_iota(jnp.int32, (seqlen, seqlen), 1)
    ).astype(F32)
    rank = jnp.dot(chosen, earlier.astype(BF), preferred_element_type=F32)
    rank = jnp.where(chosen.astype(F32) > 0.0, rank, -1.0).astype(jnp.int32)
    me = 2 * y + core

    def copy_rows(which, number):
        return pltpu.make_async_remote_copy(
            src_ref=rows_ref.at[which, number],
            dst_ref=(arrived_ref, grads_ref)[which].at[me],
            send_sem=a_send.at[which, number],
            recv_sem=a_recv.at[which, me],
            device_id=device_at(z, x, number // 2, number % 2),
            device_id_type=pl.DeviceIdType.MESH,
        )

    def keep_rows(which, number):
        return pltpu.make_async_copy(
            rows_ref.at[which, number],
            (arrived_ref, grads_ref)[which].at[number],
            a_send.at[which, number],
        )

    for number in range(experts):
        taken = (
            lax.broadcasted_iota(jnp.int32, (capacity, seqlen), 0) == rank[number : number + 1]
        ).astype(F32)
        slot_weight = jnp.sum(taken * weight[number : number + 1], 1, keepdims=True)
        pick = taken.astype(BF)

        @pl.loop(0, width // tile)
        def _(n, number=number, pick=pick, slot_weight=slot_weight):
            at = pl.ds(pl.multiple_of(n * tile, tile), tile)
            out = jnp.dot(pick, second_ref[:, at], preferred_element_type=F32)
            rows_ref[0, number, :, at] = out.astype(BF)
            out = jnp.dot(pick, cotangent_ref[:, at], preferred_element_type=F32)
            rows_ref[1, number, :, at] = (slot_weight * out).astype(BF)

        for which in range(2):
            @pl.when(me == number)
            def _(which=which, number=number):
                keep_rows(which, number).start()

            @pl.when(me != number)
            def _(which=which, number=number):
                copy_rows(which, number).start()

    for c in range(3):
        pass_on(c, 3)

    @pl.when(inner)
    def _():
        copy_x(0, outer_row).wait_recv()
        copy_turn(outer_row, outward, 1).start()

    for number in range(experts):
        for which in range(2):
            @pl.when(me == number)
            def _(which=which, number=number):
                keep_rows(which, number).wait()

            @pl.when(me != number)
            def _(which=which, number=number):
                copy_rows(which, number).wait_send()
                pltpu.make_async_remote_copy(
                    src_ref=rows_ref.at[which, number],
                    dst_ref=(arrived_ref, grads_ref)[which].at[number],
                    send_sem=a_send.at[which, number],
                    recv_sem=a_recv.at[which, number],
                    device_id=device_at(z, x, number // 2, number % 2),
                    device_id_type=pl.DeviceIdType.MESH,
                ).wait_recv()

    for row in range(4):
        for column in range(2):
            for line in range(2):
                each(dense_copies(row, column, line, "core"), "wait_send")
        for column in range(2):
            each(dense_copies(row, column, y, "y"), "wait_send")
        each(dense_copies(row, x, y, "x"), "wait_send")
        for side, link in ((1, "right"), (-1, "left")):
            sent = sides[side] & ((row <= z) if side > 0 else (row >= z))

            @pl.when(sent)
            def _(row=row, side=side, link=link):
                each(dense_copies(row, x, y, link), "wait_send")
                for c in range(3):
                    copy_z(c, row, side).wait_send()
        for c in (1, 2):
            copy_x(c, row).wait_recv()
            copy_x(c, row).wait_send()

        @pl.when(z != 3 - row)
        def _(row=row):
            copy_x(0, row).wait_send()

            @pl.when(jnp.logical_not(inner & ((z == row) | (outer_row == row))))
            def _():
                copy_x(0, row).wait_recv()

    copy_turn(3 - z, 0, 0).wait_recv()

    @pl.when(inner)
    def _():
        copy_turn(z, inward, 0).wait_send()
        copy_turn(outer_row, outward, 1).wait_send()


def gather_weights(up, down, dense, small, tokens, cotangent, chosen, hits, prefix, capacity):
    seqlen, width = tokens.shape
    devices = lax.axis_size(BOTH)
    slices, experts = lax.axis_size("dp"), lax.axis_size("expert")
    vmem, hbm = pl.BlockSpec(memory_space=pltpu.VMEM), pl.BlockSpec(memory_space=pl.ANY)
    dma = pltpu.SemaphoreType.DMA
    return pl.pallas_call(
        gather_kernel,
        in_specs=[vmem] * 8 + [pl.BlockSpec(memory_space=pltpu.SMEM)],
        out_specs=[hbm] * 3 + [vmem] * 7 + [hbm] * 2,
        out_shape=[
            jax.ShapeDtypeStruct((slices,) + up.shape[1:], BF),
            jax.ShapeDtypeStruct((slices,) + up.shape[1:], BF),
            jax.ShapeDtypeStruct((slices,) + down.shape, BF),
            jax.ShapeDtypeStruct((dense.shape[0], devices * dense.shape[1], dense.shape[2]), BF),
            jax.ShapeDtypeStruct((devices,) + small.shape, F32),
            jax.ShapeDtypeStruct((seqlen, width), BF),
            jax.ShapeDtypeStruct((seqlen, 3 * width), BF),
            jax.ShapeDtypeStruct((seqlen, width), BF),
            jax.ShapeDtypeStruct((seqlen, width), F32),
            jax.ShapeDtypeStruct((HEADS, hits.shape[1]), F32),
            jax.ShapeDtypeStruct((experts, capacity, width), BF),
            jax.ShapeDtypeStruct((experts, capacity, width), BF),
        ],
        scratch_shapes=[
            pltpu.VMEM((seqlen, width), BF),
            pltpu.VMEM((2, experts, capacity, width), BF),
            dma((5,)),
            dma((3, 2, 4)),
            dma((3, 4)),
            dma((3, 4)),
            dma((3, 4)),
            dma((2, 2, 4)),
            dma((2, 4)),
            dma((2, 3, 16)),
            dma((2, 3, 16)),
            dma((2,)),
            dma((1,)),
            dma((2, experts)),
            dma((2, experts)),
        ],
        compiler_params=pltpu.CompilerParams(collective_id=1, has_side_effects=True, vmem_limit_bytes=60 * 2**20),
        name="gather_weights",
    )(up, down, dense, small, tokens, cotangent, chosen, hits, prefix)


def reduce_kernel(
    gate_grads,
    up_grads,
    down_grads,
    dense_ref,
    hidden_turned,
    attended_turned,
    branch_ref,
    projected_ref,
    table_ref,
    prefix_ref,
    up_out,
    down_out,
    dense_out,
    hidden_grad,
    bias_ref,
    square_ref,
    wide_got,
    tall_got,
    wide_line,
    tall_line,
    wide_own,
    tall_own,
    grads_ref,
    upstream_ref,
    full_ref,
    core_got,
    y_got,
    x_got,
    line_got,
    own_sem,
    x_send,
    x_recv,
    z_send,
    z_recv,
    core_send,
    core_recv,
    y_send,
    y_recv,
    dx_send,
    dx_recv,
):
    z, x, y, core = where_am_i()
    greet(z, x, y, core)
    mesh_id = pl.DeviceIdType.MESH
    share = dense_out.shape[1]
    parts, width = full_ref.shape[0], full_ref.shape[2]
    grads = (gate_grads, up_grads, down_grads)

    def got(c, row):
        return wide_got.at[c, row] if c < 2 else tall_got.at[row] if c == 2 else x_got.at[row]

    def line(c, place):
        return wide_line.at[c, place] if c < 2 else tall_line.at[place] if c == 2 else line_got.at[place]

    def own(c):
        return wide_own.at[c] if c < 2 else tall_own

    def load(c, row):
        return pltpu.make_async_copy(grads[c].at[2 * row + x], own(c), own_sem.at[c])

    def copy_x(c, row):
        return pltpu.make_async_remote_copy(
            src_ref=grads[c].at[2 * row + 1 - x],
            dst_ref=got(c, row),
            send_sem=x_send.at[c, row],
            recv_sem=x_recv.at[c, row],
            device_id=device_at(z, 1 - x, y, core),
            device_id_type=mesh_id,
        )

    def copy_z(c, row, side, place):
        return pltpu.make_async_remote_copy(
            src_ref=got(c, row),
            dst_ref=line(c, place),
            send_sem=z_send.at[c, row],
            recv_sem=z_recv.at[c, place],
            device_id=device_at(z + side, x, y, core),
            device_id_type=mesh_id,
        )

    def add(out, terms):
        shape = out.shape
        if len(shape) == 3:
            @pl.loop(0, shape[0])
            def _(i):
                total = functools.reduce(jnp.add, [term[i].astype(F32) for term in terms])
                out[i] = total.astype(out.dtype)
        else:
            @pl.loop(0, shape[0] // 16)
            def _(i):
                at = pl.ds(pl.multiple_of(i * 16, 16), 16)
                total = functools.reduce(jnp.add, [term[at].astype(F32) for term in terms])
                out[at] = total.astype(out.dtype)

    there = {}
    for s in (3, 2, 1):
        there[s, 1] = z + s <= 3
        there[s, -1] = z >= s
    order = [(s, side) for s in (3, 2, 1) for side in (1, -1)]

    def row_of(s, side):
        return lax.rem(z + side * s + 4, 4)

    def step(c, s, side):
        row = row_of(s, side)

        def run():
            if c < 3:
                copy_x(c, row).wait_recv()
            terms = [got(c, row)] + ([own(c)] if c < 3 else [])
            before = (z > 0) if side > 0 else (z < 3)

            @pl.when(before)
            def _():
                copy_z(c, row, side, row).wait_recv()
                add(got(c, row), terms + [line(c, row)])

            if c < 3:
                @pl.when(jnp.logical_not(before))
                def _():
                    add(got(c, row), terms)

            copy_z(c, row, side, 4 if (s == 1 and side < 0) else row).start()

        if c < 3:
            load(c, row).wait()
        pl.when(there[s, side])(run)
        if c < 3:
            index = order.index((s, side)) + 1
            load(c, row_of(*order[index]) if index < len(order) else z).start()

    def last(c, out):
        if c < 3:
            copy_x(c, z).wait_recv()
            load(c, z).wait()
            add(out, [got(c, z), own(c)])
        else:
            add(out, [got(c, z)])

        @pl.when(z > 0)
        def _():
            copy_z(c, z, 1, z).wait_recv()
            add(out, [out, line(c, z)])

        @pl.when(z < 3)
        def _():
            copy_z(c, z, -1, 4).wait_recv()
            add(out, [out, line(c, 4)])

    for s, side in order:
        @pl.when(there[s, side])
        def _(s=s, side=side):
            for c in range(3):
                copy_x(c, row_of(s, side)).start()
    for c in range(3):
        load(c, row_of(3, 1)).start()

    turned = (((1,), (1,)), ((), ()))
    flip = (((0,), (0,)), ((), ()))
    tile = 256

    @pl.loop(0, width // tile)
    def _(n):
        at = pl.ds(pl.multiple_of(n * tile, tile), tile)
        out = lax.dot_general(
            branch_ref[...], dense_ref[3, at, :], turned, preferred_element_type=F32
        )
        upstream_ref[:, at] = out.astype(BF)
        out = jnp.dot(attended_turned[...], branch_ref[:, at], preferred_element_type=F32)
        full_ref[3, :, at] = out.astype(BF)

    seqlen = projected_ref.shape[0]
    blocks = seqlen // 128
    prefix = prefix_ref[0]

    def attend_pair(pair):
        def window(part):
            return pl.ds(pl.multiple_of(part * width + pair * 128, 128), 128)

        for head in range(2):
            lanes = slice(head * HEAD_DIM, (head + 1) * HEAD_DIM)
            rows = bias_rows(table_ref[pl.ds(2 * pair + head, 1), :], seqlen)
            query = projected_ref.at[:, window(0)][:, lanes]
            key = projected_ref.at[:, window(1)][:, lanes]
            value = projected_ref.at[:, window(2)][:, lanes]
            upstream = upstream_ref.at[:, window(0)][:, lanes]
            probs_low, scores_low, scores = [], [], []
            for block in range(blocks):
                at = slice(128 * block, 128 * (block + 1))
                probs = probabilities(query[at], key, rows, prefix, block, seqlen)
                probs_grad = lax.dot_general(
                    upstream[at], value, turned, preferred_element_type=F32
                )
                inner = jnp.sum(probs * probs_grad, -1, keepdims=True)
                low = (probs * (probs_grad - inner)).astype(BF)
                probs_low.append(probs.astype(BF))
                scores_low.append(low)
                scores.append(low.astype(F32))
                out = jnp.dot(low, key, preferred_element_type=F32) * 0.125
                grads_ref.at[:, window(0)][at, lanes] = out.astype(BF)
            probs_all = jnp.concatenate(probs_low, 0)
            scores_all = jnp.concatenate(scores_low, 0)
            out = lax.dot_general(probs_all, upstream, flip, preferred_element_type=F32)
            grads_ref.at[:, window(2)][:, lanes] = out.astype(BF)
            out = lax.dot_general(scores_all, query, flip, preferred_element_type=F32) * 0.125
            grads_ref.at[:, window(1)][:, lanes] = out.astype(BF)
            bias_ref[pl.ds(2 * pair + head, 1)] = diagonals(scores)[None]

    @pl.loop(0, HEADS // 2)
    def _(pair):
        attend_pair(pair)
        for c, when in ((0, 3), (1, 7)):
            @pl.when(pair == when)
            def _(c=c):
                step(c, 3, 1)
                step(c, 3, -1)

    for part in range(3):
        @pl.loop(0, width // tile)
        def _(n, part=part):
            at = pl.ds(pl.multiple_of(n * tile, tile), tile)
            from_at = pl.ds(pl.multiple_of(part * width + n * tile, tile), tile)
            out = jnp.dot(hidden_turned[...], grads_ref[:, from_at], preferred_element_type=F32)
            full_ref[part, :, at] = out.astype(BF)

    def rows_of(k, number):
        at = (k // 2) * 4 + (k % 2) * 2 + number
        return pl.ds(pl.multiple_of(at * share, share), share)

    def copy_core(k):
        return pltpu.make_async_remote_copy(
            src_ref=full_ref.at[:, rows_of(k, 1 - core)],
            dst_ref=core_got.at[k],
            send_sem=core_send.at[k],
            recv_sem=core_recv.at[k],
            device_id=device_at(z, x, y, 1 - core),
            device_id_type=mesh_id,
        )

    def copy_y(k):
        return pltpu.make_async_remote_copy(
            src_ref=core_got.at[2 * k + 1 - y],
            dst_ref=y_got.at[k],
            send_sem=y_send.at[k],
            recv_sem=y_recv.at[k],
            device_id=device_at(z, x, 1 - y, core),
            device_id_type=mesh_id,
        )

    def copy_dx(row):
        return pltpu.make_async_remote_copy(
            src_ref=y_got.at[2 * row + 1 - x],
            dst_ref=x_got.at[row],
            send_sem=dx_send.at[row],
            recv_sem=dx_recv.at[row],
            device_id=device_at(z, 1 - x, y, core),
            device_id_type=mesh_id,
        )

    @pl.loop(0, 16)
    def _(k):
        copy_core(k).start()

    step(2, 3, 1)
    step(2, 3, -1)

    @pl.loop(0, width // tile)
    def _(n):
        at = pl.ds(pl.multiple_of(n * tile, tile), tile)
        total = None
        for part in range(3):
            out = lax.dot_general(
                grads_ref[:, part * width : (part + 1) * width],
                dense_ref[part, at, :],
                turned,
                preferred_element_type=F32,
            )
            total = out if total is None else total + out
        hidden_grad[:, at] = total

    @pl.loop(0, 8)
    def _(k):
        for line_y in range(2):
            copy_core(2 * k + line_y).wait_recv()
            for part in range(parts):
                mine = full_ref.at[part, rows_of(2 * k + line_y, core)]
                other = core_got.at[2 * k + line_y, part]
                other[...] = (other[...].astype(F32) + mine[...].astype(F32)).astype(BF)
        copy_y(k).start()

    for c in range(3):
        step(c, 2, 1)
        step(c, 2, -1)
    step(0, 1, 1)
    step(0, 1, -1)

    @pl.loop(0, 4)
    def _(row):
        for column in range(2):
            k = 2 * row + column
            copy_y(k).wait_recv()
            for part in range(parts):
                mine, other = core_got.at[2 * k + y, part], y_got.at[k, part]
                other[...] = (other[...].astype(F32) + mine[...].astype(F32)).astype(BF)
        copy_dx(row).start()

    for c in range(3):
        copy_x(c, z).start()
    for c in (1, 2):
        step(c, 1, 1)
        step(c, 1, -1)

    @pl.loop(0, 4)
    def _(row):
        copy_dx(row).wait_recv()
        for part in range(parts):
            mine, other = y_got.at[2 * row + x, part], x_got.at[row, part]
            other[...] = (other[...].astype(F32) + mine[...].astype(F32)).astype(BF)

    for s, side in order:
        step(3, s, side)
    def square(ref):
        def more(i, total):
            at = pl.ds(pl.multiple_of(i * 16, 16), 16)
            return total + jnp.sum(ref[at] * ref[at], 0, keepdims=True)

        rows, columns = ref.shape
        total = lax.fori_loop(0, rows // 16, more, jnp.zeros((1, columns), F32))
        return jnp.sum(total, 1, keepdims=True)

    last(0, up_out.at[0])
    last(1, up_out.at[1])
    last(3, dense_out)
    up_square = square(up_out.at[0]) + square(up_out.at[1])
    attend_square = functools.reduce(jnp.add, [square(dense_out.at[part]) for part in range(3)])
    outward_square = square(dense_out.at[3])
    last(2, down_out)
    lane = lax.broadcasted_iota(jnp.int32, square_ref.shape, 1)
    square_ref[...] = in_lanes(
        lane, {0: attend_square, 1: outward_square, 5: up_square, 6: square(down_out)}
    )

    @pl.loop(0, 16)
    def _(k):
        copy_core(k).wait_send()

    @pl.loop(0, 8)
    def _(k):
        copy_y(k).wait_send()

    @pl.loop(0, 4)
    def _(row):
        copy_dx(row).wait_send()
        for c in range(3):
            copy_x(c, row).wait_send()

    for s, side in order:
        @pl.when(there[s, side])
        def _(s=s, side=side):
            for c in range(4):
                copy_z(c, row_of(s, side), side, row_of(s, side)).wait_send()


def reduce_weights(gate, up, down, dense, hidden, attended, branch, projected, table, prefix):
    seqlen, width = hidden.shape
    share = width // lax.axis_size(BOTH)
    vmem, hbm = pl.BlockSpec(memory_space=pltpu.VMEM), pl.BlockSpec(memory_space=pl.ANY)
    dma = pltpu.SemaphoreType.DMA
    wide, tall = gate.shape[1:], down.shape[1:]
    dense_shape = (dense.shape[0], share, width)
    return pl.pallas_call(
        reduce_kernel,
        in_specs=[hbm] * 3 + [vmem] * 6 + [pl.BlockSpec(memory_space=pltpu.SMEM)],
        out_specs=[vmem] * 6,
        out_shape=[
            jax.ShapeDtypeStruct((2,) + wide, F32),
            jax.ShapeDtypeStruct(tall, F32),
            jax.ShapeDtypeStruct(dense_shape, F32),
            jax.ShapeDtypeStruct((seqlen, width), F32),
            jax.ShapeDtypeStruct((HEADS, 8, table.shape[1]), F32),
            jax.ShapeDtypeStruct((1, width), F32),
        ],
        scratch_shapes=[
            pltpu.VMEM((2, 4) + wide, BF),
            pltpu.VMEM((4,) + tall, BF),
            pltpu.VMEM((2, 5) + wide, BF),
            pltpu.VMEM((5,) + tall, BF),
            pltpu.VMEM((2,) + wide, BF),
            pltpu.VMEM(tall, BF),
            pltpu.VMEM((seqlen, 3 * width), BF),
            pltpu.VMEM((seqlen, width), BF),
            pltpu.VMEM(dense.shape, BF),
            pltpu.VMEM((16,) + dense_shape, BF),
            pltpu.VMEM((8,) + dense_shape, BF),
            pltpu.VMEM((4,) + dense_shape, BF),
            pltpu.VMEM((5,) + dense_shape, BF),
            dma((3,)),
            dma((3, 4)),
            dma((3, 4)),
            dma((4, 4)),
            dma((4, 5)),
            dma((16,)),
            dma((16,)),
            dma((8,)),
            dma((8,)),
            dma((4,)),
            dma((4,)),
        ],
        compiler_params=pltpu.CompilerParams(
            collective_id=2, has_side_effects=True, vmem_limit_bytes=67043328
        ),
        name="reduce_weights",
    )(gate, up, down, dense, hidden.T, attended.T, branch, projected, table, prefix)


def in_lanes(lane, values):
    return functools.reduce(
        jnp.add, [jnp.where(lane == which, value, 0.0) for which, value in values.items()]
    )


def total_squares(sums):
    def square(low, high):
        both = jnp.sum(sums[low:high] * sums[low:high], 1, keepdims=True)
        return jnp.sum(both, 0, keepdims=True)

    lane = lax.broadcasted_iota(jnp.int32, (1, sums.shape[1]), 1)
    return sums[7:8] + in_lanes(lane, {2: square(0, 4), 3: square(4, 6), 4: square(6, 7)})


def sum_kernel(array_ref, out_ref, square_ref, sent, got, send_sem, recv_sem):
    z, x, y, core = where_am_i()
    barrier = pltpu.get_barrier_semaphore()
    pairs = [(z, x, y, 1 - core), (z, x, 1 - y, core), (z, 1 - x, y, core)]
    lines = [(lax.rem(z + s, 4), x, y, core) for s in (1, 2, 3)]
    for place in pairs + lines:
        pl.semaphore_signal(
            barrier, inc=1, device_id=device_at(*place), device_id_type=pl.DeviceIdType.MESH
        )
    pl.semaphore_wait(barrier, 6)

    def copy(stage, number, slot, place):
        return pltpu.make_async_remote_copy(
            src_ref=sent.at[stage],
            dst_ref=got.at[slot],
            send_sem=send_sem.at[number],
            recv_sem=recv_sem.at[slot],
            device_id=device_at(*place),
            device_id_type=pl.DeviceIdType.MESH,
        )

    total = array_ref[...]
    for stage, place in enumerate(pairs):
        sent[stage] = total
        move = copy(stage, stage, stage, place)
        move.start()
        move.wait()
        total = total + got[stage]
    sent[3] = total
    moves = [copy(3, 3 + number, 3 + z, place) for number, place in enumerate(lines)]
    for move in moves:
        move.start()
    for row in range(4):
        @pl.when(z == row)
        def _(row=row):
            got[3 + row] = sent[3]

        @pl.when(z != row)
        def _(row=row):
            copy(3, 3, 3 + row, lines[0]).wait_recv()
    total = got[3] + got[4] + got[5] + got[6]
    out_ref[...] = total
    square_ref[...] = total_squares(total)
    for move in moves:
        move.wait_send()


def sum_all(array):
    if not is_line():
        sums = lax.psum(array, BOTH)
        return sums, total_squares(sums)
    vmem = pl.BlockSpec(memory_space=pltpu.VMEM)
    dma = pltpu.SemaphoreType.DMA
    return pl.pallas_call(
        sum_kernel,
        in_specs=[vmem],
        out_specs=[vmem, vmem],
        out_shape=[
            jax.ShapeDtypeStruct(array.shape, F32),
            jax.ShapeDtypeStruct((1, array.shape[1]), F32),
        ],
        scratch_shapes=[
            pltpu.VMEM((4,) + array.shape, F32),
            pltpu.VMEM((7,) + array.shape, F32),
            dma((6,)),
            dma((7,)),
        ],
        compiler_params=pltpu.CompilerParams(collective_id=3, has_side_effects=True),
        name="sum_all",
    )(array)


def on_device(
    tokens,
    cotangent,
    routes,
    prefix,
    buckets,
    step_count,
    learn_rate,
    weight_decay,
    attend_master,
    attend_first,
    attend_second,
    outward_master,
    outward_first,
    outward_second,
    router_master,
    router_first,
    router_second,
    gains_master,
    gains_first,
    gains_second,
    bias_master,
    bias_first,
    bias_second,
    upward_master,
    upward_first,
    upward_second,
    downward_master,
    downward_first,
    downward_second,
):
    devices = lax.axis_size(BOTH)
    share = attend_master.shape[1]
    seqlen = tokens.shape[0]
    experts = router_master.shape[1]
    capacity = seqlen * TOP * 5 // (4 * experts)

    slices = lax.axis_size("dp")
    router_size, gains_size = router_master.size, gains_master.size
    bucket_hits = (buckets[:, None] == jnp.arange(BUCKETS, dtype=jnp.int32)[None, :]).astype(F32)
    offsets = buckets.shape[0]
    inputs = tokens.astype(F32)
    kinds = jnp.arange(experts, dtype=jnp.int32)
    route_hits = (routes[:, :, None] == kinds[None, None, :]).astype(F32)
    hits = jnp.sum(route_hits, 1)
    if is_line():
        chosen = jnp.sum((routes.T[:, None, :] == jnp.arange(8)[None, :, None]).astype(F32), 0)
        hits_wide = jnp.pad(bucket_hits.T, ((0, 0), (0, 2 * seqlen - offsets)))
        small = jnp.concatenate(
            [
                jnp.pad(one.reshape(1, -1), ((0, 0), (0, 128 - one.size)))
                for one in (router_master.T, gains_master, bias_master)
            ]
            + [jnp.zeros((5, 128), F32)]
        )
        dense = jnp.concatenate([attend_master.astype(BF), outward_master.astype(BF)[None]])
        (
            gate_w,
            up_w,
            downward_w,
            dense_w,
            small,
            hidden_one,
            projected,
            attended,
            residual,
            table,
            arrived,
            grad_arrived,
        ) = gather_weights(
            upward_master[:, 0].astype(BF),
            downward_master[0].astype(BF),
            dense,
            small,
            tokens,
            cotangent,
            chosen.astype(BF),
            hits_wide,
            prefix,
            capacity,
        )
        attend_w, outward_w = dense_w[:3], dense_w[3]
        gate_w, up_w = gate_w.reshape(D, FF), up_w.reshape(D, FF)
        downward_w = downward_w.reshape(FF, D)
        router_w = small[:, 0].reshape(devices, experts, share).transpose(0, 2, 1).reshape(D, experts)
        gains_w = small[:, 1, :gains_size].reshape(devices, 2, share).transpose(1, 0, 2).reshape(2, D)
        table = table.reshape(HEADS // 2, 2, 2 * seqlen)
        first_pull = jax.vjp(normed, inputs, gains_w[0])[1]
    else:
        gate_w = gather_dp(upward_master[0, 0].astype(BF)).reshape(D, FF)
        up_w = gather_dp(upward_master[1, 0].astype(BF)).reshape(D, FF)
        downward_w = gather_dp(downward_master[0].astype(BF)).reshape(FF, D)
        attend_w = lax.all_gather(attend_master.astype(BF), BOTH, axis=1, tiled=True)
        outward_w = lax.all_gather(outward_master.astype(BF), BOTH, axis=0, tiled=True)
        router_w = lax.all_gather(router_master, BOTH, axis=0, tiled=True)
        gains_w = lax.all_gather(gains_master, BOTH, axis=1, tiled=True)
        bias_w = lax.all_gather(bias_master, BOTH, axis=0, tiled=True)
        table = jnp.dot(bias_w.reshape(HEADS, BUCKETS), bucket_hits.T, precision=HIGHEST)
        table = jnp.pad(table, ((0, 0), (0, 2 * seqlen - offsets)))
        table = table.reshape(HEADS // 2, 2, 2 * seqlen)
        first_normed, first_pull = jax.vjp(normed, inputs, gains_w[0])
        hidden_one = first_normed.astype(BF)
        projected = jnp.concatenate(
            [
                jnp.dot(hidden_one, attend_w[part], preferred_element_type=F32).astype(BF)
                for part in range(3)
            ],
            1,
        )
        attended = attend(prefix, table, projected)
        residual = inputs + jnp.dot(attended, outward_w, preferred_element_type=F32)

    def gate_piece(residual_in, scale_gain, router_in):
        second_normed = normed(residual_in, scale_gain)
        logits = jnp.dot(second_normed, router_in, precision=HIGHEST)
        router_soft = jax.nn.softmax(logits, axis=-1)
        chosen = jnp.sum(router_soft[:, None, :] * route_hits, -1)
        return (second_normed, chosen / jnp.sum(chosen, -1, keepdims=True))

    (second_normed, combine), gate_pull = jax.vjp(gate_piece, residual, gains_w[1], router_w)
    second_low = second_normed.astype(BF)

    places = jnp.arange(seqlen, dtype=jnp.int32)
    earlier = (places[None, :] < places[:, None]).astype(BF)
    rank = jnp.dot(earlier, hits.astype(BF), preferred_element_type=F32)
    rank = jnp.where(hits > 0, rank, -1.0).astype(jnp.int32)
    slots = jnp.arange(capacity, dtype=jnp.int32)
    taken = rank.T[:, None, :] == slots[None, :, None]
    choose = taken.astype(BF).reshape(experts * capacity, seqlen)
    weight = jnp.sum(combine[:, :, None] * route_hits, 1)
    slot_weight = jnp.sum(jnp.where(taken, weight.T[:, None, :], 0.0), -1)
    backs = [
        (
            (rank[:, :, None] == slots[None, None, :])
            & (routes[:, k][:, None, None] == kinds[None, :, None])
        )
        .astype(BF)
        .reshape(seqlen, experts * capacity)
        for k in range(TOP)
    ]
    back = (rank[:, :, None] == slots[None, None, :]).astype(BF)
    back = back.reshape(seqlen, experts * capacity)

    def exchange(rows, home):
        if home:
            rows = rows.reshape(1, experts, capacity, D)
            rows = lax.all_to_all(rows, "expert", split_axis=1, concat_axis=0, tiled=True)
        else:
            rows = rows.reshape(experts, 1, capacity, D)
            rows = lax.all_to_all(rows, "expert", split_axis=0, concat_axis=1, tiled=True)
        return rows.reshape(experts * capacity, D)

    if is_line():
        arrived = arrived.reshape(experts * capacity, D)
        grad_arrived = grad_arrived.reshape(experts * capacity, D)
    else:
        sent_rows = jnp.dot(choose, second_low, preferred_element_type=F32).astype(BF)
        upstream_rows = jnp.dot(choose, cotangent, preferred_element_type=F32)
        grad_rows = (slot_weight.reshape(-1, 1) * upstream_rows).astype(BF)
        sent_rows, grad_rows = lax.optimization_barrier((sent_rows, grad_rows))
        arrived = exchange(sent_rows, False)
        grad_arrived = exchange(grad_rows, False)

    gate_value = jnp.dot(arrived, gate_w, preferred_element_type=F32).astype(BF)
    up_value = jnp.dot(arrived, up_w, preferred_element_type=F32).astype(BF).astype(F32)
    gelu_value, gelu_slope = gelu_both(gate_value.astype(F32))
    hidden_mid = (gelu_value * up_value).astype(BF)
    expert_out = jnp.dot(hidden_mid, downward_w, preferred_element_type=F32).astype(BF)
    returned = exchange(expert_out, True)

    turned = (((1,), (1,)), ((), ()))
    flipped = (((0,), (0,)), ((), ()))
    grad_mid = lax.dot_general(grad_arrived, downward_w, turned, preferred_element_type=F32)
    grad_gate = (grad_mid * up_value * gelu_slope).astype(BF)
    grad_up = (grad_mid * gelu_value).astype(BF)
    grad_sent = lax.dot_general(grad_gate, gate_w, turned, preferred_element_type=F32)
    grad_sent = grad_sent + lax.dot_general(grad_up, up_w, turned, preferred_element_type=F32)
    grad_sent, returned, grad_gate, grad_up, hidden_mid = lax.optimization_barrier(
        (grad_sent.astype(BF), returned, grad_gate, grad_up, hidden_mid)
    )
    grad_home = exchange(grad_sent, True)


    def weight_grad(left, right):
        full = lax.dot_general(left, right, flipped, preferred_element_type=F32).astype(BF)
        return full.reshape(slices, -1, full.shape[1])

    wide_grads = (
        weight_grad(arrived, grad_gate),
        weight_grad(arrived, grad_up),
        weight_grad(hidden_mid, grad_arrived),
    )

    came_back = jnp.stack(
        [jnp.dot(one, returned, preferred_element_type=F32) for one in backs], 1
    )
    expert_sum = jnp.sum(combine[..., None] * came_back, 1)
    block_output = (residual + expert_sum).astype(BF)
    upstream = cotangent.astype(F32)
    combine_grad = jnp.sum(upstream[:, None, :] * came_back, -1)

    grad_normed = jnp.dot(back, grad_home, preferred_element_type=F32)
    residual_part, gain_two_grad, router_full = gate_pull((grad_normed, combine_grad))
    grad_residual = upstream + residual_part
    grad_branch = grad_residual.astype(BF)
    if is_line():
        upward_g, downward_g, dense_g, grad_hidden_one, bias_parts, squares = reduce_weights(
            *wide_grads,
            dense_w,
            hidden_one,
            attended,
            grad_branch,
            projected,
            table.reshape(HEADS, 2 * seqlen),
            prefix,
        )
        attend_g, outward_g = dense_g[:3], dense_g[3]
        upward_g, downward_g = upward_g[:, None], downward_g[None]
    else:
        upward_g = jnp.stack([scatter_dp(one) for one in wide_grads[:2]])[:, None]
        downward_g = scatter_dp(wide_grads[2])[None]
        outward_full = lax.dot_general(attended, grad_branch, flipped, preferred_element_type=F32)
        outward_g = scatter_all(outward_full.astype(BF).reshape(devices, share, D))
        grad_attended = lax.dot_general(grad_branch, outward_w, turned, preferred_element_type=F32)
        query_grad, key_grad, value_grad, bias_parts = attend_back(
            prefix, table, projected, grad_attended.astype(BF)
        )
        projected_grads = (query_grad, key_grad, value_grad)
        attend_g = scatter_all(
            jnp.concatenate(
                [
                    lax.dot_general(hidden_one, part, flipped, preferred_element_type=F32)
                    .astype(BF)
                    .reshape(devices, share, D)
                    for part in projected_grads
                ],
                1,
            )
        ).reshape(3, share, D)
        grad_hidden_one = functools.reduce(
            jnp.add,
            [
                lax.dot_general(part, attend_w[which], turned, preferred_element_type=F32)
                for which, part in enumerate(projected_grads)
            ],
        )

    inputs_part, gain_one_grad = first_pull(grad_hidden_one)
    input_grad = (grad_residual + inputs_part).astype(BF)

    bias_parts = bias_parts.reshape(HEADS, 8, 2 * seqlen)
    bias_parts = jnp.pad(bias_parts, ((0, 0), (0, 0), (0, 8)))
    per_offset = functools.reduce(
        jnp.add, [bias_parts[:, row, row : row + offsets] for row in range(8)]
    )
    bias_full = jnp.dot(per_offset, bucket_hits, precision=HIGHEST).reshape(-1)

    if not is_line():
        members = {0: attend_g, 1: outward_g, 5: upward_g, 6: downward_g}
        squares = in_lanes(
            jnp.arange(D)[None], {at: jnp.sum(one * one) for at, one in members.items()}
        )
    sums, totals = sum_all(
        jnp.concatenate(
            [
                router_full.T,
                gain_one_grad[None],
                gain_two_grad[None],
                jnp.pad(bias_full, (0, D - bias_full.size))[None],
                squares,
            ]
        )
    )
    place = lax.axis_index(BOTH)
    mine = lax.dynamic_slice(sums[:6], (0, place * share), (6, share))
    router_g, gains_g = mine[:experts].T, mine[4:]
    bias_g = lax.dynamic_slice(sums[6], (place * bias_master.size,), bias_master.shape)

    grads_all = (attend_g, outward_g, router_g, gains_g, bias_g, upward_g, downward_g)
    totals = totals[0, :7]
    counts_all = jnp.array(
        [
            3 * D * D,
            D * D,
            D * experts,
            2 * D,
            HEADS * BUCKETS,
            2 * experts * D * FF,
            experts * FF * D,
        ],
        jnp.float32,
    )
    mean_squares = totals / counts_all
    grad_rms = jnp.sqrt(mean_squares)
    factors = lax.rsqrt(mean_squares + 1e-06)
    step_float = step_count.astype(jnp.float32)
    masters = (
        attend_master,
        outward_master,
        router_master,
        gains_master,
        bias_master,
        upward_master,
        downward_master,
    )
    firsts = (
        attend_first,
        outward_first,
        router_first,
        gains_first,
        bias_first,
        upward_first,
        downward_first,
    )
    seconds = (
        attend_second,
        outward_second,
        router_second,
        gains_second,
        bias_second,
        upward_second,
        downward_second,
    )
    flags = (True, True, True, False, False, True, True)
    updates = [
        adamw_update(
            masters[member],
            firsts[member],
            seconds[member],
            grads_all[member] * factors[member],
            step_float,
            learn_rate,
            weight_decay,
            flags[member],
        )
        for member in range(7)
    ]
    return (
        block_output,
        input_grad,
        grads_all[0],
        updates[0][0],
        updates[0][1],
        updates[0][2],
        grads_all[1],
        updates[1][0],
        updates[1][1],
        updates[1][2],
        grads_all[2],
        updates[2][0],
        updates[2][1],
        updates[2][2],
        grads_all[3],
        updates[3][3],
        updates[3][1],
        updates[3][2],
        grads_all[4],
        updates[4][3],
        updates[4][1],
        updates[4][2],
        grads_all[5],
        updates[5][0],
        updates[5][1],
        updates[5][2],
        grads_all[6],
        updates[6][0],
        updates[6][1],
        updates[6][2],
        grad_rms,
    )


def solution(mesh):
    placed = (
        P(("dp", "expert"), None),
        P(("dp", "expert"), None),
        P(("dp", "expert"), None),
        P(("dp", "expert")),
        P(),
        P(),
        P(),
        P(),
        P(None, ("dp", "expert"), None),
        P(None, ("dp", "expert"), None),
        P(None, ("dp", "expert"), None),
        P(("dp", "expert"), None),
        P(("dp", "expert"), None),
        P(("dp", "expert"), None),
        P(("dp", "expert"), None),
        P(("dp", "expert"), None),
        P(("dp", "expert"), None),
        P(None, ("dp", "expert")),
        P(None, ("dp", "expert")),
        P(None, ("dp", "expert")),
        P(("dp", "expert")),
        P(("dp", "expert")),
        P(("dp", "expert")),
        P(None, "expert", "dp", None),
        P(None, "expert", "dp", None),
        P(None, "expert", "dp", None),
        P("expert", "dp", None),
        P("expert", "dp", None),
        P("expert", "dp", None),
    )
    return jax.shard_map(
        on_device,
        mesh=mesh,
        in_specs=placed,
        out_specs=(
            P(("dp", "expert"), None),
            P(("dp", "expert"), None),
            P(None, ("dp", "expert"), None),
            P(None, ("dp", "expert"), None),
            P(None, ("dp", "expert"), None),
            P(None, ("dp", "expert"), None),
            P(("dp", "expert"), None),
            P(("dp", "expert"), None),
            P(("dp", "expert"), None),
            P(("dp", "expert"), None),
            P(("dp", "expert"), None),
            P(("dp", "expert"), None),
            P(("dp", "expert"), None),
            P(("dp", "expert"), None),
            P(None, ("dp", "expert")),
            P(None, ("dp", "expert")),
            P(None, ("dp", "expert")),
            P(None, ("dp", "expert")),
            P(("dp", "expert")),
            P(("dp", "expert")),
            P(("dp", "expert")),
            P(("dp", "expert")),
            P(None, "expert", "dp", None),
            P(None, "expert", "dp", None),
            P(None, "expert", "dp", None),
            P(None, "expert", "dp", None),
            P("expert", "dp", None),
            P("expert", "dp", None),
            P("expert", "dp", None),
            P("expert", "dp", None),
            P(),
        ),
        check_vma=False,
    )
```
